256 devices in a mesh: grid: 64 (over z, x, core), band: 4 (over y).
Axes of the slice: x: 4, y: 4, z: 8, core: 2. Of those that a mesh axis runs over, the one named last changes fastest.
Arguments:
- basis: float32 [2048, 65536], P('band', 'grid'), as said below
- panel: float32 [1024, 65536], P('band', 'grid'), may hold values from -6 to 6
Outputs:
- new_panel: float32 [1024, 65536], P('band', 'grid')
- coeffs: float32 [2048, 1024], P('band')
The draws below stay inside these ranges and needn't reach their ends.
Inputs may be any that keep to these rules, and one draw needn't show every extreme that they name: The rows of basis are orthogonal to each other, each with squared sum 65536 (to float32 rounding).
All inputs are finite; a program needn't handle non-finite values.
Results may differ from the reference program's by a relative error of at most 0.000073.
Values sent between devices are 32-bit elements; how exact they have to be, the bound alone decides.
A program may use at most 128 MiB of HBM per device.

```python
import jax
import jax.numpy as jnp
from jax import lax

NQ = 2048
NP = 1024
NG = 65536


def draw_basis(key, part):
    sample = jax.random.normal(key, (NG, NQ), jnp.float32)
    ortho, upper = jnp.linalg.qr(sample)
    return (ortho.T * jnp.sqrt(jnp.float32(NG))).astype(jnp.float32)


def shard_levels(key, dims, split, least, high):
    def one(axis_at, blocks):
        steps = jax.random.uniform(jax.random.fold_in(jax.random.fold_in(key, 6), axis_at), (blocks,), jnp.float32, least / len(split), high / len(split))
        return jnp.repeat(jnp.exp(steps), dims[axis_at] // blocks).reshape((-1,) + (1,) * (len(dims) - axis_at - 1))

    loudness = one(*split[0])
    for cut in split[1:]:
        loudness = loudness * one(*cut)
    return loudness


def noise(key, shape, width, bound, shards=(), kind=jnp.bfloat16):
    array = jax.random.normal(key, shape, jnp.float32) * width
    if len(shards) > 0:
        array = shard_levels(key, shape, shards, -0.22, 0.18) * array
    return jnp.clip(array, min=-bound, max=bound).astype(kind)


def setup_inputs(seed: int = 0) -> dict:
    key_list = jax.random.split(jax.random.key(seed), 3)
    basis = draw_basis(jax.random.fold_in(key_list[2], 71), 0)
    panel = noise(key_list[1], (NP, NG), 1.0, 6.0, ((0, 4), (1, 64)), jnp.float32)
    return dict(basis=basis, panel=panel)


def reference(basis, panel):
    highest = lax.Precision.HIGHEST
    n_grid = basis.shape[1]
    coeffs = jnp.dot(basis, panel.T, precision=highest) / n_grid
    projected = panel - jnp.dot(coeffs.T, basis, precision=highest)
    gram = jnp.dot(projected, projected.T, precision=highest) / n_grid
    factor = jnp.linalg.cholesky(gram)
    new_panel = lax.linalg.triangular_solve(factor, projected, left_side=True, lower=True)
    return (new_panel, coeffs)
```

```python
import functools

import jax
import jax.numpy as jnp
from jax import lax
from jax.experimental import pallas as pl
from jax.experimental.pallas import tpu as pltpu
from jax.sharding import PartitionSpec as P

BLOCK = 128
ROWS = 8
CORES = 2
BANDS = 4
ROUNDS = 4
ALONG_X = 4
MESH = pl.DeviceIdType.MESH


def cdot(left, right):
    return lax.dot_general(
        left,
        right,
        (((0,), (0,)), ((), ())),
        precision=lax.Precision.HIGH,
        preferred_element_type=jnp.float32,
    )


def halves(x):
    high = x.astype(jnp.bfloat16)
    low = (x - high.astype(jnp.float32)).astype(jnp.bfloat16)
    return high, low


def left_parts(x):
    high, low = halves(x)
    return jnp.concatenate([high, high, low], 1)


def right_parts(x, axis):
    high, low = halves(x)
    return jnp.concatenate([high, low, high], axis)


def dot_nt(left, right):
    return lax.dot_general(
        left, right, (((1,), (1,)), ((), ())), preferred_element_type=jnp.float32
    )


def tile_of(band, core, turn):
    one, two, three = (lax.rem(band + i, BANDS) for i in (1, 2, 3))
    if turn == 0:
        return 2 * band + core
    if turn == 3:
        return 2 * two + core
    return 2 * (one + core * (three - one)) + turn - 1


class Place:
    def __init__(self, nx, nz):
        self.nx, self.nz = nx, nz
        self.grid = lax.axis_index("grid")
        self.band = lax.axis_index("band")
        self.core = lax.rem(self.grid, CORES)
        self.x = lax.rem(lax.div(self.grid, CORES), nx)
        self.z = lax.div(self.grid, CORES * nx)
        self.at = self.x * nz + self.z

    def id(self, z, x, core):
        return {"grid": (z * self.nx + x) * CORES + core, "band": self.band}

    def other_core(self):
        return self.id(self.z, self.x, 1 - self.core)

    def over_x(self):
        for d in range(1, self.nx):
            x = lax.rem(self.x + d, self.nx)
            yield d - 1, x, self.id(self.z, x, self.core)

    def over_z(self):
        for d in range(1, self.nz):
            z = lax.rem(self.z + d, self.nz)
            yield d - 1, z, self.id(z, self.x, self.core)

    def over_y(self):
        for d in range(1, BANDS):
            band = lax.rem(self.band + d, BANDS)
            yield d - 1, band, {"grid": self.grid, "band": band}

    def barrier(self):
        sem = pltpu.get_barrier_semaphore()
        ids = [self.other_core()]
        ids += [i for _, _, i in self.over_x()]
        ids += [i for _, _, i in self.over_z()]
        ids += [i for _, _, i in self.over_y()]
        for i in ids:
            pl.semaphore_signal(sem, inc=1, device_id=i, device_id_type=MESH)
        pl.semaphore_wait(sem, len(ids))


def remote(src, dst, send, recv, device):
    return pltpu.make_async_remote_copy(
        src_ref=src,
        dst_ref=dst,
        send_sem=send,
        recv_sem=recv,
        device_id=device,
        device_id_type=MESH,
    )


def await_bytes(ref, sem):
    pltpu.make_async_copy(ref, ref, sem).wait()


def reduce_kernel(
    nx, nz, n_grid,
    basis_ref, panel_ref,
    coeffs_ref, own_ref,
    others, lhs, rhs, part, from_core, from_x, from_z, gathered,
    y_send, y_recv, send, recv,
):
    me = Place(nx, nz)
    me.barrier()
    nq, k = basis_ref.shape
    np_ = panel_ref.shape[0]
    pieces = nx * nz
    rq, rp = nq // pieces, np_ // pieces
    half = np_ // 2
    lo, hi = pl.ds(0, half), pl.ds(half, half)
    right = {"grid": me.grid, "band": lax.rem(me.band + 1, BANDS)}
    left = {"grid": me.grid, "band": lax.rem(me.band + BANDS - 1, BANDS)}

    def hop(i, src, dst, device):
        return remote(src, dst, y_send.at[i], y_recv.at[i], device)

    hops = [
        hop(0, panel_ref.at[lo], others.at[2, lo], right),
        hop(1, panel_ref.at[lo], others.at[0, lo], left),
        hop(2, panel_ref.at[hi], others.at[2, hi], right),
        hop(3, panel_ref.at[hi], others.at[0, hi], left),
        hop(4, others.at[2, lo], others.at[1, lo], right),
        hop(5, others.at[0, hi], others.at[1, hi], left),
    ]
    for h in hops[:4]:
        h.start()

    high, low = halves(basis_ref[...])
    lhs[:nq, :k] = high
    lhs[:nq, k : 2 * k] = high
    lhs[:nq, 2 * k :] = low
    high, low = halves(panel_ref[...])
    lhs[nq:, :k] = high
    lhs[nq:, k : 2 * k] = high
    lhs[nq:, 2 * k :] = low

    def multiply(q, tiles):
        for t, tile in enumerate(tiles):
            rows = slice(t * BLOCK, (t + 1) * BLOCK)
            high, low = halves(tile)
            rhs[rows, :k] = high
            rhs[rows, k : 2 * k] = low
            rhs[rows, 2 * k :] = high
        out = dot_nt(lhs[:nq, :], rhs[...])
        for t in range(2):
            part[q, t, :, :rq, :] = out[:, t * BLOCK : (t + 1) * BLOCK].reshape(pieces, rq, BLOCK)
        out = dot_nt(lhs[nq:, :], rhs[...])
        for t in range(2):
            part[q, t, :, rq:, :] = out[:, t * BLOCK : (t + 1) * BLOCK].reshape(pieces, rp, BLOCK)

    mine_x = pl.ds(me.x * nz, nz)

    def to_core(q):
        remote(
            part.at[q, 1 - me.core], from_core.at[q], send.at[0, q], recv.at[0, q], me.other_core()
        ).start()

    def to_x(q):
        await_bytes(from_core.at[q], recv.at[0, q])
        part[q, me.core] += from_core[q]
        for d, x, device in me.over_x():
            remote(
                part.at[q, me.core, pl.ds(x * nz, nz)],
                from_x.at[q, d],
                send.at[1, q],
                recv.at[1, q],
                device,
            ).start()

    def to_z(q):
        await_bytes(from_x.at[q], recv.at[1, q])
        total = part[q, me.core, mine_x]
        for d in range(nx - 1):
            total = total + from_x[q, d]
        part[q, me.core, mine_x] = total
        for d, z, device in me.over_z():
            remote(
                part.at[q, me.core, me.x * nz + z],
                from_z.at[q, d],
                send.at[2, q],
                recv.at[2, q],
                device,
            ).start()

    def back_z(q):
        await_bytes(from_z.at[q], recv.at[2, q])
        total = part[q, me.core, me.at]
        for d in range(nz - 1):
            total = total + from_z[q, d]
        total = total * (1.0 / n_grid)
        own_ref[q] = total[rq:]
        gathered[q, me.core, me.at] = total[:rq]
        here = gathered.at[q, me.core, me.at]
        for _, _, device in me.over_z():
            remote(here, here, send.at[3, q], recv.at[3, q], device).start()

    def back_x(q):
        await_bytes(gathered.at[q, 0, pl.ds(0, nz - 1)], recv.at[3, q])
        here = gathered.at[q, me.core, mine_x]
        for _, _, device in me.over_x():
            remote(here, here, send.at[4, q], recv.at[4, q], device).start()

    def back_core(q):
        await_bytes(gathered.at[q, 0, pl.ds(0, (nx - 1) * nz)], recv.at[4, q])
        here = gathered.at[q, me.core]
        remote(here, here, send.at[5, q], recv.at[5, q], me.other_core()).start()

    def finish(q):
        await_bytes(gathered.at[q, 0], recv.at[5, q])
        for t in range(CORES):
            at = pl.multiple_of(tile_of(me.band, t, q) * BLOCK, BLOCK)
            coeffs_ref[:, pl.ds(at, BLOCK)] = gathered[q, t].reshape(nq, BLOCK)

    multiply(0, (panel_ref[lo, :], panel_ref[hi, :]))
    to_core(0)
    to_x(0)
    to_z(0)
    hops[0].wait_recv()
    hops[4].start()
    hops[1].wait_recv()
    multiply(1, (others[0, lo, :], others[2, lo, :]))
    to_core(1)
    back_z(0)
    to_x(1)
    back_x(0)
    to_z(1)
    hops[3].wait_recv()
    hops[5].start()
    hops[2].wait_recv()
    multiply(2, (others[0, hi, :], others[2, hi, :]))
    to_core(2)
    back_z(1)
    back_core(0)
    to_x(2)
    back_x(1)
    to_z(2)
    hops[4].wait_recv()
    hops[5].wait_recv()
    multiply(3, (others[1, lo, :], others[1, hi, :]))
    to_core(3)
    back_z(2)
    to_x(3)
    back_core(1)
    back_x(2)
    finish(0)
    to_z(3)
    back_core(2)
    finish(1)
    back_z(3)
    finish(2)
    back_x(3)
    back_core(3)
    for h in hops:
        h.wait_send()
    finish(3)
    for q in range(ROUNDS):
        await_bytes(from_core.at[q], send.at[0, q])
        await_bytes(from_x.at[q], send.at[1, q])
        await_bytes(from_z.at[q], send.at[2, q])
        await_bytes(gathered.at[q, 0, pl.ds(0, nz - 1)], send.at[3, q])
        await_bytes(gathered.at[q, 0, pl.ds(0, (nx - 1) * nz)], send.at[4, q])
        await_bytes(gathered.at[q, 0], send.at[5, q])


def reduce_products(nx, nz, n_grid, basis, panel):
    nq, k = basis.shape
    np_ = panel.shape[0]
    pieces = nx * nz
    rq, rp = nq // pieces, np_ // pieces
    f32 = jnp.float32
    return pl.pallas_call(
        functools.partial(reduce_kernel, nx, nz, n_grid),
        out_shape=(
            jax.ShapeDtypeStruct((nq, np_ * BANDS), f32),
            jax.ShapeDtypeStruct((ROUNDS, rp, BLOCK), f32),
        ),
        in_specs=[pl.BlockSpec(memory_space=pltpu.VMEM)] * 2,
        out_specs=(pl.BlockSpec(memory_space=pltpu.VMEM),) * 2,
        scratch_shapes=[
            pltpu.VMEM((BANDS - 1, np_, k), f32),
            pltpu.VMEM((nq + np_, 3 * k), jnp.bfloat16),
            pltpu.VMEM((2 * BLOCK, 3 * k), jnp.bfloat16),
            pltpu.VMEM((ROUNDS, CORES, pieces, rq + rp, BLOCK), f32),
            pltpu.VMEM((ROUNDS, pieces, rq + rp, BLOCK), f32),
            pltpu.VMEM((ROUNDS, nx - 1, nz, rq + rp, BLOCK), f32),
            pltpu.VMEM((ROUNDS, nz - 1, rq + rp, BLOCK), f32),
            pltpu.VMEM((ROUNDS, CORES, pieces, rq, BLOCK), f32),
            pltpu.SemaphoreType.DMA((6,)),
            pltpu.SemaphoreType.DMA((6,)),
            pltpu.SemaphoreType.DMA((6, ROUNDS)),
            pltpu.SemaphoreType.DMA((6, ROUNDS)),
        ],
        compiler_params=pltpu.CompilerParams(
            collective_id=0, has_side_effects=True, vmem_limit_bytes=56 * 1024 * 1024
        ),
        cost_estimate=pl.CostEstimate(
            flops=60 * 1024**3, bytes_accessed=8 * 1024 * 1024, transcendentals=0
        ),
    )(basis, panel)


def gram_kernel(
    nx, nz,
    coeffs_ref, own_ref,
    gram_ref,
    rhs, square, to_y, from_y, gathered,
    send, recv,
):
    me = Place(nx, nz)
    me.barrier()
    nq, n = coeffs_ref.shape
    rp = own_ref.shape[1]
    np_ = n // BANDS
    count = BANDS * rp

    high, low = halves(coeffs_ref[...])
    rhs[:nq, :] = high
    rhs[nq : 2 * nq, :] = low
    rhs[2 * nq :, :] = high
    row = lax.broadcasted_iota(jnp.int32, (count, n), 0)
    col = lax.broadcasted_iota(jnp.int32, (count, n), 1)
    want = lax.div(row, rp) * np_ + lax.rem(row, rp) + me.at * rp
    pick = jnp.where(col == want, 1.0, 0.0).astype(jnp.bfloat16)
    high = dot_nt(pick, rhs[:nq, :]).astype(jnp.bfloat16)
    low = dot_nt(pick, rhs[nq : 2 * nq, :]).astype(jnp.bfloat16)
    square[...] = jnp.dot(
        jnp.concatenate([high, high, low], 1), rhs[...], preferred_element_type=jnp.float32
    )
    for band in range(BANDS):
        for q in range(ROUNDS):
            at = pl.multiple_of(tile_of(band, me.core, q) * BLOCK, BLOCK)
            to_y[band, q] = square[band * rp : (band + 1) * rp, pl.ds(at, BLOCK)]
    for d, band, device in me.over_y():
        remote(to_y.at[band], from_y.at[d], send.at[0], recv.at[0], device).start()
    total = own_ref[...] - to_y[me.band]
    await_bytes(from_y, recv.at[0])
    for d in range(BANDS - 1):
        total = total - from_y[d]
    here = gathered.at[me.core, me.x, me.z, me.band]
    gathered[me.core, me.x, me.z, me.band] = total
    for _, _, device in me.over_y():
        remote(here, here, send.at[1], recv.at[1], device).start()
    await_bytes(from_y, recv.at[1])
    here = gathered.at[me.core, me.x, me.z]
    for _, _, device in me.over_z():
        remote(here, here, send.at[2], recv.at[2], device).start()
    await_bytes(gathered.at[0, 0, pl.ds(0, nz - 1)], recv.at[2])
    here = gathered.at[me.core, me.x]
    for _, _, device in me.over_x():
        remote(here, here, send.at[3], recv.at[3], device).start()
    await_bytes(gathered.at[0, pl.ds(0, nx - 1)], recv.at[3])
    here = gathered.at[me.core]
    remote(here, here, send.at[4], recv.at[4], me.other_core()).start()
    await_bytes(gathered.at[0], recv.at[4])
    for band in range(BANDS):
        for core in range(CORES):
            for q in range(ROUNDS):
                at = int(static_tile(band, core, q)) * BLOCK
                gram_ref[band * np_ : (band + 1) * np_, at : at + BLOCK] = gathered[
                    core, :, :, band, q
                ].reshape(np_, BLOCK)
    await_bytes(from_y, send.at[0])
    await_bytes(from_y, send.at[1])
    await_bytes(gathered.at[0, 0, pl.ds(0, nz - 1)], send.at[2])
    await_bytes(gathered.at[0, pl.ds(0, nx - 1)], send.at[3])
    await_bytes(gathered.at[0], send.at[4])


def static_tile(band, core, turn):
    if turn == 0:
        return 2 * band + core
    if turn == 3:
        return 2 * ((band + 2) % BANDS) + core
    return 2 * ((band + (3 if core else 1)) % BANDS) + turn - 1


def gather_gram(nx, nz, coeffs, own):
    nq, n = coeffs.shape
    rp = own.shape[1]
    f32 = jnp.float32
    return pl.pallas_call(
        functools.partial(gram_kernel, nx, nz),
        out_shape=jax.ShapeDtypeStruct((n, n), f32),
        in_specs=[pl.BlockSpec(memory_space=pltpu.VMEM)] * 2,
        out_specs=pl.BlockSpec(memory_space=pltpu.VMEM),
        scratch_shapes=[
            pltpu.VMEM((3 * nq, n), jnp.bfloat16),
            pltpu.VMEM((BANDS * rp, n), f32),
            pltpu.VMEM((BANDS, ROUNDS, rp, BLOCK), f32),
            pltpu.VMEM((BANDS - 1, ROUNDS, rp, BLOCK), f32),
            pltpu.VMEM((CORES, nx, nz, BANDS, ROUNDS, rp, BLOCK), f32),
            pltpu.SemaphoreType.DMA((5,)),
            pltpu.SemaphoreType.DMA((5,)),
        ],
        compiler_params=pltpu.CompilerParams(
            collective_id=1, has_side_effects=True, vmem_limit_bytes=40 * 1024 * 1024
        ),
        cost_estimate=pl.CostEstimate(
            flops=40 * 1024**3, bytes_accessed=8 * 1024 * 1024, transcendentals=0
        ),
    )(coeffs, own)


def block_inverse(tiles):
    lanes = lax.broadcasted_iota(jnp.int32, (ROWS, BLOCK), 1)
    subs = lax.broadcasted_iota(jnp.int32, (ROWS, BLOCK), 0)
    shape = (ROWS, BLOCK)
    tiles = list(tiles)
    count = len(tiles)
    done = []
    for t in range(count):
        tile = tiles[t]
        base = ROWS * t
        here = (lanes >= base) & (lanes < base + ROWS)
        cols = [jnp.broadcast_to(tile[:, base + q : base + q + 1], shape) for q in range(ROWS)]
        entry = {
            (p, q): jnp.broadcast_to(cols[q][p : p + 1, :], shape)
            for q in range(ROWS)
            for p in range(q, ROWS)
        }
        start = jnp.where(here, jnp.where(lanes - base == subs, 1.0, 0.0), tile)
        rows = [jnp.broadcast_to(start[p : p + 1, :], shape) for p in range(ROWS)]
        unit = {}
        root = []
        scaled = []
        for q in range(ROWS):
            inv_root = lax.rsqrt(entry[q, q])
            inv = inv_root * inv_root
            root.append(inv_root)
            scaled.append(inv)
            for p in range(q + 1, ROWS):
                unit[p, q] = entry[p, q] * inv
            for p in range(q + 1, ROWS):
                for s in range(q + 1, p + 1):
                    entry[p, s] = entry[p, s] - unit[p, q] * entry[s, q]
                rows[p] = rows[p] - unit[p, q] * rows[q]
        out = rows[0] * root[0]
        for p in range(1, ROWS):
            out = jnp.where(subs == p, rows[p] * root[p], out)
        done.append(jnp.where(lanes <= base + subs, out, 0.0))
        if t + 1 < count:
            back = [rows[p] * scaled[p] for p in range(ROWS)]
            for p in range(ROWS - 1, 0, -1):
                for q in range(p):
                    back[q] = back[q] - unit[p, q] * back[p]
            for u in range(t + 1, count):
                old = tiles[u]
                new = jnp.where(here, 0.0, old)
                for p in range(ROWS):
                    new = new - jnp.broadcast_to(old[:, base + p : base + p + 1], shape) * back[p]
                tiles[u] = new
    return done


def factor_kernel(gram_ref, out_ref, diag_ref, right_ref):
    blocks = out_ref.shape[0] // BLOCK
    out_ref[...] = gram_ref[...]

    def step(k, carry):
        at = pl.ds(pl.multiple_of(k * BLOCK, BLOCK), BLOCK)
        base = pl.multiple_of(k * BLOCK, BLOCK)
        tiles = [
            out_ref[pl.ds(base + ROWS * t, ROWS), at] for t in range(BLOCK // ROWS)
        ]
        for t, tile in enumerate(block_inverse(tiles)):
            diag_ref[pl.ds(ROWS * t, ROWS), :] = tile
        diag = diag_ref[...]
        panel = jnp.dot(
            left_parts(diag),
            right_parts(out_ref[at, :], 0),
            preferred_element_type=jnp.float32,
        )
        out_ref[at, :] = panel
        out_ref[at, at] = diag
        right_ref[...] = right_parts(out_ref[at, :], 0)
        diag_right = right_parts(diag, 1)

        def update(i, carry):
            rows = pl.ds(pl.multiple_of(i * BLOCK, BLOCK), BLOCK)
            lower = dot_nt(left_parts(out_ref[rows, at]), diag_right)
            out_ref[rows, at] = jnp.zeros((BLOCK, BLOCK), jnp.float32)
            out_ref[rows, :] -= jnp.dot(
                left_parts(lower), right_ref[...], preferred_element_type=jnp.float32
            )
            return carry

        lax.fori_loop(k + 1, blocks, update, 0)
        return carry

    lax.fori_loop(0, blocks, step, 0)
    row = lax.broadcasted_iota(jnp.int32, (BLOCK, out_ref.shape[1]), 0)
    col = lax.broadcasted_iota(jnp.int32, (BLOCK, out_ref.shape[1]), 1)

    def clear(i, carry):
        rows = pl.ds(pl.multiple_of(i * BLOCK, BLOCK), BLOCK)
        out_ref[rows, :] = jnp.where(col <= row + i * BLOCK, out_ref[rows, :], 0.0)
        return carry

    lax.fori_loop(0, blocks, clear, 0)


def inverse_factor(gram):
    n = gram.shape[0]
    return pl.pallas_call(
        factor_kernel,
        out_shape=jax.ShapeDtypeStruct((n, n), jnp.float32),
        in_specs=[pl.BlockSpec(memory_space=pltpu.VMEM)],
        out_specs=pl.BlockSpec(memory_space=pltpu.VMEM),
        scratch_shapes=[
            pltpu.VMEM((BLOCK, BLOCK), jnp.float32),
            pltpu.VMEM((3 * BLOCK, n), jnp.bfloat16),
        ],
        compiler_params=pltpu.CompilerParams(vmem_limit_bytes=32 * 1024 * 1024),
        cost_estimate=pl.CostEstimate(
            flops=60 * n * n * n, bytes_accessed=8 * n * n, transcendentals=n
        ),
    )(gram)


def swap(x, band, bit):
    return lax.ppermute(x, "band", [(i, i ^ bit) for i in range(band)])


def body(basis, panel):
    grid, band = lax.axis_size("grid"), lax.axis_size("band")
    at_band = lax.axis_index("band")
    n_grid = panel.shape[1] * grid
    rows_p = panel.shape[0]
    nz = grid // (CORES * ALONG_X)
    coeffs, own = reduce_products(ALONG_X, nz, n_grid, basis, panel)
    gram = gather_gram(ALONG_X, nz, coeffs, own)

    bits = [1 << i for i in range(band.bit_length() - 1)]
    odd = at_band % 2

    def removed_rows(which):
        cols = [
            lax.dynamic_slice_in_dim(coeffs, (which + i) * rows_p, rows_p, 1)
            for i in range(0, band, 2)
        ]
        return cdot(jnp.concatenate(cols, 1), basis).reshape(band // 2, rows_p, -1)

    kept = removed_rows(odd) + swap(removed_rows(1 - odd), band, 1)
    for bit in bits[1:]:
        halves_of = kept.reshape(-1, 2, rows_p, kept.shape[-1])
        side = (at_band // bit) % 2
        sent = lax.dynamic_index_in_dim(halves_of, 1 - side, 1, keepdims=False)
        kept = lax.dynamic_index_in_dim(halves_of, side, 1, keepdims=False) + swap(sent, band, bit)
    projected = panel - kept.reshape(panel.shape)
    projected, gram = lax.optimization_barrier((projected, gram))
    others = [projected] + [swap(projected, band, d) for d in range(1, band)]
    inverse = inverse_factor(gram)
    inverse_rows = lax.dynamic_slice_in_dim(inverse, at_band * rows_p, rows_p, 0)
    new_panel = 0.0
    for d, rows in enumerate(others):
        cols = lax.dynamic_slice_in_dim(inverse_rows, (at_band ^ d) * rows_p, rows_p, 1)
        new_panel = new_panel + jnp.dot(cols, rows, precision=lax.Precision.HIGH)
    return (new_panel, coeffs)


def solution(mesh):
    placed = (P("band", "grid"), P("band", "grid"))
    return jax.shard_map(
        body,
        mesh=mesh,
        in_specs=placed,
        out_specs=(P("band", "grid"), P("band", None)),
        check_vma=False,
    )
```

```python
import functools

import jax
import jax.numpy as jnp
from jax import lax
from jax.experimental import pallas as pl
from jax.experimental.pallas import tpu as pltpu
from jax.sharding import PartitionSpec as P

BLOCK = 128
ROWS = 8
CORES = 2
BANDS = 4
ROUNDS = 4
KEPT = 3
ALONG_X = 4
MESH = pl.DeviceIdType.MESH


def halves(x):
    high = x.astype(jnp.bfloat16)
    low = (x - high.astype(jnp.float32)).astype(jnp.bfloat16)
    return high, low


def left_parts(x):
    high, low = halves(x)
    return jnp.concatenate([high, high, low], 1)


def right_parts(x, axis):
    high, low = halves(x)
    return jnp.concatenate([high, low, high], axis)


def dot_nt(left, right):
    return lax.dot_general(
        left, right, (((1,), (1,)), ((), ())), preferred_element_type=jnp.float32
    )


def tile_of(band, core, turn):
    one, two, three = (lax.rem(band + i, BANDS) for i in (1, 2, 3))
    if turn == 0:
        return 2 * band + core
    if turn == 1:
        return 2 * (one + core * (three - one))
    if turn == 2:
        return 2 * (three + core * (one - three)) + 1
    return 2 * two + core


class Place:
    def __init__(self, nx, nz):
        self.nx, self.nz = nx, nz
        self.grid = lax.axis_index("grid")
        self.band = lax.axis_index("band")
        self.core = lax.rem(self.grid, CORES)
        self.x = lax.rem(lax.div(self.grid, CORES), nx)
        self.z = lax.div(self.grid, CORES * nx)
        self.at = self.x * nz + self.z

    def id(self, z, x, core):
        return {"grid": (z * self.nx + x) * CORES + core, "band": self.band}

    def other_core(self):
        return self.id(self.z, self.x, 1 - self.core)

    def over_x(self):
        for d in range(1, self.nx):
            x = lax.rem(self.x + d, self.nx)
            yield d - 1, x, self.id(self.z, x, self.core)

    def over_z(self):
        for d in range(1, self.nz):
            z = lax.rem(self.z + d, self.nz)
            yield d - 1, z, self.id(z, self.x, self.core)

    def over_y(self):
        for d in range(1, BANDS):
            band = lax.rem(self.band + d, BANDS)
            yield d - 1, band, {"grid": self.grid, "band": band}

    def barrier(self):
        sem = pltpu.get_barrier_semaphore()
        ids = [self.other_core()]
        ids += [i for _, _, i in self.over_x()]
        ids += [i for _, _, i in self.over_z()]
        ids += [i for _, _, i in self.over_y()]
        for i in ids:
            pl.semaphore_signal(sem, inc=1, device_id=i, device_id_type=MESH)
        pl.semaphore_wait(sem, len(ids))


def remote(src, dst, send, recv, device):
    return pltpu.make_async_remote_copy(
        src_ref=src,
        dst_ref=dst,
        send_sem=send,
        recv_sem=recv,
        device_id=device,
        device_id_type=MESH,
    )


def await_bytes(ref, sem):
    pltpu.make_async_copy(ref, ref, sem).wait()


def gather_kernel(
    nx, nz, n_grid,
    basis_ref, panel_ref,
    coeffs_ref, gram_ref, projected_ref,
    others, lhs, rhs, part, from_core, from_x, from_z, gathered, own,
    removed, from_band, stacked, share, pieces_of,
    y_send, y_recv, send, recv, b_send, b_recv, g_send, z_recv, x_recv, g_recv,
):
    me = Place(nx, nz)
    me.barrier()
    nq, k = basis_ref.shape
    np_ = panel_ref.shape[0]
    pieces = nx * nz
    rq, rp = nq // pieces, np_ // pieces
    half = np_ // 2
    lo, hi = pl.ds(0, half), pl.ds(half, half)
    right = {"grid": me.grid, "band": lax.rem(me.band + 1, BANDS)}
    left = {"grid": me.grid, "band": lax.rem(me.band + BANDS - 1, BANDS)}

    def hop(i, src, dst, device):
        return remote(src, dst, y_send.at[i], y_recv.at[i], device)

    hops = [
        hop(0, panel_ref.at[lo], others.at[2, lo], right),
        hop(1, panel_ref.at[lo], others.at[0, lo], left),
        hop(2, panel_ref.at[hi], others.at[2, hi], right),
        hop(3, panel_ref.at[hi], others.at[0, hi], left),
        hop(4, others.at[2, lo], others.at[1, lo], right),
        hop(5, others.at[0, hi], others.at[1, hi], left),
    ]
    for h in hops[:4]:
        h.start()

    high, low = halves(basis_ref[...])
    lhs[:nq, :k] = high
    lhs[:nq, k : 2 * k] = high
    lhs[:nq, 2 * k :] = low
    high, low = halves(panel_ref[...])
    lhs[nq:, :k] = high
    lhs[nq:, k : 2 * k] = high
    lhs[nq:, 2 * k :] = low

    def multiply(q, tiles):
        for t, tile in enumerate(tiles):
            rows = slice(t * BLOCK, (t + 1) * BLOCK)
            high, low = halves(tile)
            rhs[rows, :k] = high
            rhs[rows, k : 2 * k] = low
            rhs[rows, 2 * k :] = high
        out = dot_nt(lhs[:nq, :], rhs[...])
        for t in range(2):
            part[q, t, :, :rq, :] = out[:, t * BLOCK : (t + 1) * BLOCK].reshape(pieces, rq, BLOCK)
        out = dot_nt(lhs[nq:, :], rhs[...])
        for t in range(2):
            part[q, t, :, rq:, :] = out[:, t * BLOCK : (t + 1) * BLOCK].reshape(pieces, rp, BLOCK)

    mine_x = pl.ds(me.x * nz, nz)

    def to_core(q):
        remote(
            part.at[q, 1 - me.core], from_core.at[q], send.at[0, q], recv.at[0, q], me.other_core()
        ).start()

    def to_x(q):
        await_bytes(from_core.at[q], recv.at[0, q])
        part[q, me.core] += from_core[q]
        for d, x, device in me.over_x():
            remote(
                part.at[q, me.core, pl.ds(x * nz, nz)],
                from_x.at[q, d],
                send.at[1, q],
                recv.at[1, q],
                device,
            ).start()

    def to_z(q):
        await_bytes(from_x.at[q], recv.at[1, q])
        total = part[q, me.core, mine_x]
        for d in range(nx - 1):
            total = total + from_x[q, d]
        part[q, me.core, mine_x] = total
        for d, z, device in me.over_z():
            remote(
                part.at[q, me.core, me.x * nz + z],
                from_z.at[q, d],
                send.at[2, q],
                recv.at[2, q],
                device,
            ).start()

    def back_z(q):
        await_bytes(from_z.at[q], recv.at[2, q])
        total = part[q, me.core, me.at]
        for d in range(nz - 1):
            total = total + from_z[q, d]
        total = total * (1.0 / n_grid)
        own[q] = total[rq:]
        gathered[q, me.core, me.at] = total[:rq]
        here = gathered.at[q, me.core, me.at]
        for _, _, device in me.over_z():
            remote(here, here, send.at[3, q], recv.at[3, q], device).start()

    def back_x(q):
        await_bytes(gathered.at[q, 0, pl.ds(0, nz - 1)], recv.at[3, q])
        here = gathered.at[q, me.core, mine_x]
        for _, _, device in me.over_x():
            remote(here, here, send.at[4, q], recv.at[4, q], device).start()

    def back_core(q):
        await_bytes(gathered.at[q, 0, pl.ds(0, (nx - 1) * nz)], recv.at[4, q])
        here = gathered.at[q, me.core]
        remote(here, here, send.at[5, q], recv.at[5, q], me.other_core()).start()

    def finish(q):
        await_bytes(gathered.at[q, 0], recv.at[5, q])
        for t in range(CORES):
            at = pl.multiple_of(tile_of(me.band, t, q) * BLOCK, BLOCK)
            coeffs_ref[:, pl.ds(at, BLOCK)] = gathered[q, t].reshape(nq, BLOCK)

    def remove(q):
        parts = [halves(gathered[q, t].reshape(nq, BLOCK).T) for t in range(CORES)]
        high = jnp.concatenate([p[0] for p in parts], 0)
        both = jnp.concatenate([high] + [p[1] for p in parts], 0)
        out = jnp.dot(both, lhs[:nq, :k], preferred_element_type=jnp.float32)
        out = out[: 2 * BLOCK] + out[2 * BLOCK :]
        out = out + jnp.dot(high, lhs[:nq, 2 * k :], preferred_element_type=jnp.float32)
        removed[q] = out.reshape(CORES, BLOCK, k)

    across = {"grid": me.grid, "band": lax.rem(me.band + 2, BANDS)}

    def bulk(i, src, dst, device):
        return remote(src, dst, b_send.at[i], b_recv.at[i], device)

    bulks = [
        bulk(0, removed.at[1, 0], from_band.at[0, 0], right),
        bulk(1, removed.at[1, 1], from_band.at[2, 0], left),
        bulk(2, removed.at[2, 0], from_band.at[2, 1], left),
        bulk(3, removed.at[2, 1], from_band.at[0, 1], right),
        bulk(4, removed.at[3], from_band.at[1], across),
    ]

    multiply(0, (panel_ref[lo, :], panel_ref[hi, :]))
    to_core(0)
    to_x(0)
    to_z(0)
    hops[0].wait_recv()
    hops[4].start()
    hops[1].wait_recv()
    multiply(1, (others[0, lo, :], others[2, lo, :]))
    to_core(1)
    back_z(0)
    to_x(1)
    back_x(0)
    to_z(1)
    hops[3].wait_recv()
    hops[5].start()
    hops[2].wait_recv()
    multiply(2, (others[2, hi, :], others[0, hi, :]))
    to_core(2)
    back_z(1)
    back_core(0)
    to_x(2)
    back_x(1)
    to_z(2)
    hops[4].wait_recv()
    hops[5].wait_recv()
    multiply(3, (others[1, lo, :], others[1, hi, :]))
    to_core(3)
    back_z(2)
    to_x(3)
    back_core(1)
    back_x(2)
    finish(0)
    to_z(3)
    back_core(2)
    finish(1)
    remove(1)
    bulks[0].start()
    bulks[1].start()
    back_z(3)
    finish(2)
    remove(2)
    back_x(3)
    remove(0)
    back_core(3)
    for h in hops:
        h.wait_send()
    finish(3)

    high, low = halves(coeffs_ref[...])
    stacked[:nq, :] = high
    stacked[nq : 2 * nq, :] = low
    stacked[2 * nq :, :] = high
    n = coeffs_ref.shape[1]
    count = BANDS * rp
    row = lax.broadcasted_iota(jnp.int32, (count, n), 0)
    col = lax.broadcasted_iota(jnp.int32, (count, n), 1)
    want = lax.div(row, rp) * np_ + lax.rem(row, rp) + me.at * rp
    pick = jnp.where(col == want, 1.0, 0.0).astype(jnp.bfloat16)
    high = dot_nt(pick, stacked[:nq, :]).astype(jnp.bfloat16)
    low = dot_nt(pick, stacked[nq : 2 * nq, :]).astype(jnp.bfloat16)
    square = jnp.dot(
        jnp.concatenate([high, high, low], 1), stacked[...], preferred_element_type=jnp.float32
    )
    for band in range(BANDS):
        rows = square[band * rp : (band + 1) * rp]
        for i in range(KEPT):
            first = 2 * ((band + i) % BANDS) * BLOCK
            pair = [rows[:, first + t * BLOCK : first + (t + 1) * BLOCK] for t in range(CORES)]
            share[me.band, band, i] = -jnp.where(me.core == 0, pair[0], pair[1])
    for i, q in enumerate((0, 1 + me.core, ROUNDS - 1)):
        share[me.band, me.band, i] += own[q]
    for _, _, device in me.over_y():
        remote(share.at[me.band], share.at[me.band], g_send.at[0], g_recv.at[0], device).start()
    bulks[2].start()
    bulks[3].start()
    remove(3)
    bulks[4].start()
    await_bytes(share.at[pl.ds(0, BANDS - 1)], g_recv.at[0])
    pieces_of[me.core, me.x, me.z] = (share[0] + share[1]) + (share[2] + share[3])

    up, down = lax.rem(me.x + 1, nx), lax.rem(me.x + nx - 1, nx)
    to_up, to_down = me.id(me.z, up, me.core), me.id(me.z, down, me.core)
    first, second = pl.ds(0, BANDS // 2), pl.ds(BANDS // 2, BANDS // 2)

    def spread(i, z):
        here = pieces_of.at[me.core, me.x, z]
        remote(here, here, g_send.at[2], x_recv.at[0, i], to_up).start()
        remote(here, here, g_send.at[2], x_recv.at[1, i], to_down).start()

    def relay(i, z):
        await_bytes(pieces_of.at[0, 0, 0], x_recv.at[0, i])
        here = pieces_of.at[me.core, down, z, first]
        remote(here, here, g_send.at[3], g_recv.at[1], to_up).start()
        await_bytes(pieces_of.at[0, 0, 0], x_recv.at[1, i])
        here = pieces_of.at[me.core, up, z, second]
        remote(here, here, g_send.at[3], g_recv.at[1], to_down).start()

    def cross(x):
        here = pieces_of.at[me.core, x]
        remote(here, here, g_send.at[4], g_recv.at[2], me.other_core()).start()

    here = pieces_of.at[me.core, me.x, me.z]
    for d, _, device in me.over_z():
        remote(here, here, g_send.at[1], z_recv.at[d], device).start()
    spread(0, me.z)
    order = [me.z]
    for i, d in enumerate(sorted(range(1, nz), key=lambda d: min(d, nz - d))):
        z = lax.rem(me.z + nz - d, nz)
        await_bytes(pieces_of.at[0, 0, 0], z_recv.at[d - 1])
        spread(i + 1, z)
        relay(i, order[i])
        order.append(z)
    cross(me.x)
    relay(nz - 1, order[nz - 1])
    cross(up)
    cross(down)
    await_bytes(pieces_of.at[0, 0], g_recv.at[1])
    cross(lax.rem(me.x + 2, nx))

    def place(core):
        for band in range(BANDS):
            for i in range(KEPT):
                at = (2 * ((band + i) % BANDS) + core) * BLOCK
                tile = pieces_of[core, :, :, band, i].reshape(np_, BLOCK)
                gram_ref[band * np_ : (band + 1) * np_, at : at + BLOCK] = tile
                if i == 1:
                    to = (2 * ((band + i) % BANDS) + core) * BLOCK
                    gram_ref[to : to + BLOCK, band * np_ : (band + 1) * np_] = tile.T

    await_bytes(pieces_of.at[0], g_recv.at[2])
    place(0)
    place(1)
    for h in bulks:
        h.wait_recv()
    for t in range(CORES):
        rows = slice(t * BLOCK, (t + 1) * BLOCK)
        total = removed[0, t]
        for d in range(BANDS - 1):
            total = total + from_band[d, t]
        projected_ref[rows, :] = panel_ref[rows, :] - total

    for h in bulks:
        h.wait_send()
    for q in range(ROUNDS):
        await_bytes(from_core.at[q], send.at[0, q])
        await_bytes(from_x.at[q], send.at[1, q])
        await_bytes(from_z.at[q], send.at[2, q])
        await_bytes(gathered.at[q, 0, pl.ds(0, nz - 1)], send.at[3, q])
        await_bytes(gathered.at[q, 0, pl.ds(0, (nx - 1) * nz)], send.at[4, q])
        await_bytes(gathered.at[q, 0], send.at[5, q])
    await_bytes(share.at[pl.ds(0, BANDS - 1)], g_send.at[0])
    await_bytes(pieces_of.at[0, 0, pl.ds(0, nz - 1)], g_send.at[1])
    await_bytes(pieces_of.at[0, pl.ds(0, 2)], g_send.at[2])
    await_bytes(pieces_of.at[0, 0], g_send.at[3])
    await_bytes(pieces_of.at[0], g_send.at[4])


def reduce_and_project(nx, nz, n_grid, basis, panel):
    nq, k = basis.shape
    np_ = panel.shape[0]
    n = np_ * BANDS
    pieces = nx * nz
    rq, rp = nq // pieces, np_ // pieces
    f32 = jnp.float32
    dma = pltpu.SemaphoreType.DMA
    return pl.pallas_call(
        functools.partial(gather_kernel, nx, nz, n_grid),
        out_shape=(
            jax.ShapeDtypeStruct((nq, n), f32),
            jax.ShapeDtypeStruct((n, n), f32),
            jax.ShapeDtypeStruct((np_, k), f32),
        ),
        in_specs=[pl.BlockSpec(memory_space=pltpu.VMEM)] * 2,
        out_specs=(pl.BlockSpec(memory_space=pltpu.VMEM),) * 3,
        scratch_shapes=[
            pltpu.VMEM((BANDS - 1, np_, k), f32),
            pltpu.VMEM((nq + np_, 3 * k), jnp.bfloat16),
            pltpu.VMEM((2 * BLOCK, 3 * k), jnp.bfloat16),
            pltpu.VMEM((ROUNDS, CORES, pieces, rq + rp, BLOCK), f32),
            pltpu.VMEM((ROUNDS, pieces, rq + rp, BLOCK), f32),
            pltpu.VMEM((ROUNDS, nx - 1, nz, rq + rp, BLOCK), f32),
            pltpu.VMEM((ROUNDS, nz - 1, rq + rp, BLOCK), f32),
            pltpu.VMEM((ROUNDS, CORES, pieces, rq, BLOCK), f32),
            pltpu.VMEM((ROUNDS, rp, BLOCK), f32),
            pltpu.VMEM((ROUNDS, CORES, BLOCK, k), f32),
            pltpu.VMEM((BANDS - 1, CORES, BLOCK, k), f32),
            pltpu.VMEM((3 * nq, n), jnp.bfloat16),
            pltpu.VMEM((BANDS, BANDS, KEPT, rp, BLOCK), f32),
            pltpu.VMEM((CORES, nx, nz, BANDS, KEPT, rp, BLOCK), f32),
            dma((6,)),
            dma((6,)),
            dma((6, ROUNDS)),
            dma((6, ROUNDS)),
            dma((5,)),
            dma((5,)),
            dma((5,)),
            dma((nz - 1,)),
            dma((2, nz)),
            dma((3,)),
        ],
        compiler_params=pltpu.CompilerParams(
            collective_id=0, has_side_effects=True, vmem_limit_bytes=58 * 1024 * 1024
        ),
        cost_estimate=pl.CostEstimate(
            flops=60 * 1024**3, bytes_accessed=8 * 1024 * 1024, transcendentals=0
        ),
    )(basis, panel)


def block_inverse(tiles):
    lanes = lax.broadcasted_iota(jnp.int32, (ROWS, BLOCK), 1)
    subs = lax.broadcasted_iota(jnp.int32, (ROWS, BLOCK), 0)
    shape = (ROWS, BLOCK)
    tiles = list(tiles)
    count = len(tiles)
    done = []
    for t in range(count):
        tile = tiles[t]
        base = ROWS * t
        here = (lanes >= base) & (lanes < base + ROWS)
        cols = [jnp.broadcast_to(tile[:, base + q : base + q + 1], shape) for q in range(ROWS)]
        entry = {
            (p, q): jnp.broadcast_to(cols[q][p : p + 1, :], shape)
            for q in range(ROWS)
            for p in range(q, ROWS)
        }
        start = jnp.where(here, jnp.where(lanes - base == subs, 1.0, 0.0), tile)
        rows = [jnp.broadcast_to(start[p : p + 1, :], shape) for p in range(ROWS)]
        unit = {}
        root = []
        scaled = []
        for q in range(ROWS):
            inv_root = lax.rsqrt(entry[q, q])
            inv = inv_root * inv_root
            root.append(inv_root)
            scaled.append(inv)
            for p in range(q + 1, ROWS):
                unit[p, q] = entry[p, q] * inv
            for p in range(q + 1, ROWS):
                for s in range(q + 1, p + 1):
                    entry[p, s] = entry[p, s] - unit[p, q] * entry[s, q]
                rows[p] = rows[p] - unit[p, q] * rows[q]
        out = rows[0] * root[0]
        for p in range(1, ROWS):
            out = jnp.where(subs == p, rows[p] * root[p], out)
        done.append(jnp.where(lanes <= base + subs, out, 0.0))
        if t + 1 < count:
            back = [rows[p] * scaled[p] for p in range(ROWS)]
            for p in range(ROWS - 1, 0, -1):
                for q in range(p):
                    back[q] = back[q] - unit[p, q] * back[p]
            for u in range(t + 1, count):
                old = tiles[u]
                new = jnp.where(here, 0.0, old)
                for p in range(ROWS):
                    new = new - jnp.broadcast_to(old[:, base + p : base + p + 1], shape) * back[p]
                tiles[u] = new
    return done


def factor_kernel(gram_ref, out_ref, diag_ref, right_ref):
    blocks = out_ref.shape[0] // BLOCK
    out_ref[...] = gram_ref[...]

    def step(k, carry):
        at = pl.ds(pl.multiple_of(k * BLOCK, BLOCK), BLOCK)
        base = pl.multiple_of(k * BLOCK, BLOCK)
        tiles = [
            out_ref[pl.ds(base + ROWS * t, ROWS), at] for t in range(BLOCK // ROWS)
        ]
        for t, tile in enumerate(block_inverse(tiles)):
            diag_ref[pl.ds(ROWS * t, ROWS), :] = tile
        diag = diag_ref[...]
        panel = jnp.dot(
            left_parts(diag),
            right_parts(out_ref[at, :], 0),
            preferred_element_type=jnp.float32,
        )
        out_ref[at, :] = panel
        out_ref[at, at] = diag
        right_ref[...] = right_parts(out_ref[at, :], 0)
        diag_right = right_parts(diag, 1)

        def update(i, carry):
            rows = pl.ds(pl.multiple_of(i * BLOCK, BLOCK), BLOCK)
            lower = dot_nt(left_parts(out_ref[rows, at]), diag_right)
            out_ref[rows, at] = jnp.zeros((BLOCK, BLOCK), jnp.float32)
            out_ref[rows, :] -= jnp.dot(
                left_parts(lower), right_ref[...], preferred_element_type=jnp.float32
            )
            return carry

        lax.fori_loop(k + 1, blocks, update, 0)
        return carry

    lax.fori_loop(0, blocks, step, 0)
    row = lax.broadcasted_iota(jnp.int32, (BLOCK, out_ref.shape[1]), 0)
    col = lax.broadcasted_iota(jnp.int32, (BLOCK, out_ref.shape[1]), 1)

    def clear(i, carry):
        rows = pl.ds(pl.multiple_of(i * BLOCK, BLOCK), BLOCK)
        out_ref[rows, :] = jnp.where(col <= row + i * BLOCK, out_ref[rows, :], 0.0)
        return carry

    lax.fori_loop(0, blocks, clear, 0)


def inverse_factor(gram):
    n = gram.shape[0]
    return pl.pallas_call(
        factor_kernel,
        out_shape=jax.ShapeDtypeStruct((n, n), jnp.float32),
        in_specs=[pl.BlockSpec(memory_space=pltpu.VMEM)],
        out_specs=pl.BlockSpec(memory_space=pltpu.VMEM),
        scratch_shapes=[
            pltpu.VMEM((BLOCK, BLOCK), jnp.float32),
            pltpu.VMEM((3 * BLOCK, n), jnp.bfloat16),
        ],
        compiler_params=pltpu.CompilerParams(vmem_limit_bytes=32 * 1024 * 1024),
        cost_estimate=pl.CostEstimate(
            flops=60 * n * n * n, bytes_accessed=8 * n * n, transcendentals=n
        ),
    )(gram)


def swap(x, band, bit):
    return lax.ppermute(x, "band", [(i, i ^ bit) for i in range(band)])


def body(basis, panel):
    grid, band = lax.axis_size("grid"), lax.axis_size("band")
    at_band = lax.axis_index("band")
    n_grid = panel.shape[1] * grid
    rows_p = panel.shape[0]
    nz = grid // (CORES * ALONG_X)
    coeffs, gram, projected = reduce_and_project(ALONG_X, nz, n_grid, basis, panel)
    projected, gram = lax.optimization_barrier((projected, gram))
    others = [projected] + [swap(projected, band, d) for d in range(1, band)]
    inverse = inverse_factor(gram)
    inverse_rows = lax.dynamic_slice_in_dim(inverse, at_band * rows_p, rows_p, 0)
    new_panel = 0.0
    for d, rows in enumerate(others):
        cols = lax.dynamic_slice_in_dim(inverse_rows, (at_band ^ d) * rows_p, rows_p, 1)
        new_panel = new_panel + jnp.dot(cols, rows, precision=lax.Precision.HIGH)
    return (new_panel, coeffs)


def solution(mesh):
    placed = (P("band", "grid"), P("band", "grid"))
    return jax.shard_map(
        body,
        mesh=mesh,
        in_specs=placed,
        out_specs=(P("band", "grid"), P("band", None)),
        check_vma=False,
    )
```

```python
import functools

import jax
import jax.numpy as jnp
from jax import lax
from jax.experimental import pallas as pl
from jax.experimental.pallas import tpu as pltpu
from jax.sharding import PartitionSpec as P

BLOCK = 128
ROWS = 8
CORES = 2
BANDS = 4
ROUNDS = 4
KEPT = 3
GROUP = 4
MIDWAY = 5
ALONG_X = 4
MESH = pl.DeviceIdType.MESH


def halves(x):
    high = x.astype(jnp.bfloat16)
    low = (x - high.astype(jnp.float32)).astype(jnp.bfloat16)
    return high, low


def left_parts(x):
    high, low = halves(x)
    return jnp.concatenate([high, high, low], 1)


def right_parts(x, axis):
    high, low = halves(x)
    return jnp.concatenate([high, low, high], axis)


def dot_nt(left, right):
    return lax.dot_general(
        left, right, (((1,), (1,)), ((), ())), preferred_element_type=jnp.float32
    )


def tile_of(band, core, turn):
    one, two, three = (lax.rem(band + i, BANDS) for i in (1, 2, 3))
    if turn == 0:
        return 2 * band + core
    if turn == 1:
        return 2 * (one + core * (three - one))
    if turn == 2:
        return 2 * (three + core * (one - three)) + 1
    return 2 * two + core


class Place:
    def __init__(self, nx, nz):
        self.nx, self.nz = nx, nz
        self.grid = lax.axis_index("grid")
        self.band = lax.axis_index("band")
        self.core = lax.rem(self.grid, CORES)
        self.x = lax.rem(lax.div(self.grid, CORES), nx)
        self.z = lax.div(self.grid, CORES * nx)
        self.at = self.x * nz + self.z

    def id(self, z, x, core):
        return {"grid": (z * self.nx + x) * CORES + core, "band": self.band}

    def other_core(self):
        return self.id(self.z, self.x, 1 - self.core)

    def over_x(self):
        for d in range(1, self.nx):
            x = lax.rem(self.x + d, self.nx)
            yield d - 1, x, self.id(self.z, x, self.core)

    def over_z(self):
        for d in range(1, self.nz):
            z = lax.rem(self.z + d, self.nz)
            yield d - 1, z, self.id(z, self.x, self.core)

    def over_y(self):
        for d in range(1, BANDS):
            band = lax.rem(self.band + d, BANDS)
            yield d - 1, band, {"grid": self.grid, "band": band}

    def barrier(self):
        sem = pltpu.get_barrier_semaphore()
        ids = [self.other_core()]
        ids += [i for _, _, i in self.over_x()]
        ids += [i for _, _, i in self.over_z()]
        ids += [i for _, _, i in self.over_y()]
        for i in ids:
            pl.semaphore_signal(sem, inc=1, device_id=i, device_id_type=MESH)
        pl.semaphore_wait(sem, len(ids))


def remote(src, dst, send, recv, device):
    return pltpu.make_async_remote_copy(
        src_ref=src,
        dst_ref=dst,
        send_sem=send,
        recv_sem=recv,
        device_id=device,
        device_id_type=MESH,
    )


def await_bytes(ref, sem):
    pltpu.make_async_copy(ref, ref, sem).wait()


def across_lanes(tile, lane):
    return jnp.broadcast_to(tile[:, lane : lane + 1], (ROWS, BLOCK))


def down_rows(tile, row):
    return jnp.broadcast_to(tile[row : row + 1, :], (ROWS, BLOCK))


def block_inverse(tiles):
    lanes = lax.broadcasted_iota(jnp.int32, (ROWS, BLOCK), 1)
    subs = lax.broadcasted_iota(jnp.int32, (ROWS, BLOCK), 0)
    tiles = list(tiles)
    count = len(tiles)
    done = []
    outs = []
    square = [across_lanes(tiles[0], q) for q in range(ROWS)]
    for t in range(count):
        base = ROWS * t
        here = (lanes >= base) & (lanes < base + ROWS)
        more = t + 1 < count
        if more:
            ahead = tiles[t + 1]
            side = [across_lanes(ahead, base + q) for q in range(ROWS)]
            following = [across_lanes(ahead, base + ROWS + q) for q in range(ROWS)]
        far = t + 2 < min(count, (t // GROUP + 1) * GROUP + 1)
        if far:
            beyond = tiles[t + 2]
            wing = [across_lanes(beyond, base + q) for q in range(ROWS)]
        current = jnp.where(here, jnp.where(lanes - base == subs, 1.0, 0.0), tiles[t])
        rows, scaled, unit = [], [], {}
        out = None
        for q in range(ROWS):
            root = lax.rsqrt(down_rows(square[q], q))
            inv = root * root
            scaled.append(inv)
            row = down_rows(current, q)
            rows.append(row)
            out = row * root if q == 0 else jnp.where(subs == q, row * root, out)
            if q + 1 < ROWS:
                current = current - (square[q] * inv) * row
            for s in range(q + 1, ROWS):
                unit[s, q] = down_rows(square[q], s) * inv
                square[s] = square[s] - unit[s, q] * square[q]
            if far:
                for s in range(q + 1, ROWS):
                    wing[s] = wing[s] - unit[s, q] * wing[q]
                beyond = (jnp.where(here, 0.0, beyond) if q == 0 else beyond) - (wing[q] * inv) * row
            if more:
                weight = side[q] * inv
                for s in range(q + 1, ROWS):
                    side[s] = side[s] - unit[s, q] * side[q]
                for s in range(ROWS):
                    following[s] = following[s] - weight * down_rows(side[q], s)
                ahead = (jnp.where(here, 0.0, ahead) if q == 0 else ahead) - weight * row
        if far:
            tiles[t + 2] = beyond
        done.append(jnp.where(lanes <= base + subs, out, 0.0))
        ends = (t // GROUP + 1) * GROUP * ROWS
        outs.append((out, jnp.where((lanes < base + ROWS) | (lanes >= ends), out, 0.0)))
        if more:
            square = following
            tiles[t + 1] = ahead
        if t + 3 < min(count, (t // GROUP + 1) * GROUP + 1):
            back = [rows[p] * scaled[p] for p in range(ROWS)]
            for p in range(ROWS - 1, 0, -1):
                for q in range(p):
                    back[q] = back[q] - unit[p, q] * back[p]
            for u in range(t + 3, min(count, (t // GROUP + 1) * GROUP + 1)):
                old = tiles[u]
                new = jnp.where(here, 0.0, old)
                for p in range(ROWS):
                    new = new - across_lanes(old, base + p) * back[p]
                tiles[u] = new
        first = t + 1 + 1
        if (t + 1) % GROUP == 0 and first < count:
            high, low = halves(jnp.concatenate([o[0] for o in outs[t + 1 - GROUP :]], 0))
            rhigh, rlow = halves(jnp.concatenate([o[1] for o in outs[t + 1 - GROUP :]], 0))
            change = lax.dot_general(
                jnp.concatenate([high, high, low], 0),
                jnp.concatenate([rhigh, rlow, rhigh], 0),
                (((0,), (0,)), ((), ())),
                preferred_element_type=jnp.float32,
            )
            group = (lanes >= base + ROWS - GROUP * ROWS) & (lanes < base + ROWS)
            for u in range(first, count):
                tiles[u] = jnp.where(group, 0.0, tiles[u]) - change[u * ROWS : (u + 1) * ROWS]
    return done


def factor_steps(a_ref, diag_ref, diag_right, lower_ref, right_ref, midway):
    n = a_ref.shape[0]
    blocks = n // BLOCK
    wide = 2 * BLOCK
    diag_right[...] = jnp.zeros_like(diag_right)
    right_ref[...] = jnp.zeros_like(right_ref)

    def step(k, carry):
        pl.when(k == MIDWAY)(midway)
        at = pl.ds(pl.multiple_of(k * BLOCK, BLOCK), BLOCK)
        before = pl.ds(pl.multiple_of(jnp.maximum(k - 1, 0) * BLOCK, BLOCK), BLOCK)
        after = pl.ds(pl.multiple_of(jnp.minimum(k + 1, blocks - 1) * BLOCK, BLOCK), BLOCK)
        base = pl.multiple_of(k * BLOCK, BLOCK)
        tiles = [a_ref[pl.ds(base + ROWS * t, ROWS), at] for t in range(BLOCK // ROWS)]

        for j in range(2, blocks):
            rows = slice(j * BLOCK, (j + 1) * BLOCK)
            on = jnp.where((j > k) & (k > 0), 1.0, 0.0).astype(jnp.float32)
            old = a_ref[rows, before]
            lower_ref[rows, :] = left_parts(dot_nt(left_parts(old), diag_right[...]) * on)
            a_ref[rows, before] = old * (1.0 - on)
        for c in range(n // wide):
            cols = slice(c * wide, (c + 1) * wide)
            for j in range(1, blocks // 2):
                rows = slice(j * wide, (j + 1) * wide)
                a_ref[rows, cols] -= jnp.dot(
                    lower_ref[rows, :], right_ref[:, cols], preferred_element_type=jnp.float32
                )
        for t, tile in enumerate(block_inverse(tiles)):
            diag_ref[ROWS * t : ROWS * (t + 1), :] = tile

        diag = diag_ref[...]
        a_ref[at, :] = jnp.dot(
            left_parts(diag), right_parts(a_ref[at, :], 0), preferred_element_type=jnp.float32
        )
        a_ref[at, at] = diag
        right_ref[...] = right_parts(a_ref[at, :], 0)
        diag_right[...] = right_parts(diag, 1)
        on = jnp.where(k < blocks - 1, 1.0, 0.0).astype(jnp.float32)
        old = a_ref[after, at]
        low = dot_nt(left_parts(old), diag_right[...]) * on
        a_ref[after, at] = old * (1.0 - on)
        a_ref[after, :] -= jnp.dot(left_parts(low), right_ref[...], preferred_element_type=jnp.float32)
        return carry

    lax.fori_loop(0, blocks, step, 0)


def gather_kernel(
    nx, nz, n_grid,
    basis_ref, panel_ref,
    coeffs_ref, panel_out_ref,
    others, lhs, rhs, part, from_core, from_x, from_z, gathered, own,
    removed, from_band, stacked, share, pieces_of,
    gram_ref, diag, diag_right, lower, right_parts_of, projected, projected_others,
    y_send, y_recv, send, recv, b_send, b_recv, g_send, z_recv, x_recv, g_recv, p_send, p_recv,
):
    me = Place(nx, nz)
    me.barrier()
    nq, k = basis_ref.shape
    np_ = panel_ref.shape[0]
    pieces = nx * nz
    rq, rp = nq // pieces, np_ // pieces
    half = np_ // 2
    lo, hi = pl.ds(0, half), pl.ds(half, half)
    right = {"grid": me.grid, "band": lax.rem(me.band + 1, BANDS)}
    left = {"grid": me.grid, "band": lax.rem(me.band + BANDS - 1, BANDS)}

    def hop(i, src, dst, device):
        return remote(src, dst, y_send.at[i], y_recv.at[i], device)

    hops = [
        hop(0, panel_ref.at[lo], others.at[2, lo], right),
        hop(1, panel_ref.at[lo], others.at[0, lo], left),
        hop(2, panel_ref.at[hi], others.at[2, hi], right),
        hop(3, panel_ref.at[hi], others.at[0, hi], left),
        hop(4, others.at[2, lo], others.at[1, lo], right),
        hop(5, others.at[0, hi], others.at[1, hi], left),
    ]
    for h in hops[:4]:
        h.start()

    high, low = halves(basis_ref[...])
    lhs[:nq, :k] = high
    lhs[:nq, k : 2 * k] = high
    lhs[:nq, 2 * k :] = low
    high, low = halves(panel_ref[...])
    lhs[nq:, :k] = high
    lhs[nq:, k : 2 * k] = high
    lhs[nq:, 2 * k :] = low

    def multiply(q, tiles):
        for t, tile in enumerate(tiles):
            rows = slice(t * BLOCK, (t + 1) * BLOCK)
            high, low = halves(tile)
            rhs[rows, :k] = high
            rhs[rows, k : 2 * k] = low
            rhs[rows, 2 * k :] = high
        out = dot_nt(lhs[:nq, :], rhs[...])
        for t in range(2):
            part[q, t, :, :rq, :] = out[:, t * BLOCK : (t + 1) * BLOCK].reshape(pieces, rq, BLOCK)
        out = dot_nt(lhs[nq:, :], rhs[...])
        for t in range(2):
            part[q, t, :, rq:, :] = out[:, t * BLOCK : (t + 1) * BLOCK].reshape(pieces, rp, BLOCK)

    mine_x = pl.ds(me.x * nz, nz)

    def to_core(q):
        remote(
            part.at[q, 1 - me.core], from_core.at[q], send.at[0, q], recv.at[0, q], me.other_core()
        ).start()

    def to_x(q):
        await_bytes(from_core.at[q], recv.at[0, q])
        part[q, me.core] += from_core[q]
        for d, x, device in me.over_x():
            remote(
                part.at[q, me.core, pl.ds(x * nz, nz)],
                from_x.at[q, d],
                send.at[1, q],
                recv.at[1, q],
                device,
            ).start()

    def to_z(q):
        await_bytes(from_x.at[q], recv.at[1, q])
        total = part[q, me.core, mine_x]
        for d in range(nx - 1):
            total = total + from_x[q, d]
        part[q, me.core, mine_x] = total
        for d, z, device in me.over_z():
            remote(
                part.at[q, me.core, me.x * nz + z],
                from_z.at[q, d],
                send.at[2, q],
                recv.at[2, q],
                device,
            ).start()

    def back_z(q):
        await_bytes(from_z.at[q], recv.at[2, q])
        total = part[q, me.core, me.at]
        for d in range(nz - 1):
            total = total + from_z[q, d]
        total = total * (1.0 / n_grid)
        own[q] = total[rq:]
        gathered[q, me.core, me.at] = total[:rq]
        here = gathered.at[q, me.core, me.at]
        for _, _, device in me.over_z():
            remote(here, here, send.at[3, q], recv.at[3, q], device).start()

    def back_x(q):
        await_bytes(gathered.at[q, 0, pl.ds(0, nz - 1)], recv.at[3, q])
        here = gathered.at[q, me.core, mine_x]
        for _, _, device in me.over_x():
            remote(here, here, send.at[4, q], recv.at[4, q], device).start()

    def back_core(q):
        await_bytes(gathered.at[q, 0, pl.ds(0, (nx - 1) * nz)], recv.at[4, q])
        here = gathered.at[q, me.core]
        remote(here, here, send.at[5, q], recv.at[5, q], me.other_core()).start()

    def finish(q):
        await_bytes(gathered.at[q, 0], recv.at[5, q])
        for t in range(CORES):
            at = pl.multiple_of(tile_of(me.band, t, q) * BLOCK, BLOCK)
            coeffs_ref[:, pl.ds(at, BLOCK)] = gathered[q, t].reshape(nq, BLOCK)

    def remove(q):
        parts = [halves(gathered[q, t].reshape(nq, BLOCK).T) for t in range(CORES)]
        high = jnp.concatenate([p[0] for p in parts], 0)
        both = jnp.concatenate([high] + [p[1] for p in parts], 0)
        out = jnp.dot(both, lhs[:nq, :k], preferred_element_type=jnp.float32)
        out = out[: 2 * BLOCK] + out[2 * BLOCK :]
        out = out + jnp.dot(high, lhs[:nq, 2 * k :], preferred_element_type=jnp.float32)
        removed[q] = out.reshape(CORES, BLOCK, k)

    across = {"grid": me.grid, "band": lax.rem(me.band + 2, BANDS)}

    def bulk(i, src, dst, device):
        return remote(src, dst, b_send.at[i], b_recv.at[i], device)

    bulks = [
        bulk(0, removed.at[1, 0], from_band.at[0, 0], right),
        bulk(1, removed.at[1, 1], from_band.at[2, 0], left),
        bulk(2, removed.at[2, 0], from_band.at[2, 1], left),
        bulk(3, removed.at[2, 1], from_band.at[0, 1], right),
        bulk(4, removed.at[3], from_band.at[1], across),
    ]

    multiply(0, (panel_ref[lo, :], panel_ref[hi, :]))
    to_core(0)
    to_x(0)
    to_z(0)
    hops[0].wait_recv()
    hops[4].start()
    hops[1].wait_recv()
    multiply(1, (others[0, lo, :], others[2, lo, :]))
    to_core(1)
    back_z(0)
    to_x(1)
    back_x(0)
    to_z(1)
    hops[3].wait_recv()
    hops[5].start()
    hops[2].wait_recv()
    multiply(2, (others[2, hi, :], others[0, hi, :]))
    to_core(2)
    back_z(1)
    back_core(0)
    to_x(2)
    back_x(1)
    to_z(2)
    hops[4].wait_recv()
    hops[5].wait_recv()
    multiply(3, (others[1, lo, :], others[1, hi, :]))
    to_core(3)
    back_z(2)
    to_x(3)
    back_core(1)
    back_x(2)
    finish(0)
    to_z(3)
    back_core(2)
    finish(1)
    remove(1)
    bulks[0].start()
    bulks[1].start()
    back_z(3)
    finish(2)
    remove(2)
    back_x(3)
    remove(0)
    back_core(3)
    for h in hops:
        h.wait_send()
    finish(3)

    high, low = halves(coeffs_ref[...])
    stacked[:nq, :] = high
    stacked[nq : 2 * nq, :] = low
    stacked[2 * nq :, :] = high
    n = coeffs_ref.shape[1]
    count = BANDS * rp
    row = lax.broadcasted_iota(jnp.int32, (count, n), 0)
    col = lax.broadcasted_iota(jnp.int32, (count, n), 1)
    want = lax.div(row, rp) * np_ + lax.rem(row, rp) + me.at * rp
    pick = jnp.where(col == want, 1.0, 0.0).astype(jnp.bfloat16)
    high = dot_nt(pick, stacked[:nq, :]).astype(jnp.bfloat16)
    low = dot_nt(pick, stacked[nq : 2 * nq, :]).astype(jnp.bfloat16)
    square = jnp.dot(
        jnp.concatenate([high, high, low], 1), stacked[...], preferred_element_type=jnp.float32
    )
    for band in range(BANDS):
        rows = square[band * rp : (band + 1) * rp]
        for i in range(KEPT):
            first = 2 * ((band + i) % BANDS) * BLOCK
            pair = [rows[:, first + t * BLOCK : first + (t + 1) * BLOCK] for t in range(CORES)]
            share[me.band, band, i] = -jnp.where(me.core == 0, pair[0], pair[1])
    for i, q in enumerate((0, 1 + me.core, ROUNDS - 1)):
        share[me.band, me.band, i] += own[q]
    for _, _, device in me.over_y():
        remote(share.at[me.band], share.at[me.band], g_send.at[0], g_recv.at[0], device).start()
    bulks[2].start()
    bulks[3].start()
    remove(3)
    bulks[4].start()
    await_bytes(share.at[pl.ds(0, BANDS - 1)], g_recv.at[0])
    pieces_of[me.core, me.x, me.z] = (share[0] + share[1]) + (share[2] + share[3])

    up, down = lax.rem(me.x + 1, nx), lax.rem(me.x + nx - 1, nx)
    to_up, to_down = me.id(me.z, up, me.core), me.id(me.z, down, me.core)
    first, second = pl.ds(0, BANDS // 2), pl.ds(BANDS // 2, BANDS // 2)

    def spread(i, z):
        here = pieces_of.at[me.core, me.x, z]
        remote(here, here, g_send.at[2], x_recv.at[0, i], to_up).start()
        remote(here, here, g_send.at[2], x_recv.at[1, i], to_down).start()

    def relay(i, z):
        await_bytes(pieces_of.at[0, 0, 0], x_recv.at[0, i])
        here = pieces_of.at[me.core, down, z, first]
        remote(here, here, g_send.at[3], g_recv.at[1], to_up).start()
        await_bytes(pieces_of.at[0, 0, 0], x_recv.at[1, i])
        here = pieces_of.at[me.core, up, z, second]
        remote(here, here, g_send.at[3], g_recv.at[1], to_down).start()

    def cross(x):
        here = pieces_of.at[me.core, x]
        remote(here, here, g_send.at[4], g_recv.at[2], me.other_core()).start()

    here = pieces_of.at[me.core, me.x, me.z]
    for d, _, device in me.over_z():
        remote(here, here, g_send.at[1], z_recv.at[d], device).start()
    spread(0, me.z)
    order = [me.z]
    for i, d in enumerate(sorted(range(1, nz), key=lambda d: min(d, nz - d))):
        z = lax.rem(me.z + nz - d, nz)
        await_bytes(pieces_of.at[0, 0, 0], z_recv.at[d - 1])
        spread(i + 1, z)
        relay(i, order[i])
        order.append(z)
    cross(me.x)
    relay(nz - 1, order[nz - 1])
    cross(up)
    cross(down)
    await_bytes(pieces_of.at[0, 0], g_recv.at[1])
    cross(lax.rem(me.x + 2, nx))

    def place(core):
        for band in range(BANDS):
            for i in range(KEPT):
                at = (2 * ((band + i) % BANDS) + core) * BLOCK
                tile = pieces_of[core, :, :, band, i].reshape(np_, BLOCK)
                gram_ref[band * np_ : (band + 1) * np_, at : at + BLOCK] = tile
                if i == 1:
                    to = (2 * ((band + i) % BANDS) + core) * BLOCK
                    gram_ref[to : to + BLOCK, band * np_ : (band + 1) * np_] = tile.T

    await_bytes(pieces_of.at[0], g_recv.at[2])
    place(0)
    place(1)
    for h in bulks:
        h.wait_recv()
    for t in range(CORES):
        rows = slice(t * BLOCK, (t + 1) * BLOCK)
        total = removed[0, t]
        for d in range(BANDS - 1):
            total = total + from_band[d, t]
        projected[rows, :] = panel_ref[rows, :] - total

    def carry(i, src, dst, device):
        return remote(src, dst, p_send.at[i], p_recv.at[i], device)

    carried = [
        carry(0, projected.at[lo], projected_others.at[2, lo], right),
        carry(1, projected.at[lo], projected_others.at[0, lo], left),
        carry(2, projected.at[hi], projected_others.at[2, hi], right),
        carry(3, projected.at[hi], projected_others.at[0, hi], left),
        carry(4, projected_others.at[2, lo], projected_others.at[1, lo], right),
        carry(5, projected_others.at[0, hi], projected_others.at[1, hi], left),
    ]
    for h in carried[:4]:
        h.start()

    def midway():
        carried[0].wait_recv()
        carried[4].start()
        carried[3].wait_recv()
        carried[5].start()

    factor_steps(gram_ref, diag, diag_right, lower, right_parts_of, midway)
    mine = pl.ds(pl.multiple_of(me.band * np_, np_), np_)
    row = lax.broadcasted_iota(jnp.int32, (np_, np_), 0) + me.band * np_
    col = lax.broadcasted_iota(jnp.int32, (np_, np_), 1)

    def times(r, block):
        first = lax.rem(me.band + r, BANDS) * np_
        tile = gram_ref[mine, pl.ds(pl.multiple_of(first, np_), np_)]
        tile = jnp.where(col + first <= row, tile, 0.0)
        return jnp.dot(
            left_parts(tile), right_parts(block, 0), preferred_element_type=jnp.float32
        )

    panel_out_ref[...] = times(0, projected[...])
    carried[1].wait_recv()
    carried[2].wait_recv()
    panel_out_ref[...] += times(1, projected_others[0])
    panel_out_ref[...] += times(3, projected_others[2])
    carried[4].wait_recv()
    carried[5].wait_recv()
    panel_out_ref[...] += times(2, projected_others[1])
    for h in carried:
        h.wait_send()

    for h in bulks:
        h.wait_send()
    for q in range(ROUNDS):
        await_bytes(from_core.at[q], send.at[0, q])
        await_bytes(from_x.at[q], send.at[1, q])
        await_bytes(from_z.at[q], send.at[2, q])
        await_bytes(gathered.at[q, 0, pl.ds(0, nz - 1)], send.at[3, q])
        await_bytes(gathered.at[q, 0, pl.ds(0, (nx - 1) * nz)], send.at[4, q])
        await_bytes(gathered.at[q, 0], send.at[5, q])
    await_bytes(share.at[pl.ds(0, BANDS - 1)], g_send.at[0])
    await_bytes(pieces_of.at[0, 0, pl.ds(0, nz - 1)], g_send.at[1])
    await_bytes(pieces_of.at[0, pl.ds(0, 2)], g_send.at[2])
    await_bytes(pieces_of.at[0, 0], g_send.at[3])
    await_bytes(pieces_of.at[0], g_send.at[4])


def reduce_and_project(nx, nz, n_grid, basis, panel):
    nq, k = basis.shape
    np_ = panel.shape[0]
    n = np_ * BANDS
    pieces = nx * nz
    rq, rp = nq // pieces, np_ // pieces
    f32 = jnp.float32
    dma = pltpu.SemaphoreType.DMA
    return pl.pallas_call(
        functools.partial(gather_kernel, nx, nz, n_grid),
        out_shape=(
            jax.ShapeDtypeStruct((nq, n), f32),
            jax.ShapeDtypeStruct((np_, k), f32),
        ),
        in_specs=[pl.BlockSpec(memory_space=pltpu.VMEM)] * 2,
        out_specs=(pl.BlockSpec(memory_space=pltpu.VMEM),) * 2,
        scratch_shapes=[
            pltpu.VMEM((BANDS - 1, np_, k), f32),
            pltpu.VMEM((nq + np_, 3 * k), jnp.bfloat16),
            pltpu.VMEM((2 * BLOCK, 3 * k), jnp.bfloat16),
            pltpu.VMEM((ROUNDS, CORES, pieces, rq + rp, BLOCK), f32),
            pltpu.VMEM((ROUNDS, pieces, rq + rp, BLOCK), f32),
            pltpu.VMEM((ROUNDS, nx - 1, nz, rq + rp, BLOCK), f32),
            pltpu.VMEM((ROUNDS, nz - 1, rq + rp, BLOCK), f32),
            pltpu.VMEM((ROUNDS, CORES, pieces, rq, BLOCK), f32),
            pltpu.VMEM((ROUNDS, rp, BLOCK), f32),
            pltpu.VMEM((ROUNDS, CORES, BLOCK, k), f32),
            pltpu.VMEM((BANDS - 1, CORES, BLOCK, k), f32),
            pltpu.VMEM((3 * nq, n), jnp.bfloat16),
            pltpu.VMEM((BANDS, BANDS, KEPT, rp, BLOCK), f32),
            pltpu.VMEM((CORES, nx, nz, BANDS, KEPT, rp, BLOCK), f32),
            pltpu.VMEM((n, n), f32),
            pltpu.VMEM((BLOCK, BLOCK), f32),
            pltpu.VMEM((BLOCK, 3 * BLOCK), jnp.bfloat16),
            pltpu.VMEM((n, 3 * BLOCK), jnp.bfloat16),
            pltpu.VMEM((3 * BLOCK, n), jnp.bfloat16),
            pltpu.VMEM((np_, k), f32),
            pltpu.VMEM((BANDS - 1, np_, k), f32),
            dma((6,)),
            dma((6,)),
            dma((6, ROUNDS)),
            dma((6, ROUNDS)),
            dma((5,)),
            dma((5,)),
            dma((5,)),
            dma((nz - 1,)),
            dma((2, nz)),
            dma((3,)),
            dma((6,)),
            dma((6,)),
        ],
        compiler_params=pltpu.CompilerParams(
            collective_id=0, has_side_effects=True, vmem_limit_bytes=60 * 1024 * 1024
        ),
        cost_estimate=pl.CostEstimate(
            flops=60 * 1024**3, bytes_accessed=8 * 1024 * 1024, transcendentals=0
        ),
    )(basis, panel)


def body(basis, panel):
    grid = lax.axis_size("grid")
    nz = grid // (CORES * ALONG_X)
    coeffs, new_panel = reduce_and_project(
        ALONG_X, nz, panel.shape[1] * grid, basis, panel
    )
    return (new_panel, coeffs)


def solution(mesh):
    placed = (P("band", "grid"), P("band", "grid"))
    return jax.shard_map(
        body,
        mesh=mesh,
        in_specs=placed,
        out_specs=(P("band", "grid"), P("band", None)),
        check_vma=False,
    )
```

```python
import functools

import jax
import jax.numpy as jnp
from jax import lax
from jax.experimental import pallas as pl
from jax.experimental.pallas import tpu as pltpu
from jax.sharding import PartitionSpec as P

BLOCK = 128
ROWS = 8
CORES = 2
BANDS = 4
ROUNDS = 4
KEPT = 3
GROUP = 4
EARLY = 1
MIDWAY = 4
ALONG_X = 4
MESH = pl.DeviceIdType.MESH


def halves(x):
    high = x.astype(jnp.bfloat16)
    low = (x - high.astype(jnp.float32)).astype(jnp.bfloat16)
    return high, low


def left_parts(x):
    high, low = halves(x)
    return jnp.concatenate([high, high, low], 1)


def right_parts(x, axis):
    high, low = halves(x)
    return jnp.concatenate([high, low, high], axis)


def dot_nt(left, right):
    return lax.dot_general(
        left, right, (((1,), (1,)), ((), ())), preferred_element_type=jnp.float32
    )


def tile_of(band, core, turn):
    one, two, three = (lax.rem(band + i, BANDS) for i in (1, 2, 3))
    if turn == 0:
        return 2 * band + core
    if turn == 1:
        return 2 * (three + core * (one - three)) + core
    if turn == 2:
        return 2 * (one + core * (three - one)) + core
    return 2 * two + core


class Place:
    def __init__(self, nx, nz):
        self.nx, self.nz = nx, nz
        self.grid = lax.axis_index("grid")
        self.band = lax.axis_index("band")
        self.core = lax.rem(self.grid, CORES)
        self.x = lax.rem(lax.div(self.grid, CORES), nx)
        self.z = lax.div(self.grid, CORES * nx)
        self.at = self.x * nz + self.z

    def id(self, z, x, core):
        return {"grid": (z * self.nx + x) * CORES + core, "band": self.band}

    def other_core(self):
        return self.id(self.z, self.x, 1 - self.core)

    def over_x(self):
        for d in range(1, self.nx):
            x = lax.rem(self.x + d, self.nx)
            yield d - 1, x, self.id(self.z, x, self.core)

    def over_z(self):
        for d in range(1, self.nz):
            z = lax.rem(self.z + d, self.nz)
            yield d - 1, z, self.id(z, self.x, self.core)

    def over_y(self):
        for d in range(1, BANDS):
            band = lax.rem(self.band + d, BANDS)
            yield d - 1, band, {"grid": self.grid, "band": band}

    def barrier(self):
        sem = pltpu.get_barrier_semaphore()
        ids = [self.other_core()]
        ids += [i for _, _, i in self.over_x()]
        ids += [i for _, _, i in self.over_z()]
        ids += [i for _, _, i in self.over_y()]
        for i in ids:
            pl.semaphore_signal(sem, inc=1, device_id=i, device_id_type=MESH)
        pl.semaphore_wait(sem, len(ids))


def remote(src, dst, send, recv, device):
    return pltpu.make_async_remote_copy(
        src_ref=src,
        dst_ref=dst,
        send_sem=send,
        recv_sem=recv,
        device_id=device,
        device_id_type=MESH,
    )


def await_bytes(ref, sem):
    pltpu.make_async_copy(ref, ref, sem).wait()


def across_lanes(tile, lane):
    return jnp.broadcast_to(tile[:, lane : lane + 1], (ROWS, BLOCK))


def down_rows(tile, row):
    return jnp.broadcast_to(tile[row : row + 1, :], (ROWS, BLOCK))


def block_inverse(tiles):
    lanes = lax.broadcasted_iota(jnp.int32, (ROWS, BLOCK), 1)
    subs = lax.broadcasted_iota(jnp.int32, (ROWS, BLOCK), 0)
    tiles = list(tiles)
    count = len(tiles)
    done = []
    outs = []
    square = [across_lanes(tiles[0], q) for q in range(ROWS)]
    for t in range(count):
        base = ROWS * t
        here = (lanes >= base) & (lanes < base + ROWS)
        more = t + 1 < count
        if more:
            ahead = tiles[t + 1]
            side = [across_lanes(ahead, base + q) for q in range(ROWS)]
            following = [across_lanes(ahead, base + ROWS + q) for q in range(ROWS)]
        far = t + 2 < min(count, (t // GROUP + 1) * GROUP + 1)
        if far:
            beyond = tiles[t + 2]
            wing = [across_lanes(beyond, base + q) for q in range(ROWS)]
        current = jnp.where(here, jnp.where(lanes - base == subs, 1.0, 0.0), tiles[t])
        rows, scaled, unit = [], [], {}
        out = None
        for q in range(ROWS):
            root = lax.rsqrt(down_rows(square[q], q))
            inv = root * root
            scaled.append(inv)
            row = down_rows(current, q)
            rows.append(row)
            out = row * root if q == 0 else jnp.where(subs == q, row * root, out)
            if q + 1 < ROWS:
                current = current - (square[q] * inv) * row
            for s in range(q + 1, ROWS):
                unit[s, q] = down_rows(square[q], s) * inv
                square[s] = square[s] - unit[s, q] * square[q]
            if far:
                for s in range(q + 1, ROWS):
                    wing[s] = wing[s] - unit[s, q] * wing[q]
                beyond = (jnp.where(here, 0.0, beyond) if q == 0 else beyond) - (wing[q] * inv) * row
            if more:
                weight = side[q] * inv
                for s in range(q + 1, ROWS):
                    side[s] = side[s] - unit[s, q] * side[q]
                for s in range(ROWS):
                    following[s] = following[s] - weight * down_rows(side[q], s)
                ahead = (jnp.where(here, 0.0, ahead) if q == 0 else ahead) - weight * row
        if far:
            tiles[t + 2] = beyond
        done.append(jnp.where(lanes <= base + subs, out, 0.0))
        ends = (t // GROUP + 1) * GROUP * ROWS
        outs.append((out, jnp.where((lanes < base + ROWS) | (lanes >= ends), out, 0.0)))
        if more:
            square = following
            tiles[t + 1] = ahead
        if t + 3 < min(count, (t // GROUP + 1) * GROUP + 1):
            back = [rows[p] * scaled[p] for p in range(ROWS)]
            for p in range(ROWS - 1, 0, -1):
                for q in range(p):
                    back[q] = back[q] - unit[p, q] * back[p]
            for u in range(t + 3, min(count, (t // GROUP + 1) * GROUP + 1)):
                old = tiles[u]
                new = jnp.where(here, 0.0, old)
                for p in range(ROWS):
                    new = new - across_lanes(old, base + p) * back[p]
                tiles[u] = new
        first = t + 1 + 1
        if (t + 1) % GROUP == 0 and first < count:
            high, low = halves(jnp.concatenate([o[0] for o in outs[t + 1 - GROUP :]], 0))
            rhigh, rlow = halves(jnp.concatenate([o[1] for o in outs[t + 1 - GROUP :]], 0))
            change = lax.dot_general(
                jnp.concatenate([high, high, low], 0),
                jnp.concatenate([rhigh, rlow, rhigh], 0),
                (((0,), (0,)), ((), ())),
                preferred_element_type=jnp.float32,
            )
            group = (lanes >= base + ROWS - GROUP * ROWS) & (lanes < base + ROWS)
            for u in range(first, count):
                tiles[u] = jnp.where(group, 0.0, tiles[u]) - change[u * ROWS : (u + 1) * ROWS]
    return done


def factor_steps(a_ref, diag_ref, diag_right, lower_ref, right_ref, early, midway):
    n = a_ref.shape[0]
    blocks = n // BLOCK
    wide = 2 * BLOCK
    diag_right[...] = jnp.zeros_like(diag_right)
    right_ref[...] = jnp.zeros_like(right_ref)

    def step(k, carry):
        pl.when(k == EARLY)(early)
        pl.when(k == MIDWAY)(midway)
        at = pl.ds(pl.multiple_of(k * BLOCK, BLOCK), BLOCK)
        before = pl.ds(pl.multiple_of(jnp.maximum(k - 1, 0) * BLOCK, BLOCK), BLOCK)
        after = pl.ds(pl.multiple_of(jnp.minimum(k + 1, blocks - 1) * BLOCK, BLOCK), BLOCK)
        base = pl.multiple_of(k * BLOCK, BLOCK)
        tiles = [a_ref[pl.ds(base + ROWS * t, ROWS), at] for t in range(BLOCK // ROWS)]

        for j in range(2, blocks):
            rows = slice(j * BLOCK, (j + 1) * BLOCK)
            on = jnp.where((j > k) & (k > 0), 1.0, 0.0).astype(jnp.float32)
            old = a_ref[rows, before]
            lower_ref[rows, :] = left_parts(dot_nt(left_parts(old), diag_right[...]) * on)
            a_ref[rows, before] = old * (1.0 - on)
        for c in range(n // wide):
            cols = slice(c * wide, (c + 1) * wide)
            for j in range(1, blocks // 2):
                rows = slice(j * wide, (j + 1) * wide)
                a_ref[rows, cols] -= jnp.dot(
                    lower_ref[rows, :], right_ref[:, cols], preferred_element_type=jnp.float32
                )
        for t, tile in enumerate(block_inverse(tiles)):
            diag_ref[ROWS * t : ROWS * (t + 1), :] = tile

        diag = diag_ref[...]
        a_ref[at, :] = jnp.dot(
            left_parts(diag), right_parts(a_ref[at, :], 0), preferred_element_type=jnp.float32
        )
        a_ref[at, at] = diag
        right_ref[...] = right_parts(a_ref[at, :], 0)
        diag_right[...] = right_parts(diag, 1)
        on = jnp.where(k < blocks - 1, 1.0, 0.0).astype(jnp.float32)
        old = a_ref[after, at]
        low = dot_nt(left_parts(old), diag_right[...]) * on
        a_ref[after, at] = old * (1.0 - on)
        a_ref[after, :] -= jnp.dot(left_parts(low), right_ref[...], preferred_element_type=jnp.float32)
        return carry

    lax.fori_loop(0, blocks, step, 0)


def gather_kernel(
    nx, nz, n_grid,
    basis_in, panel_in,
    coeffs_out, panel_out,
    basis_ref, panel_ref, coeffs_ref,
    others, lhs, rhs, part, from_core, from_x, from_z, gathered, own,
    removed, from_band, stacked, share, pieces_of,
    gram_ref, diag, diag_right, lower, right_parts_of, projected, projected_others,
    y_send, y_recv, send, recv, b_send, b_recv, g_send, z_recv, x_recv, g_recv, p_send, p_recv, io_sem,
):
    me = Place(nx, nz)
    fetch_panel = pltpu.make_async_copy(panel_in, panel_ref, io_sem.at[0])
    fetch_basis = pltpu.make_async_copy(basis_in, basis_ref, io_sem.at[1])
    fetch_panel.start()
    fetch_basis.start()
    me.barrier()
    nq, k = basis_ref.shape
    np_ = panel_ref.shape[0]
    pieces = nx * nz
    rq, rp = nq // pieces, np_ // pieces
    half = np_ // 2
    lo, hi = pl.ds(0, half), pl.ds(half, half)
    right = {"grid": me.grid, "band": lax.rem(me.band + 1, BANDS)}
    left = {"grid": me.grid, "band": lax.rem(me.band + BANDS - 1, BANDS)}

    def hop(i, src, dst, device):
        return remote(src, dst, y_send.at[i], y_recv.at[i], device)

    hops = [
        hop(0, panel_ref.at[lo], others.at[2, lo], right),
        hop(1, panel_ref.at[hi], others.at[0, hi], left),
        hop(2, panel_ref.at[hi], others.at[2, hi], right),
        hop(3, panel_ref.at[lo], others.at[0, lo], left),
        hop(4, others.at[2, lo], others.at[1, lo], right),
        hop(5, others.at[0, hi], others.at[1, hi], left),
    ]
    fetch_panel.wait()
    for h in hops[:4]:
        h.start()
    fetch_basis.wait()

    high, low = halves(basis_ref[...])
    lhs[:nq, :k] = high
    lhs[:nq, k : 2 * k] = high
    lhs[:nq, 2 * k :] = low
    high, low = halves(panel_ref[...])
    lhs[nq:, :k] = high
    lhs[nq:, k : 2 * k] = high
    lhs[nq:, 2 * k :] = low

    def multiply(q, tiles):
        for t, tile in enumerate(tiles):
            rows = slice(t * BLOCK, (t + 1) * BLOCK)
            high, low = halves(tile)
            rhs[rows, :k] = high
            rhs[rows, k : 2 * k] = low
            rhs[rows, 2 * k :] = high
        out = dot_nt(lhs[:nq, :], rhs[...])
        for t in range(2):
            part[q, t, :, :rq, :] = out[:, t * BLOCK : (t + 1) * BLOCK].reshape(pieces, rq, BLOCK)
        out = dot_nt(lhs[nq:, :], rhs[...])
        for t in range(2):
            part[q, t, :, rq:, :] = out[:, t * BLOCK : (t + 1) * BLOCK].reshape(pieces, rp, BLOCK)

    mine_x = pl.ds(me.x * nz, nz)

    def to_core(q):
        remote(
            part.at[q, 1 - me.core], from_core.at[q], send.at[0, q], recv.at[0, q], me.other_core()
        ).start()

    def to_x(q):
        await_bytes(from_core.at[q], recv.at[0, q])
        part[q, me.core] += from_core[q]
        for d, x, device in me.over_x():
            remote(
                part.at[q, me.core, pl.ds(x * nz, nz)],
                from_x.at[q, d],
                send.at[1, q],
                recv.at[1, q],
                device,
            ).start()

    def to_z(q):
        await_bytes(from_x.at[q], recv.at[1, q])
        total = part[q, me.core, mine_x]
        for d in range(nx - 1):
            total = total + from_x[q, d]
        part[q, me.core, mine_x] = total
        for d, z, device in me.over_z():
            remote(
                part.at[q, me.core, me.x * nz + z],
                from_z.at[q, d],
                send.at[2, q],
                recv.at[2, q],
                device,
            ).start()

    def back_z(q):
        await_bytes(from_z.at[q], recv.at[2, q])
        total = part[q, me.core, me.at]
        for d in range(nz - 1):
            total = total + from_z[q, d]
        total = total * (1.0 / n_grid)
        own[q] = total[rq:]
        gathered[q, me.core, me.at] = total[:rq]
        here = gathered.at[q, me.core, me.at]
        for _, _, device in me.over_z():
            remote(here, here, send.at[3, q], recv.at[3, q], device).start()

    def back_x(q):
        await_bytes(gathered.at[q, 0, pl.ds(0, nz - 1)], recv.at[3, q])
        here = gathered.at[q, me.core, mine_x]
        for _, _, device in me.over_x():
            remote(here, here, send.at[4, q], recv.at[4, q], device).start()

    def back_core(q):
        await_bytes(gathered.at[q, 0, pl.ds(0, (nx - 1) * nz)], recv.at[4, q])
        here = gathered.at[q, me.core]
        remote(here, here, send.at[5, q], recv.at[5, q], me.other_core()).start()

    def finish(q):
        await_bytes(gathered.at[q, 0], recv.at[5, q])
        for t in range(CORES):
            at = pl.multiple_of(tile_of(me.band, t, q) * BLOCK, BLOCK)
            coeffs_ref[:, pl.ds(at, BLOCK)] = gathered[q, t].reshape(nq, BLOCK)

    def remove(q):
        parts = [halves(gathered[q, t].reshape(nq, BLOCK).T) for t in range(CORES)]
        high = jnp.concatenate([p[0] for p in parts], 0)
        both = jnp.concatenate([high] + [p[1] for p in parts], 0)
        out = jnp.dot(both, lhs[:nq, :k], preferred_element_type=jnp.float32)
        out = out[: 2 * BLOCK] + out[2 * BLOCK :]
        out = out + jnp.dot(high, lhs[:nq, 2 * k :], preferred_element_type=jnp.float32)
        removed[q] = out.reshape(CORES, BLOCK, k)

    def bulk(i, src, dst, device):
        return remote(src, dst, b_send.at[i], b_recv.at[i], device)

    bulks = [
        bulk(0, removed.at[1, 0], from_band.at[2, 0], left),
        bulk(1, removed.at[1, 1], from_band.at[0, 1], right),
        bulk(2, removed.at[3, 0], from_band.at[1, 0], right),
        bulk(3, removed.at[3, 1], from_band.at[1, 1], left),
        bulk(4, removed.at[2, 0], from_band.at[0, 0], right),
        bulk(5, removed.at[2, 1], from_band.at[2, 1], left),
    ]

    multiply(0, (panel_ref[lo, :], panel_ref[hi, :]))
    to_core(0)
    to_x(0)
    to_z(0)
    hops[0].wait_recv()
    hops[4].start()
    hops[1].wait_recv()
    hops[5].start()
    multiply(1, (others[2, lo, :], others[0, hi, :]))
    to_core(1)
    back_z(0)
    to_x(1)
    back_x(0)
    to_z(1)
    hops[2].wait_recv()
    hops[3].wait_recv()
    multiply(2, (others[0, lo, :], others[2, hi, :]))
    to_core(2)
    back_z(1)
    back_core(0)
    to_x(2)
    back_x(1)
    to_z(2)
    hops[4].wait_recv()
    hops[5].wait_recv()
    multiply(3, (others[1, lo, :], others[1, hi, :]))
    to_core(3)
    back_z(2)
    to_x(3)
    back_core(1)
    finish(0)
    finish(1)
    remove(1)
    bulks[0].start()
    bulks[1].start()
    back_x(2)
    to_z(3)
    back_core(2)
    finish(2)
    remove(2)
    back_z(3)
    remove(0)
    back_x(3)
    back_core(3)
    for h in hops:
        h.wait_send()
    finish(3)
    leave_coeffs = pltpu.make_async_copy(coeffs_ref, coeffs_out, io_sem.at[2])
    leave_coeffs.start()

    high, low = halves(coeffs_ref[...])
    stacked[:nq, :] = high
    stacked[nq : 2 * nq, :] = low
    stacked[2 * nq :, :] = high
    n = coeffs_ref.shape[1]
    count = BANDS * rp
    row = lax.broadcasted_iota(jnp.int32, (count, n), 0)
    col = lax.broadcasted_iota(jnp.int32, (count, n), 1)
    want = lax.div(row, rp) * np_ + lax.rem(row, rp) + me.at * rp
    pick = jnp.where(col == want, 1.0, 0.0).astype(jnp.bfloat16)
    high = dot_nt(pick, stacked[:nq, :]).astype(jnp.bfloat16)
    low = dot_nt(pick, stacked[nq : 2 * nq, :]).astype(jnp.bfloat16)
    square = jnp.dot(
        jnp.concatenate([high, high, low], 1), stacked[...], preferred_element_type=jnp.float32
    )
    for band in range(BANDS):
        rows = square[band * rp : (band + 1) * rp]
        for i in range(KEPT):
            first = 2 * ((band + i) % BANDS) * BLOCK
            pair = [rows[:, first + t * BLOCK : first + (t + 1) * BLOCK] for t in range(CORES)]
            share[me.band, band, i] = -jnp.where(me.core == 0, pair[0], pair[1])
    for i, q in enumerate((0, 2 - me.core, ROUNDS - 1)):
        share[me.band, me.band, i] += own[q]
    for _, _, device in me.over_y():
        remote(share.at[me.band], share.at[me.band], g_send.at[0], g_recv.at[0], device).start()
    remove(3)
    bulks[2].start()
    bulks[3].start()
    await_bytes(share.at[pl.ds(0, BANDS - 1)], g_recv.at[0])
    pieces_of[me.core, me.x, me.z] = (share[0] + share[1]) + (share[2] + share[3])

    up, down = lax.rem(me.x + 1, nx), lax.rem(me.x + nx - 1, nx)
    to_up, to_down = me.id(me.z, up, me.core), me.id(me.z, down, me.core)
    first, second = pl.ds(0, BANDS // 2), pl.ds(BANDS // 2, BANDS // 2)

    def spread(i, z):
        here = pieces_of.at[me.core, me.x, z]
        remote(here, here, g_send.at[2], x_recv.at[0, i], to_up).start()
        remote(here, here, g_send.at[2], x_recv.at[1, i], to_down).start()

    def relay(i, z):
        await_bytes(pieces_of.at[0, 0, 0], x_recv.at[0, i])
        here = pieces_of.at[me.core, down, z, first]
        remote(here, here, g_send.at[3], g_recv.at[1], to_up).start()
        await_bytes(pieces_of.at[0, 0, 0], x_recv.at[1, i])
        here = pieces_of.at[me.core, up, z, second]
        remote(here, here, g_send.at[3], g_recv.at[1], to_down).start()

    def cross(x):
        here = pieces_of.at[me.core, x]
        remote(here, here, g_send.at[4], g_recv.at[2], me.other_core()).start()

    here = pieces_of.at[me.core, me.x, me.z]
    nearest = sorted(range(1, nz), key=lambda d: min(d, nz - d))
    for d in nearest:
        device = me.id(lax.rem(me.z + d, nz), me.x, me.core)
        remote(here, here, g_send.at[1], z_recv.at[d - 1], device).start()
    spread(0, me.z)
    order = [me.z]
    for i, d in enumerate(nearest):
        z = lax.rem(me.z + nz - d, nz)
        await_bytes(pieces_of.at[0, 0, 0], z_recv.at[d - 1])
        spread(i + 1, z)
        relay(i, order[i])
        order.append(z)
        if i == nz // 2:
            for t in range(CORES):
                bulks[2 + t].wait_recv()
                removed[2, t] += from_band[1, t]
                bulks[4 + t].start()
    cross(me.x)
    relay(nz - 1, order[nz - 1])
    cross(up)
    cross(down)
    await_bytes(pieces_of.at[0, 0], g_recv.at[1])
    cross(lax.rem(me.x + 2, nx))

    def place(core):
        for band in range(BANDS):
            for i in range(KEPT):
                at = (2 * ((band + i) % BANDS) + core) * BLOCK
                tile = pieces_of[core, :, :, band, i].reshape(np_, BLOCK)
                gram_ref[band * np_ : (band + 1) * np_, at : at + BLOCK] = tile
                if i == 1:
                    to = (2 * ((band + i) % BANDS) + core) * BLOCK
                    gram_ref[to : to + BLOCK, band * np_ : (band + 1) * np_] = tile.T

    await_bytes(pieces_of.at[0], g_recv.at[2])
    place(0)
    place(1)
    def carry(i, src, dst, device):
        return remote(src, dst, p_send.at[i], p_recv.at[i], device)

    carried = [
        carry(0, projected.at[lo], projected_others.at[2, lo], right),
        carry(1, projected.at[hi], projected_others.at[0, hi], left),
        carry(2, projected.at[hi], projected_others.at[2, hi], right),
        carry(3, projected.at[lo], projected_others.at[0, lo], left),
        carry(4, projected_others.at[2, lo], projected_others.at[1, lo], right),
        carry(5, projected_others.at[0, hi], projected_others.at[1, hi], left),
    ]
    def early():
        for i in (0, 1, 4, 5):
            bulks[i].wait_recv()
        for t in range(CORES):
            rows = slice(t * BLOCK, (t + 1) * BLOCK)
            total = removed[0, t] + (from_band[0, t] + from_band[2, t])
            projected[rows, :] = panel_ref[rows, :] - total
        for h in carried[:4]:
            h.start()

    def midway():
        carried[0].wait_recv()
        carried[4].start()
        carried[1].wait_recv()
        carried[5].start()

    factor_steps(gram_ref, diag, diag_right, lower, right_parts_of, early, midway)
    mine = pl.ds(pl.multiple_of(me.band * np_, np_), np_)
    row = lax.broadcasted_iota(jnp.int32, (np_, np_), 0) + me.band * np_
    col = lax.broadcasted_iota(jnp.int32, (np_, np_), 1)

    def times(r, block):
        first = lax.rem(me.band + r, BANDS) * np_
        tile = gram_ref[mine, pl.ds(pl.multiple_of(first, np_), np_)]
        tile = jnp.where(col + first <= row, tile, 0.0)
        return jnp.dot(
            left_parts(tile), right_parts(block, 0), preferred_element_type=jnp.float32
        )

    panel_ref[...] = times(0, projected[...])
    carried[2].wait_recv()
    carried[3].wait_recv()
    panel_ref[...] += times(1, projected_others[0])
    panel_ref[...] += times(3, projected_others[2])
    carried[4].wait_recv()
    carried[5].wait_recv()
    panel_ref[...] += times(2, projected_others[1])
    leave_panel = pltpu.make_async_copy(panel_ref, panel_out, io_sem.at[3])
    leave_panel.start()
    leave_coeffs.wait()
    for h in carried:
        h.wait_send()

    for h in bulks:
        h.wait_send()
    for q in range(ROUNDS):
        await_bytes(from_core.at[q], send.at[0, q])
        await_bytes(from_x.at[q], send.at[1, q])
        await_bytes(from_z.at[q], send.at[2, q])
        await_bytes(gathered.at[q, 0, pl.ds(0, nz - 1)], send.at[3, q])
        await_bytes(gathered.at[q, 0, pl.ds(0, (nx - 1) * nz)], send.at[4, q])
        await_bytes(gathered.at[q, 0], send.at[5, q])
    await_bytes(share.at[pl.ds(0, BANDS - 1)], g_send.at[0])
    await_bytes(pieces_of.at[0, 0, pl.ds(0, nz - 1)], g_send.at[1])
    await_bytes(pieces_of.at[0, pl.ds(0, 2)], g_send.at[2])
    await_bytes(pieces_of.at[0, 0], g_send.at[3])
    await_bytes(pieces_of.at[0], g_send.at[4])
    leave_panel.wait()


def reduce_and_project(nx, nz, n_grid, basis, panel):
    nq, k = basis.shape
    np_ = panel.shape[0]
    n = np_ * BANDS
    pieces = nx * nz
    rq, rp = nq // pieces, np_ // pieces
    f32 = jnp.float32
    dma = pltpu.SemaphoreType.DMA
    return pl.pallas_call(
        functools.partial(gather_kernel, nx, nz, n_grid),
        out_shape=(
            jax.ShapeDtypeStruct((nq, n), f32),
            jax.ShapeDtypeStruct((np_, k), f32),
        ),
        in_specs=[pl.BlockSpec(memory_space=pl.ANY)] * 2,
        out_specs=(pl.BlockSpec(memory_space=pl.ANY),) * 2,
        scratch_shapes=[
            pltpu.VMEM((nq, k), f32),
            pltpu.VMEM((np_, k), f32),
            pltpu.VMEM((nq, n), f32),
            pltpu.VMEM((BANDS - 1, np_, k), f32),
            pltpu.VMEM((nq + np_, 3 * k), jnp.bfloat16),
            pltpu.VMEM((2 * BLOCK, 3 * k), jnp.bfloat16),
            pltpu.VMEM((ROUNDS, CORES, pieces, rq + rp, BLOCK), f32),
            pltpu.VMEM((ROUNDS, pieces, rq + rp, BLOCK), f32),
            pltpu.VMEM((ROUNDS, nx - 1, nz, rq + rp, BLOCK), f32),
            pltpu.VMEM((ROUNDS, nz - 1, rq + rp, BLOCK), f32),
            pltpu.VMEM((ROUNDS, CORES, pieces, rq, BLOCK), f32),
            pltpu.VMEM((ROUNDS, rp, BLOCK), f32),
            pltpu.VMEM((ROUNDS, CORES, BLOCK, k), f32),
            pltpu.VMEM((BANDS - 1, CORES, BLOCK, k), f32),
            pltpu.VMEM((3 * nq, n), jnp.bfloat16),
            pltpu.VMEM((BANDS, BANDS, KEPT, rp, BLOCK), f32),
            pltpu.VMEM((CORES, nx, nz, BANDS, KEPT, rp, BLOCK), f32),
            pltpu.VMEM((n, n), f32),
            pltpu.VMEM((BLOCK, BLOCK), f32),
            pltpu.VMEM((BLOCK, 3 * BLOCK), jnp.bfloat16),
            pltpu.VMEM((n, 3 * BLOCK), jnp.bfloat16),
            pltpu.VMEM((3 * BLOCK, n), jnp.bfloat16),
            pltpu.VMEM((np_, k), f32),
            pltpu.VMEM((BANDS - 1, np_, k), f32),
            dma((6,)),
            dma((6,)),
            dma((6, ROUNDS)),
            dma((6, ROUNDS)),
            dma((6,)),
            dma((6,)),
            dma((5,)),
            dma((nz - 1,)),
            dma((2, nz)),
            dma((3,)),
            dma((6,)),
            dma((6,)),
            dma((4,)),
        ],
        compiler_params=pltpu.CompilerParams(
            collective_id=0, has_side_effects=True, vmem_limit_bytes=60 * 1024 * 1024
        ),
        cost_estimate=pl.CostEstimate(
            flops=60 * 1024**3, bytes_accessed=8 * 1024 * 1024, transcendentals=0
        ),
    )(basis, panel)


def body(basis, panel):
    grid = lax.axis_size("grid")
    nz = grid // (CORES * ALONG_X)
    coeffs, new_panel = reduce_and_project(
        ALONG_X, nz, panel.shape[1] * grid, basis, panel
    )
    return (new_panel, coeffs)


def solution(mesh):
    placed = (P("band", "grid"), P("band", "grid"))
    return jax.shard_map(
        body,
        mesh=mesh,
        in_specs=placed,
        out_specs=(P("band", "grid"), P("band", None)),
        check_vma=False,
    )
```

```python
import functools

import jax
import jax.numpy as jnp
from jax import lax
from jax.experimental import pallas as pl
from jax.experimental.pallas import tpu as pltpu
from jax.sharding import PartitionSpec as P

BLOCK = 128
ROWS = 8
CORES = 2
BANDS = 4
ROUNDS = 4
KEPT = 3
GROUP = 4
EARLY = 0
MIDWAY = 4
ALONG_X = 4
MESH = pl.DeviceIdType.MESH


def halves(x):
    high = x.astype(jnp.bfloat16)
    low = (x - high.astype(jnp.float32)).astype(jnp.bfloat16)
    return high, low


def left_parts(x):
    high, low = halves(x)
    return jnp.concatenate([high, high, low], 1)


def right_parts(x, axis):
    high, low = halves(x)
    return jnp.concatenate([high, low, high], axis)


def dot_nt(left, right):
    return lax.dot_general(
        left, right, (((1,), (1,)), ((), ())), preferred_element_type=jnp.float32
    )


def tile_of(band, core, turn):
    one, two, three = (lax.rem(band + i, BANDS) for i in (1, 2, 3))
    if turn == 0:
        return 2 * band + core
    if turn == 1:
        return 2 * (three + core * (one - three)) + core
    if turn == 2:
        return 2 * (one + core * (three - one)) + core
    return 2 * two + core


class Place:
    def __init__(self, nx, nz):
        self.nx, self.nz = nx, nz
        self.grid = lax.axis_index("grid")
        self.band = lax.axis_index("band")
        self.core = lax.rem(self.grid, CORES)
        self.x = lax.rem(lax.div(self.grid, CORES), nx)
        self.z = lax.div(self.grid, CORES * nx)
        self.at = self.x * nz + self.z

    def id(self, z, x, core):
        return {"grid": (z * self.nx + x) * CORES + core, "band": self.band}

    def other_core(self):
        return self.id(self.z, self.x, 1 - self.core)

    def over_x(self):
        for d in range(1, self.nx):
            x = lax.rem(self.x + d, self.nx)
            yield d - 1, x, self.id(self.z, x, self.core)

    def over_z(self):
        for d in range(1, self.nz):
            z = lax.rem(self.z + d, self.nz)
            yield d - 1, z, self.id(z, self.x, self.core)

    def over_y(self):
        for d in range(1, BANDS):
            band = lax.rem(self.band + d, BANDS)
            yield d - 1, band, {"grid": self.grid, "band": band}

    def barrier(self):
        sem = pltpu.get_barrier_semaphore()
        ids = [self.other_core()]
        ids += [i for _, _, i in self.over_x()]
        ids += [i for _, _, i in self.over_z()]
        ids += [i for _, _, i in self.over_y()]
        for i in ids:
            pl.semaphore_signal(sem, inc=1, device_id=i, device_id_type=MESH)
        pl.semaphore_wait(sem, len(ids))


def remote(src, dst, send, recv, device):
    return pltpu.make_async_remote_copy(
        src_ref=src,
        dst_ref=dst,
        send_sem=send,
        recv_sem=recv,
        device_id=device,
        device_id_type=MESH,
    )


def await_bytes(ref, sem):
    pltpu.make_async_copy(ref, ref, sem).wait()


def across_lanes(tile, lane):
    return jnp.broadcast_to(tile[:, lane : lane + 1], (ROWS, BLOCK))


def down_rows(tile, row):
    return jnp.broadcast_to(tile[row : row + 1, :], (ROWS, BLOCK))


def block_inverse(tiles):
    lanes = lax.broadcasted_iota(jnp.int32, (ROWS, BLOCK), 1)
    subs = lax.broadcasted_iota(jnp.int32, (ROWS, BLOCK), 0)
    tiles = list(tiles)
    count = len(tiles)
    done = []
    outs = []
    square = [across_lanes(tiles[0], q) for q in range(ROWS)]
    for t in range(count):
        base = ROWS * t
        here = (lanes >= base) & (lanes < base + ROWS)
        more = t + 1 < count
        if more:
            ahead = tiles[t + 1]
            side = [across_lanes(ahead, base + q) for q in range(ROWS)]
            following = [across_lanes(ahead, base + ROWS + q) for q in range(ROWS)]
        far = t + 2 < min(count, (t // GROUP + 1) * GROUP + 1)
        if far:
            beyond = tiles[t + 2]
            wing = [across_lanes(beyond, base + q) for q in range(ROWS)]
        current = jnp.where(here, jnp.where(lanes - base == subs, 1.0, 0.0), tiles[t])
        rows, scaled, unit = [], [], {}
        out = None
        for q in range(ROWS):
            root = lax.rsqrt(down_rows(square[q], q))
            inv = root * root
            scaled.append(inv)
            row = down_rows(current, q)
            rows.append(row)
            out = row * root if q == 0 else jnp.where(subs == q, row * root, out)
            if q + 1 < ROWS:
                current = current - (square[q] * inv) * row
            for s in range(q + 1, ROWS):
                unit[s, q] = down_rows(square[q], s) * inv
                square[s] = square[s] - unit[s, q] * square[q]
            if far:
                for s in range(q + 1, ROWS):
                    wing[s] = wing[s] - unit[s, q] * wing[q]
                beyond = (jnp.where(here, 0.0, beyond) if q == 0 else beyond) - (wing[q] * inv) * row
            if more:
                weight = side[q] * inv
                for s in range(q + 1, ROWS):
                    side[s] = side[s] - unit[s, q] * side[q]
                for s in range(ROWS):
                    following[s] = following[s] - weight * down_rows(side[q], s)
                ahead = (jnp.where(here, 0.0, ahead) if q == 0 else ahead) - weight * row
        if far:
            tiles[t + 2] = beyond
        done.append(jnp.where(lanes <= base + subs, out, 0.0))
        ends = (t // GROUP + 1) * GROUP * ROWS
        outs.append((out, jnp.where((lanes < base + ROWS) | (lanes >= ends), out, 0.0)))
        if more:
            square = following
            tiles[t + 1] = ahead
        if t + 3 < min(count, (t // GROUP + 1) * GROUP + 1):
            back = [rows[p] * scaled[p] for p in range(ROWS)]
            for p in range(ROWS - 1, 0, -1):
                for q in range(p):
                    back[q] = back[q] - unit[p, q] * back[p]
            for u in range(t + 3, min(count, (t // GROUP + 1) * GROUP + 1)):
                old = tiles[u]
                new = jnp.where(here, 0.0, old)
                for p in range(ROWS):
                    new = new - across_lanes(old, base + p) * back[p]
                tiles[u] = new
        first = t + 1 + 1
        if (t + 1) % GROUP == 0 and first < count:
            high, low = halves(jnp.concatenate([o[0] for o in outs[t + 1 - GROUP :]], 0))
            rhigh, rlow = halves(jnp.concatenate([o[1] for o in outs[t + 1 - GROUP :]], 0))
            change = lax.dot_general(
                jnp.concatenate([high, high, low], 0),
                jnp.concatenate([rhigh, rlow, rhigh], 0),
                (((0,), (0,)), ((), ())),
                preferred_element_type=jnp.float32,
            )
            group = (lanes >= base + ROWS - GROUP * ROWS) & (lanes < base + ROWS)
            for u in range(first, count):
                tiles[u] = jnp.where(group, 0.0, tiles[u]) - change[u * ROWS : (u + 1) * ROWS]
    return done


def factor_steps(a_ref, diag_ref, diag_right, lower_ref, right_ref, early, midway):
    n = a_ref.shape[0]
    blocks = n // BLOCK
    wide = 2 * BLOCK
    diag_right[...] = jnp.zeros_like(diag_right)
    right_ref[...] = jnp.zeros_like(right_ref)

    def step(k, carry):
        pl.when(k == EARLY)(early)
        pl.when(k == MIDWAY)(midway)
        at = pl.ds(pl.multiple_of(k * BLOCK, BLOCK), BLOCK)
        before = pl.ds(pl.multiple_of(jnp.maximum(k - 1, 0) * BLOCK, BLOCK), BLOCK)
        after = pl.ds(pl.multiple_of(jnp.minimum(k + 1, blocks - 1) * BLOCK, BLOCK), BLOCK)
        base = pl.multiple_of(k * BLOCK, BLOCK)
        tiles = [a_ref[pl.ds(base + ROWS * t, ROWS), at] for t in range(BLOCK // ROWS)]

        for j in range(2, blocks):
            rows = slice(j * BLOCK, (j + 1) * BLOCK)
            on = jnp.where((j > k) & (k > 0), 1.0, 0.0).astype(jnp.float32)
            old = a_ref[rows, before]
            lower_ref[rows, :] = left_parts(dot_nt(left_parts(old), diag_right[...]) * on)
            a_ref[rows, before] = old * (1.0 - on)
        for c in range(n // wide):
            cols = slice(c * wide, (c + 1) * wide)
            for j in range(1, blocks // 2):
                rows = slice(j * wide, (j + 1) * wide)
                a_ref[rows, cols] -= jnp.dot(
                    lower_ref[rows, :], right_ref[:, cols], preferred_element_type=jnp.float32
                )
        for t, tile in enumerate(block_inverse(tiles)):
            diag_ref[ROWS * t : ROWS * (t + 1), :] = tile

        diag = diag_ref[...]
        a_ref[at, :] = jnp.dot(
            left_parts(diag), right_parts(a_ref[at, :], 0), preferred_element_type=jnp.float32
        )
        a_ref[at, at] = diag
        right_ref[...] = right_parts(a_ref[at, :], 0)
        diag_right[...] = right_parts(diag, 1)
        on = jnp.where(k < blocks - 1, 1.0, 0.0).astype(jnp.float32)
        old = a_ref[after, at]
        low = dot_nt(left_parts(old), diag_right[...]) * on
        a_ref[after, at] = old * (1.0 - on)
        a_ref[after, :] -= jnp.dot(left_parts(low), right_ref[...], preferred_element_type=jnp.float32)
        return carry

    lax.fori_loop(0, blocks, step, 0)


def gather_kernel(
    nx, nz, n_grid,
    basis_in, panel_in,
    coeffs_ref, panel_out_ref,
    basis_ref, panel_ref,
    others, lhs, rhs, part, from_core, from_x, from_z, gathered, own,
    removed, from_band, stacked, share, pieces_of,
    gram_ref, diag, diag_right, lower, right_parts_of, projected, projected_others,
    y_send, y_recv, send, recv, b_send, b_recv, g_send, z_recv, x_recv, g_recv, p_send, p_recv, io_sem,
):
    me = Place(nx, nz)
    fetch_panel = pltpu.make_async_copy(panel_in, panel_ref, io_sem.at[0])
    fetch_basis = pltpu.make_async_copy(basis_in, basis_ref, io_sem.at[1])
    fetch_panel.start()
    fetch_basis.start()
    me.barrier()
    nq, k = basis_ref.shape
    np_ = panel_ref.shape[0]
    pieces = nx * nz
    rq, rp = nq // pieces, np_ // pieces
    half = np_ // 2
    lo, hi = pl.ds(0, half), pl.ds(half, half)
    right = {"grid": me.grid, "band": lax.rem(me.band + 1, BANDS)}
    left = {"grid": me.grid, "band": lax.rem(me.band + BANDS - 1, BANDS)}

    def hop(i, src, dst, device):
        return remote(src, dst, y_send.at[i], y_recv.at[i], device)

    hops = [
        hop(0, panel_ref.at[lo], others.at[2, lo], right),
        hop(1, panel_ref.at[hi], others.at[0, hi], left),
        hop(2, panel_ref.at[hi], others.at[2, hi], right),
        hop(3, panel_ref.at[lo], others.at[0, lo], left),
        hop(4, others.at[2, lo], others.at[1, lo], right),
        hop(5, others.at[0, hi], others.at[1, hi], left),
    ]
    fetch_panel.wait()
    for h in hops[:4]:
        h.start()
    fetch_basis.wait()

    high, low = halves(basis_ref[...])
    lhs[:nq, :k] = high
    lhs[:nq, k : 2 * k] = high
    lhs[:nq, 2 * k :] = low
    high, low = halves(panel_ref[...])
    lhs[nq:, :k] = high
    lhs[nq:, k : 2 * k] = high
    lhs[nq:, 2 * k :] = low

    def multiply(q, tiles):
        for t, tile in enumerate(tiles):
            rows = slice(t * BLOCK, (t + 1) * BLOCK)
            high, low = halves(tile)
            rhs[rows, :k] = high
            rhs[rows, k : 2 * k] = low
            rhs[rows, 2 * k :] = high
        out = dot_nt(lhs[:nq, :], rhs[...])
        for t in range(2):
            part[q, t, :, :rq, :] = out[:, t * BLOCK : (t + 1) * BLOCK].reshape(pieces, rq, BLOCK)
        out = dot_nt(lhs[nq:, :], rhs[...])
        for t in range(2):
            part[q, t, :, rq:, :] = out[:, t * BLOCK : (t + 1) * BLOCK].reshape(pieces, rp, BLOCK)

    mine_x = pl.ds(me.x * nz, nz)

    def to_core(q):
        remote(
            part.at[q, 1 - me.core], from_core.at[q], send.at[0, q], recv.at[0, q], me.other_core()
        ).start()

    def to_x(q):
        await_bytes(from_core.at[q], recv.at[0, q])
        part[q, me.core] += from_core[q]
        for d, x, device in me.over_x():
            remote(
                part.at[q, me.core, pl.ds(x * nz, nz)],
                from_x.at[q, d],
                send.at[1, q],
                recv.at[1, q],
                device,
            ).start()

    def to_z(q):
        await_bytes(from_x.at[q], recv.at[1, q])
        total = part[q, me.core, mine_x]
        for d in range(nx - 1):
            total = total + from_x[q, d]
        part[q, me.core, mine_x] = total
        for d, z, device in me.over_z():
            remote(
                part.at[q, me.core, me.x * nz + z],
                from_z.at[q, d],
                send.at[2, q],
                recv.at[2, q],
                device,
            ).start()

    def back_z(q):
        await_bytes(from_z.at[q], recv.at[2, q])
        total = part[q, me.core, me.at]
        for d in range(nz - 1):
            total = total + from_z[q, d]
        total = total * (1.0 / n_grid)
        own[q] = total[rq:]
        gathered[q, me.core, me.at] = total[:rq]
        here = gathered.at[q, me.core, me.at]
        for _, _, device in me.over_z():
            remote(here, here, send.at[3, q], recv.at[3, q], device).start()

    def back_x(q):
        await_bytes(gathered.at[q, 0, pl.ds(0, nz - 1)], recv.at[3, q])
        here = gathered.at[q, me.core, mine_x]
        for _, _, device in me.over_x():
            remote(here, here, send.at[4, q], recv.at[4, q], device).start()

    def back_core(q):
        await_bytes(gathered.at[q, 0, pl.ds(0, (nx - 1) * nz)], recv.at[4, q])
        here = gathered.at[q, me.core]
        remote(here, here, send.at[5, q], recv.at[5, q], me.other_core()).start()

    def finish(q):
        await_bytes(gathered.at[q, 0], recv.at[5, q])
        for t in range(CORES):
            at = pl.multiple_of(tile_of(me.band, t, q) * BLOCK, BLOCK)
            coeffs_ref[:, pl.ds(at, BLOCK)] = gathered[q, t].reshape(nq, BLOCK)

    def remove(q):
        parts = [halves(gathered[q, t].reshape(nq, BLOCK).T) for t in range(CORES)]
        high = jnp.concatenate([p[0] for p in parts], 0)
        both = jnp.concatenate([high] + [p[1] for p in parts], 0)
        out = jnp.dot(both, lhs[:nq, :k], preferred_element_type=jnp.float32)
        out = out[: 2 * BLOCK] + out[2 * BLOCK :]
        out = out + jnp.dot(high, lhs[:nq, 2 * k :], preferred_element_type=jnp.float32)
        removed[q] = out.reshape(CORES, BLOCK, k)

    def bulk(i, src, dst, device):
        return remote(src, dst, b_send.at[i], b_recv.at[i], device)

    bulks = [
        bulk(0, removed.at[1, 0], from_band.at[2, 0], left),
        bulk(1, removed.at[1, 1], from_band.at[0, 1], right),
        bulk(2, removed.at[3, 0], from_band.at[1, 0], right),
        bulk(3, removed.at[3, 1], from_band.at[1, 1], left),
        bulk(4, removed.at[2, 0], from_band.at[0, 0], right),
        bulk(5, removed.at[2, 1], from_band.at[2, 1], left),
    ]

    multiply(0, (panel_ref[lo, :], panel_ref[hi, :]))
    to_core(0)
    to_x(0)
    to_z(0)
    hops[0].wait_recv()
    hops[4].start()
    hops[1].wait_recv()
    hops[5].start()
    multiply(1, (others[2, lo, :], others[0, hi, :]))
    to_core(1)
    back_z(0)
    to_x(1)
    back_x(0)
    to_z(1)
    hops[2].wait_recv()
    hops[3].wait_recv()
    multiply(2, (others[0, lo, :], others[2, hi, :]))
    to_core(2)
    back_z(1)
    back_core(0)
    to_x(2)
    hops[4].wait_recv()
    hops[5].wait_recv()
    multiply(3, (others[1, lo, :], others[1, hi, :]))
    to_core(3)
    to_z(2)
    to_x(3)
    back_x(1)
    finish(0)
    back_z(2)
    back_core(1)
    to_z(3)
    back_x(2)
    finish(1)
    remove(1)
    bulks[0].start()
    bulks[1].start()
    back_z(3)
    back_core(2)
    remove(0)
    finish(2)
    remove(2)
    back_x(3)
    back_core(3)
    for h in hops:
        h.wait_send()
    finish(3)

    high, low = halves(coeffs_ref[...])
    stacked[:nq, :] = high
    stacked[nq : 2 * nq, :] = low
    stacked[2 * nq :, :] = high
    n = coeffs_ref.shape[1]
    count = BANDS * rp
    row = lax.broadcasted_iota(jnp.int32, (count, n), 0)
    col = lax.broadcasted_iota(jnp.int32, (count, n), 1)
    want = lax.div(row, rp) * np_ + lax.rem(row, rp) + me.at * rp
    pick = jnp.where(col == want, 1.0, 0.0).astype(jnp.bfloat16)
    high = dot_nt(pick, stacked[:nq, :]).astype(jnp.bfloat16)
    low = dot_nt(pick, stacked[nq : 2 * nq, :]).astype(jnp.bfloat16)
    square = jnp.dot(
        jnp.concatenate([high, high, low], 1), stacked[...], preferred_element_type=jnp.float32
    )
    for band in range(BANDS):
        rows = square[band * rp : (band + 1) * rp]
        for i in range(KEPT):
            first = 2 * ((band + i) % BANDS) * BLOCK
            pair = [rows[:, first + t * BLOCK : first + (t + 1) * BLOCK] for t in range(CORES)]
            share[me.band, band, i] = -jnp.where(me.core == 0, pair[0], pair[1])
    for i, q in enumerate((0, 2 - me.core, ROUNDS - 1)):
        share[me.band, me.band, i] += own[q]
    for _, _, device in me.over_y():
        remote(share.at[me.band], share.at[me.band], g_send.at[0], g_recv.at[0], device).start()
    remove(3)
    bulks[2].start()
    bulks[3].start()
    await_bytes(share.at[pl.ds(0, BANDS - 1)], g_recv.at[0])
    pieces_of[me.core, me.x, me.z] = (share[0] + share[1]) + (share[2] + share[3])

    up, down = lax.rem(me.x + 1, nx), lax.rem(me.x + nx - 1, nx)
    to_up, to_down = me.id(me.z, up, me.core), me.id(me.z, down, me.core)
    first, second = pl.ds(0, BANDS // 2), pl.ds(BANDS // 2, BANDS // 2)

    def spread(i, z):
        here = pieces_of.at[me.core, me.x, z]
        remote(here, here, g_send.at[2], x_recv.at[0, i], to_up).start()
        remote(here, here, g_send.at[2], x_recv.at[1, i], to_down).start()

    def relay(i, z):
        await_bytes(pieces_of.at[0, 0, 0], x_recv.at[0, i])
        here = pieces_of.at[me.core, down, z, first]
        remote(here, here, g_send.at[3], g_recv.at[1], to_up).start()
        await_bytes(pieces_of.at[0, 0, 0], x_recv.at[1, i])
        here = pieces_of.at[me.core, up, z, second]
        remote(here, here, g_send.at[3], g_recv.at[1], to_down).start()

    def cross(x):
        here = pieces_of.at[me.core, x]
        remote(here, here, g_send.at[4], g_recv.at[2], me.other_core()).start()

    here = pieces_of.at[me.core, me.x, me.z]
    nearest = sorted(range(1, nz), key=lambda d: min(d, nz - d))
    for d in nearest:
        device = me.id(lax.rem(me.z + d, nz), me.x, me.core)
        remote(here, here, g_send.at[1], z_recv.at[d - 1], device).start()
    spread(0, me.z)
    order = [me.z]
    for i, d in enumerate(nearest):
        z = lax.rem(me.z + nz - d, nz)
        await_bytes(pieces_of.at[0, 0, 0], z_recv.at[d - 1])
        spread(i + 1, z)
        relay(i, order[i])
        order.append(z)
        if i == nz // 4:
            for t in range(CORES):
                bulks[2 + t].wait_recv()
                removed[2, t] += from_band[1, t]
                bulks[4 + t].start()
    cross(me.x)
    relay(nz - 1, order[nz - 1])
    cross(up)
    cross(down)
    await_bytes(pieces_of.at[0, 0], g_recv.at[1])
    cross(lax.rem(me.x + 2, nx))

    def place(core):
        for band in range(BANDS):
            for i in range(KEPT):
                at = (2 * ((band + i) % BANDS) + core) * BLOCK
                tile = pieces_of[core, :, :, band, i].reshape(np_, BLOCK)
                gram_ref[band * np_ : (band + 1) * np_, at : at + BLOCK] = tile
                if i == 1:
                    to = (2 * ((band + i) % BANDS) + core) * BLOCK
                    gram_ref[to : to + BLOCK, band * np_ : (band + 1) * np_] = tile.T

    await_bytes(pieces_of.at[0], g_recv.at[2])
    place(0)
    place(1)
    def carry(i, src, dst, device):
        return remote(src, dst, p_send.at[i], p_recv.at[i], device)

    carried = [
        carry(0, projected.at[lo], projected_others.at[2, lo], right),
        carry(1, projected.at[hi], projected_others.at[0, hi], left),
        carry(2, projected.at[hi], projected_others.at[2, hi], right),
        carry(3, projected.at[lo], projected_others.at[0, lo], left),
        carry(4, projected_others.at[2, lo], projected_others.at[1, lo], right),
        carry(5, projected_others.at[0, hi], projected_others.at[1, hi], left),
    ]
    def early():
        for i in (0, 1, 4, 5):
            bulks[i].wait_recv()
        for t in range(CORES):
            rows = slice(t * BLOCK, (t + 1) * BLOCK)
            total = removed[0, t] + (from_band[0, t] + from_band[2, t])
            projected[rows, :] = panel_ref[rows, :] - total
        for h in carried[:4]:
            h.start()

    def midway():
        carried[0].wait_recv()
        carried[4].start()
        carried[1].wait_recv()
        carried[5].start()

    factor_steps(gram_ref, diag, diag_right, lower, right_parts_of, early, midway)
    mine = pl.ds(pl.multiple_of(me.band * np_, np_), np_)
    row = lax.broadcasted_iota(jnp.int32, (np_, np_), 0) + me.band * np_
    col = lax.broadcasted_iota(jnp.int32, (np_, np_), 1)

    def times(r, block):
        first = lax.rem(me.band + r, BANDS) * np_
        tile = gram_ref[mine, pl.ds(pl.multiple_of(first, np_), np_)]
        tile = jnp.where(col + first <= row, tile, 0.0)
        return jnp.dot(
            left_parts(tile), right_parts(block, 0), preferred_element_type=jnp.float32
        )

    panel_out_ref[...] = times(0, projected[...])
    carried[2].wait_recv()
    carried[3].wait_recv()
    panel_out_ref[...] += times(1, projected_others[0])
    panel_out_ref[...] += times(3, projected_others[2])
    carried[4].wait_recv()
    carried[5].wait_recv()
    panel_out_ref[...] += times(2, projected_others[1])
    for h in carried:
        h.wait_send()

    for h in bulks:
        h.wait_send()
    for q in range(ROUNDS):
        await_bytes(from_core.at[q], send.at[0, q])
        await_bytes(from_x.at[q], send.at[1, q])
        await_bytes(from_z.at[q], send.at[2, q])
        await_bytes(gathered.at[q, 0, pl.ds(0, nz - 1)], send.at[3, q])
        await_bytes(gathered.at[q, 0, pl.ds(0, (nx - 1) * nz)], send.at[4, q])
        await_bytes(gathered.at[q, 0], send.at[5, q])
    await_bytes(share.at[pl.ds(0, BANDS - 1)], g_send.at[0])
    await_bytes(pieces_of.at[0, 0, pl.ds(0, nz - 1)], g_send.at[1])
    await_bytes(pieces_of.at[0, pl.ds(0, 2)], g_send.at[2])
    await_bytes(pieces_of.at[0, 0], g_send.at[3])
    await_bytes(pieces_of.at[0], g_send.at[4])


def reduce_and_project(nx, nz, n_grid, basis, panel):
    nq, k = basis.shape
    np_ = panel.shape[0]
    n = np_ * BANDS
    pieces = nx * nz
    rq, rp = nq // pieces, np_ // pieces
    f32 = jnp.float32
    dma = pltpu.SemaphoreType.DMA
    return pl.pallas_call(
        functools.partial(gather_kernel, nx, nz, n_grid),
        out_shape=(
            jax.ShapeDtypeStruct((nq, n), f32),
            jax.ShapeDtypeStruct((np_, k), f32),
        ),
        in_specs=[pl.BlockSpec(memory_space=pltpu.HBM)] * 2,
        out_specs=(pl.BlockSpec(memory_space=pltpu.VMEM),) * 2,
        scratch_shapes=[
            pltpu.VMEM((nq, k), f32),
            pltpu.VMEM((np_, k), f32),
            pltpu.VMEM((BANDS - 1, np_, k), f32),
            pltpu.VMEM((nq + np_, 3 * k), jnp.bfloat16),
            pltpu.VMEM((2 * BLOCK, 3 * k), jnp.bfloat16),
            pltpu.VMEM((ROUNDS, CORES, pieces, rq + rp, BLOCK), f32),
            pltpu.VMEM((ROUNDS, pieces, rq + rp, BLOCK), f32),
            pltpu.VMEM((ROUNDS, nx - 1, nz, rq + rp, BLOCK), f32),
            pltpu.VMEM((ROUNDS, nz - 1, rq + rp, BLOCK), f32),
            pltpu.VMEM((ROUNDS, CORES, pieces, rq, BLOCK), f32),
            pltpu.VMEM((ROUNDS, rp, BLOCK), f32),
            pltpu.VMEM((ROUNDS, CORES, BLOCK, k), f32),
            pltpu.VMEM((BANDS - 1, CORES, BLOCK, k), f32),
            pltpu.VMEM((3 * nq, n), jnp.bfloat16),
            pltpu.VMEM((BANDS, BANDS, KEPT, rp, BLOCK), f32),
            pltpu.VMEM((CORES, nx, nz, BANDS, KEPT, rp, BLOCK), f32),
            pltpu.VMEM((n, n), f32),
            pltpu.VMEM((BLOCK, BLOCK), f32),
            pltpu.VMEM((BLOCK, 3 * BLOCK), jnp.bfloat16),
            pltpu.VMEM((n, 3 * BLOCK), jnp.bfloat16),
            pltpu.VMEM((3 * BLOCK, n), jnp.bfloat16),
            pltpu.VMEM((np_, k), f32),
            pltpu.VMEM((BANDS - 1, np_, k), f32),
            dma((6,)),
            dma((6,)),
            dma((6, ROUNDS)),
            dma((6, ROUNDS)),
            dma((6,)),
            dma((6,)),
            dma((5,)),
            dma((nz - 1,)),
            dma((2, nz)),
            dma((3,)),
            dma((6,)),
            dma((6,)),
            dma((2,)),
        ],
        compiler_params=pltpu.CompilerParams(
            collective_id=0, has_side_effects=True, vmem_limit_bytes=48 * 1024 * 1024
        ),
        cost_estimate=pl.CostEstimate(
            flops=60 * 1024**3, bytes_accessed=8 * 1024 * 1024, transcendentals=0
        ),
    )(basis, panel)


def body(basis, panel):
    grid = lax.axis_size("grid")
    nz = grid // (CORES * ALONG_X)
    coeffs, new_panel = reduce_and_project(
        ALONG_X, nz, panel.shape[1] * grid, basis, panel
    )
    return (new_panel, coeffs)


def solution(mesh):
    placed = (P("band", "grid"), P("band", "grid"))
    return jax.shard_map(
        body,
        mesh=mesh,
        in_specs=placed,
        out_specs=(P("band", "grid"), P("band", None)),
        check_vma=False,
    )
```

```python
import functools

import jax
import jax.numpy as jnp
from jax import lax
from jax.experimental import pallas as pl
from jax.experimental.pallas import tpu as pltpu
from jax.sharding import PartitionSpec as P

BLOCK = 128
ROWS = 8
CORES = 2
BANDS = 4
ROUNDS = 4
KEPT = 3
GROUP = 4
EARLY = 0
MIDWAY = 4
ALONG_X = 4
MESH = pl.DeviceIdType.MESH


def halves(x):
    high = x.astype(jnp.bfloat16)
    low = (x - high.astype(jnp.float32)).astype(jnp.bfloat16)
    return high, low


def left_parts(x):
    high, low = halves(x)
    return jnp.concatenate([high, high, low], 1)


def right_parts(x, axis):
    high, low = halves(x)
    return jnp.concatenate([high, low, high], axis)


def dot_nt(left, right):
    return lax.dot_general(
        left, right, (((1,), (1,)), ((), ())), preferred_element_type=jnp.float32
    )


def tile_of(band, core, turn):
    one, two, three = (lax.rem(band + i, BANDS) for i in (1, 2, 3))
    if turn == 0:
        return 2 * band + core
    if turn == 1:
        return 2 * (three + core * (one - three)) + core
    if turn == 2:
        return 2 * (one + core * (three - one)) + core
    return 2 * two + core


class Place:
    def __init__(self, nx, nz):
        self.nx, self.nz = nx, nz
        self.grid = lax.axis_index("grid")
        self.band = lax.axis_index("band")
        self.core = lax.rem(self.grid, CORES)
        self.x = lax.rem(lax.div(self.grid, CORES), nx)
        self.z = lax.div(self.grid, CORES * nx)
        self.at = self.x * nz + self.z

    def id(self, z, x, core):
        return {"grid": (z * self.nx + x) * CORES + core, "band": self.band}

    def other_core(self):
        return self.id(self.z, self.x, 1 - self.core)

    def over_x(self):
        for d in range(1, self.nx):
            x = lax.rem(self.x + d, self.nx)
            yield d - 1, x, self.id(self.z, x, self.core)

    def over_z(self):
        for d in range(1, self.nz):
            z = lax.rem(self.z + d, self.nz)
            yield d - 1, z, self.id(z, self.x, self.core)

    def over_y(self):
        for d in range(1, BANDS):
            band = lax.rem(self.band + d, BANDS)
            yield d - 1, band, {"grid": self.grid, "band": band}

    def barrier(self):
        sem = pltpu.get_barrier_semaphore()
        ids = [self.other_core()]
        ids += [i for _, _, i in self.over_x()]
        ids += [i for _, _, i in self.over_z()]
        ids += [i for _, _, i in self.over_y()]
        for i in ids:
            pl.semaphore_signal(sem, inc=1, device_id=i, device_id_type=MESH)
        pl.semaphore_wait(sem, len(ids))


def remote(src, dst, send, recv, device):
    return pltpu.make_async_remote_copy(
        src_ref=src,
        dst_ref=dst,
        send_sem=send,
        recv_sem=recv,
        device_id=device,
        device_id_type=MESH,
    )


def await_bytes(ref, sem):
    pltpu.make_async_copy(ref, ref, sem).wait()


def across_lanes(tile, lane):
    return jnp.broadcast_to(tile[:, lane : lane + 1], (ROWS, BLOCK))


def down_rows(tile, row):
    return jnp.broadcast_to(tile[row : row + 1, :], (ROWS, BLOCK))


def block_inverse(tiles):
    lanes = lax.broadcasted_iota(jnp.int32, (ROWS, BLOCK), 1)
    subs = lax.broadcasted_iota(jnp.int32, (ROWS, BLOCK), 0)
    tiles = list(tiles)
    count = len(tiles)
    done = []
    outs = []
    square = [across_lanes(tiles[0], q) for q in range(ROWS)]
    for t in range(count):
        base = ROWS * t
        here = (lanes >= base) & (lanes < base + ROWS)
        more = t + 1 < count
        if more:
            ahead = tiles[t + 1]
            side = [across_lanes(ahead, base + q) for q in range(ROWS)]
            following = [across_lanes(ahead, base + ROWS + q) for q in range(ROWS)]
        far = t + 2 < min(count, (t // GROUP + 1) * GROUP + 1)
        if far:
            beyond = tiles[t + 2]
            wing = [across_lanes(beyond, base + q) for q in range(ROWS)]
        current = jnp.where(here, jnp.where(lanes - base == subs, 1.0, 0.0), tiles[t])
        rows, scaled, unit = [], [], {}
        out = None
        for q in range(ROWS):
            root = lax.rsqrt(down_rows(square[q], q))
            inv = root * root
            scaled.append(inv)
            row = down_rows(current, q)
            rows.append(row)
            out = row * root if q == 0 else jnp.where(subs == q, row * root, out)
            if q + 1 < ROWS:
                current = current - (square[q] * inv) * row
            for s in range(q + 1, ROWS):
                unit[s, q] = down_rows(square[q], s) * inv
                square[s] = square[s] - unit[s, q] * square[q]
            if far:
                for s in range(q + 1, ROWS):
                    wing[s] = wing[s] - unit[s, q] * wing[q]
                beyond = (jnp.where(here, 0.0, beyond) if q == 0 else beyond) - (wing[q] * inv) * row
            if more:
                weight = side[q] * inv
                for s in range(q + 1, ROWS):
                    side[s] = side[s] - unit[s, q] * side[q]
                for s in range(ROWS):
                    following[s] = following[s] - weight * down_rows(side[q], s)
                ahead = (jnp.where(here, 0.0, ahead) if q == 0 else ahead) - weight * row
        if far:
            tiles[t + 2] = beyond
        done.append(jnp.where(lanes <= base + subs, out, 0.0))
        ends = (t // GROUP + 1) * GROUP * ROWS
        outs.append((out, jnp.where((lanes < base + ROWS) | (lanes >= ends), out, 0.0)))
        if more:
            square = following
            tiles[t + 1] = ahead
        if t + 3 < min(count, (t // GROUP + 1) * GROUP + 1):
            back = [rows[p] * scaled[p] for p in range(ROWS)]
            for p in range(ROWS - 1, 0, -1):
                for q in range(p):
                    back[q] = back[q] - unit[p, q] * back[p]
            for u in range(t + 3, min(count, (t // GROUP + 1) * GROUP + 1)):
                old = tiles[u]
                new = jnp.where(here, 0.0, old)
                for p in range(ROWS):
                    new = new - across_lanes(old, base + p) * back[p]
                tiles[u] = new
        first = t + 1 + 1
        if (t + 1) % GROUP == 0 and first < count:
            high, low = halves(jnp.concatenate([o[0] for o in outs[t + 1 - GROUP :]], 0))
            rhigh, rlow = halves(jnp.concatenate([o[1] for o in outs[t + 1 - GROUP :]], 0))
            change = lax.dot_general(
                jnp.concatenate([high, high, low], 0),
                jnp.concatenate([rhigh, rlow, rhigh], 0),
                (((0,), (0,)), ((), ())),
                preferred_element_type=jnp.float32,
            )
            group = (lanes >= base + ROWS - GROUP * ROWS) & (lanes < base + ROWS)
            for u in range(first, count):
                tiles[u] = jnp.where(group, 0.0, tiles[u]) - change[u * ROWS : (u + 1) * ROWS]
    return done


def factor_steps(a_ref, diag_ref, diag_right, lower_ref, right_ref, early, midway):
    n = a_ref.shape[0]
    blocks = n // BLOCK
    wide = 2 * BLOCK
    diag_right[...] = jnp.zeros_like(diag_right)
    right_ref[...] = jnp.zeros_like(right_ref)

    def step(k, carry):
        pl.when(k == EARLY)(early)
        pl.when(k == MIDWAY)(midway)
        at = pl.ds(pl.multiple_of(k * BLOCK, BLOCK), BLOCK)
        before = pl.ds(pl.multiple_of(jnp.maximum(k - 1, 0) * BLOCK, BLOCK), BLOCK)
        after = pl.ds(pl.multiple_of(jnp.minimum(k + 1, blocks - 1) * BLOCK, BLOCK), BLOCK)
        base = pl.multiple_of(k * BLOCK, BLOCK)
        tiles = [a_ref[pl.ds(base + ROWS * t, ROWS), at] for t in range(BLOCK // ROWS)]

        for j in range(2, blocks):
            rows = slice(j * BLOCK, (j + 1) * BLOCK)
            on = jnp.where((j > k) & (k > 0), 1.0, 0.0).astype(jnp.float32)
            old = a_ref[rows, before]
            lower_ref[rows, :] = left_parts(dot_nt(left_parts(old), diag_right[...]) * on)
            a_ref[rows, before] = old * (1.0 - on)
        for c in range(n // wide):
            cols = slice(c * wide, (c + 1) * wide)
            for j in range(1, blocks // 2):
                rows = slice(j * wide, (j + 1) * wide)
                a_ref[rows, cols] -= jnp.dot(
                    lower_ref[rows, :], right_ref[:, cols], preferred_element_type=jnp.float32
                )
        for t, tile in enumerate(block_inverse(tiles)):
            diag_ref[ROWS * t : ROWS * (t + 1), :] = tile

        diag = diag_ref[...]
        a_ref[at, :] = jnp.dot(
            left_parts(diag), right_parts(a_ref[at, :], 0), preferred_element_type=jnp.float32
        )
        a_ref[at, at] = diag
        right_ref[...] = right_parts(a_ref[at, :], 0)
        diag_right[...] = right_parts(diag, 1)
        on = jnp.where(k < blocks - 1, 1.0, 0.0).astype(jnp.float32)
        old = a_ref[after, at]
        low = dot_nt(left_parts(old), diag_right[...]) * on
        a_ref[after, at] = old * (1.0 - on)
        a_ref[after, :] -= jnp.dot(left_parts(low), right_ref[...], preferred_element_type=jnp.float32)
        return carry

    lax.fori_loop(0, blocks, step, 0)


def gather_kernel(
    nx, nz, n_grid,
    basis_in, panel_in,
    coeffs_ref, panel_out_ref,
    basis_ref, panel_ref,
    others, lhs, rhs, part, from_core, from_x, from_z, gathered, own,
    removed, from_band, stacked, share, pieces_of,
    gram_ref, diag, diag_right, lower, right_parts_of, projected, projected_others,
    y_send, y_recv, send, recv, b_send, b_recv, g_send, z_recv, x_recv, g_recv, p_send, p_recv, io_sem,
):
    me = Place(nx, nz)
    fetch_panel = pltpu.make_async_copy(panel_in, panel_ref, io_sem.at[0])
    fetch_basis = pltpu.make_async_copy(basis_in, basis_ref, io_sem.at[1])
    fetch_panel.start()
    fetch_basis.start()
    me.barrier()
    nq, k = basis_ref.shape
    np_ = panel_ref.shape[0]
    pieces = nx * nz
    rq, rp = nq // pieces, np_ // pieces
    half = np_ // 2
    lo, hi = pl.ds(0, half), pl.ds(half, half)
    right = {"grid": me.grid, "band": lax.rem(me.band + 1, BANDS)}
    left = {"grid": me.grid, "band": lax.rem(me.band + BANDS - 1, BANDS)}

    def hop(i, src, dst, device):
        return remote(src, dst, y_send.at[i], y_recv.at[i], device)

    hops = [
        hop(0, panel_ref.at[lo], others.at[2, lo], right),
        hop(1, panel_ref.at[hi], others.at[0, hi], left),
        hop(2, panel_ref.at[hi], others.at[2, hi], right),
        hop(3, panel_ref.at[lo], others.at[0, lo], left),
        hop(4, others.at[2, lo], others.at[1, lo], right),
        hop(5, others.at[0, hi], others.at[1, hi], left),
    ]
    fetch_panel.wait()
    for h in hops[:4]:
        h.start()
    fetch_basis.wait()

    high, low = halves(basis_ref[...])
    lhs[:nq, :k] = high
    lhs[:nq, k : 2 * k] = high
    lhs[:nq, 2 * k :] = low
    high, low = halves(panel_ref[...])
    lhs[nq:, :k] = high
    lhs[nq:, k : 2 * k] = high
    lhs[nq:, 2 * k :] = low

    def multiply(q, tiles):
        for t, tile in enumerate(tiles):
            rows = slice(t * BLOCK, (t + 1) * BLOCK)
            high, low = halves(tile)
            rhs[rows, :k] = high
            rhs[rows, k : 2 * k] = low
            rhs[rows, 2 * k :] = high
        out = dot_nt(lhs[:nq, :], rhs[...])
        for t in range(2):
            part[q, t, :, :rq, :] = out[:, t * BLOCK : (t + 1) * BLOCK].reshape(pieces, rq, BLOCK)
        out = dot_nt(lhs[nq:, :], rhs[...])
        for t in range(2):
            part[q, t, :, rq:, :] = out[:, t * BLOCK : (t + 1) * BLOCK].reshape(pieces, rp, BLOCK)

    mine_x = pl.ds(me.x * nz, nz)

    def to_core(q):
        remote(
            part.at[q, 1 - me.core], from_core.at[q], send.at[0, q], recv.at[0, q], me.other_core()
        ).start()

    def to_x(q):
        await_bytes(from_core.at[q], recv.at[0, q])
        part[q, me.core] += from_core[q]
        for d, x, device in me.over_x():
            remote(
                part.at[q, me.core, pl.ds(x * nz, nz)],
                from_x.at[q, d],
                send.at[1, q],
                recv.at[1, q],
                device,
            ).start()

    def to_z(q):
        await_bytes(from_x.at[q], recv.at[1, q])
        total = part[q, me.core, mine_x]
        for d in range(nx - 1):
            total = total + from_x[q, d]
        part[q, me.core, mine_x] = total
        for d, z, device in me.over_z():
            remote(
                part.at[q, me.core, me.x * nz + z],
                from_z.at[q, d],
                send.at[2, q],
                recv.at[2, q],
                device,
            ).start()

    def back_z(q):
        await_bytes(from_z.at[q], recv.at[2, q])
        total = part[q, me.core, me.at]
        for d in range(nz - 1):
            total = total + from_z[q, d]
        total = total * (1.0 / n_grid)
        own[q] = total[rq:]
        gathered[q, me.core, me.at] = total[:rq]
        here = gathered.at[q, me.core, me.at]
        for _, _, device in me.over_z():
            remote(here, here, send.at[3, q], recv.at[3, q], device).start()

    def back_x(q):
        await_bytes(gathered.at[q, 0, pl.ds(0, nz - 1)], recv.at[3, q])
        here = gathered.at[q, me.core, mine_x]
        for _, _, device in me.over_x():
            remote(here, here, send.at[4, q], recv.at[4, q], device).start()

    def back_core(q):
        await_bytes(gathered.at[q, 0, pl.ds(0, (nx - 1) * nz)], recv.at[4, q])
        here = gathered.at[q, me.core]
        remote(here, here, send.at[5, q], recv.at[5, q], me.other_core()).start()

    def finish(q):
        await_bytes(gathered.at[q, 0], recv.at[5, q])
        for t in range(CORES):
            at = pl.multiple_of(tile_of(me.band, t, q) * BLOCK, BLOCK)
            coeffs_ref[:, pl.ds(at, BLOCK)] = gathered[q, t].reshape(nq, BLOCK)

    def remove(q):
        parts = [halves(gathered[q, t].reshape(nq, BLOCK).T) for t in range(CORES)]
        high = jnp.concatenate([p[0] for p in parts], 0)
        both = jnp.concatenate([high] + [p[1] for p in parts], 0)
        out = jnp.dot(both, lhs[:nq, :k], preferred_element_type=jnp.float32)
        out = out[: 2 * BLOCK] + out[2 * BLOCK :]
        out = out + jnp.dot(high, lhs[:nq, 2 * k :], preferred_element_type=jnp.float32)
        removed[q] = out.reshape(CORES, BLOCK, k)

    def bulk(i, src, dst, device):
        return remote(src, dst, b_send.at[i], b_recv.at[i], device)

    bulks = [
        bulk(0, removed.at[1, 0], from_band.at[2, 0], left),
        bulk(1, removed.at[1, 1], from_band.at[0, 1], right),
        bulk(2, removed.at[3, 0], from_band.at[1, 0], right),
        bulk(3, removed.at[3, 1], from_band.at[1, 1], left),
        bulk(4, removed.at[2, 0], from_band.at[0, 0], right),
        bulk(5, removed.at[2, 1], from_band.at[2, 1], left),
    ]

    multiply(0, (panel_ref[lo, :], panel_ref[hi, :]))
    to_core(0)
    to_x(0)
    to_z(0)
    hops[0].wait_recv()
    hops[4].start()
    hops[1].wait_recv()
    hops[5].start()
    multiply(1, (others[2, lo, :], others[0, hi, :]))
    to_core(1)
    back_z(0)
    to_x(1)
    back_x(0)
    to_z(1)
    hops[2].wait_recv()
    hops[3].wait_recv()
    multiply(2, (others[0, lo, :], others[2, hi, :]))
    to_core(2)
    back_z(1)
    back_core(0)
    to_x(2)
    hops[4].wait_recv()
    hops[5].wait_recv()
    multiply(3, (others[1, lo, :], others[1, hi, :]))
    to_core(3)
    to_z(2)
    to_x(3)
    back_x(1)
    finish(0)
    back_z(2)
    to_z(3)
    back_core(1)
    back_x(2)
    back_z(3)
    finish(1)
    remove(1)
    bulks[0].start()
    bulks[1].start()
    back_core(2)
    back_x(3)
    remove(0)
    finish(2)
    remove(2)
    back_core(3)
    for h in hops:
        h.wait_send()
    finish(3)

    high, low = halves(coeffs_ref[...])
    stacked[:nq, :] = high
    stacked[nq : 2 * nq, :] = low
    stacked[2 * nq :, :] = high
    n = coeffs_ref.shape[1]
    count = BANDS * rp
    row = lax.broadcasted_iota(jnp.int32, (count, n), 0)
    col = lax.broadcasted_iota(jnp.int32, (count, n), 1)
    want = lax.div(row, rp) * np_ + lax.rem(row, rp) + me.at * rp
    pick = jnp.where(col == want, 1.0, 0.0).astype(jnp.bfloat16)
    high = dot_nt(pick, stacked[:nq, :]).astype(jnp.bfloat16)
    low = dot_nt(pick, stacked[nq : 2 * nq, :]).astype(jnp.bfloat16)
    square = jnp.dot(
        jnp.concatenate([high, high, low], 1), stacked[...], preferred_element_type=jnp.float32
    )
    for band in range(BANDS):
        rows = square[band * rp : (band + 1) * rp]
        for i in range(KEPT):
            first = 2 * ((band + i) % BANDS) * BLOCK
            pair = [rows[:, first + t * BLOCK : first + (t + 1) * BLOCK] for t in range(CORES)]
            share[me.band, band, i] = -jnp.where(me.core == 0, pair[0], pair[1])
    for i, q in enumerate((0, 2 - me.core, ROUNDS - 1)):
        share[me.band, me.band, i] += own[q]
    for _, _, device in me.over_y():
        remote(share.at[me.band], share.at[me.band], g_send.at[0], g_recv.at[0], device).start()
    remove(3)
    bulks[2].start()
    bulks[3].start()
    await_bytes(share.at[pl.ds(0, BANDS - 1)], g_recv.at[0])
    pieces_of[me.core, me.x, me.z] = (share[0] + share[1]) + (share[2] + share[3])

    up, down = lax.rem(me.x + 1, nx), lax.rem(me.x + nx - 1, nx)
    to_up, to_down = me.id(me.z, up, me.core), me.id(me.z, down, me.core)
    first, second = pl.ds(0, BANDS // 2), pl.ds(BANDS // 2, BANDS // 2)

    def spread(i, z):
        here = pieces_of.at[me.core, me.x, z]
        remote(here, here, g_send.at[2], x_recv.at[0, i], to_up).start()
        remote(here, here, g_send.at[2], x_recv.at[1, i], to_down).start()

    def relay(i, z):
        await_bytes(pieces_of.at[0, 0, 0], x_recv.at[0, i])
        here = pieces_of.at[me.core, down, z, first]
        remote(here, here, g_send.at[3], g_recv.at[1], to_up).start()
        await_bytes(pieces_of.at[0, 0, 0], x_recv.at[1, i])
        here = pieces_of.at[me.core, up, z, second]
        remote(here, here, g_send.at[3], g_recv.at[1], to_down).start()

    def cross(x):
        here = pieces_of.at[me.core, x]
        remote(here, here, g_send.at[4], g_recv.at[2], me.other_core()).start()

    here = pieces_of.at[me.core, me.x, me.z]
    nearest = sorted(range(1, nz), key=lambda d: min(d, nz - d))
    for d in nearest:
        device = me.id(lax.rem(me.z + d, nz), me.x, me.core)
        remote(here, here, g_send.at[1], z_recv.at[d - 1], device).start()
    spread(0, me.z)
    order = [me.z]
    for i, d in enumerate(nearest):
        z = lax.rem(me.z + nz - d, nz)
        await_bytes(pieces_of.at[0, 0, 0], z_recv.at[d - 1])
        spread(i + 1, z)
        relay(i, order[i])
        order.append(z)
        if i == nz // 4:
            for t in range(CORES):
                bulks[2 + t].wait_recv()
                removed[2, t] += from_band[1, t]
                bulks[4 + t].start()
    cross(me.x)
    relay(nz - 1, order[nz - 1])
    cross(up)
    cross(down)
    await_bytes(pieces_of.at[0, 0], g_recv.at[1])
    cross(lax.rem(me.x + 2, nx))

    def place(core):
        for band in range(BANDS):
            for i in range(KEPT):
                at = (2 * ((band + i) % BANDS) + core) * BLOCK
                tile = pieces_of[core, :, :, band, i].reshape(np_, BLOCK)
                gram_ref[band * np_ : (band + 1) * np_, at : at + BLOCK] = tile
                if i == 1:
                    to = (2 * ((band + i) % BANDS) + core) * BLOCK
                    gram_ref[to : to + BLOCK, band * np_ : (band + 1) * np_] = tile.T

    await_bytes(pieces_of.at[0], g_recv.at[2])
    place(0)
    place(1)
    def carry(i, src, dst, device):
        return remote(src, dst, p_send.at[i], p_recv.at[i], device)

    carried = [
        carry(0, projected.at[lo], projected_others.at[2, lo], right),
        carry(1, projected.at[hi], projected_others.at[0, hi], left),
        carry(2, projected.at[hi], projected_others.at[2, hi], right),
        carry(3, projected.at[lo], projected_others.at[0, lo], left),
        carry(4, projected_others.at[2, lo], projected_others.at[1, lo], right),
        carry(5, projected_others.at[0, hi], projected_others.at[1, hi], left),
    ]
    def early():
        for i in (0, 1, 4, 5):
            bulks[i].wait_recv()
        for t in range(CORES):
            rows = slice(t * BLOCK, (t + 1) * BLOCK)
            total = removed[0, t] + (from_band[0, t] + from_band[2, t])
            projected[rows, :] = panel_ref[rows, :] - total
        for h in carried[:4]:
            h.start()

    def midway():
        carried[0].wait_recv()
        carried[4].start()
        carried[1].wait_recv()
        carried[5].start()

    factor_steps(gram_ref, diag, diag_right, lower, right_parts_of, early, midway)
    mine = pl.ds(pl.multiple_of(me.band * np_, np_), np_)
    row = lax.broadcasted_iota(jnp.int32, (np_, np_), 0) + me.band * np_
    col = lax.broadcasted_iota(jnp.int32, (np_, np_), 1)

    def times(r, block):
        first = lax.rem(me.band + r, BANDS) * np_
        tile = gram_ref[mine, pl.ds(pl.multiple_of(first, np_), np_)]
        tile = jnp.where(col + first <= row, tile, 0.0)
        return jnp.dot(
            left_parts(tile), right_parts(block, 0), preferred_element_type=jnp.float32
        )

    panel_out_ref[...] = times(0, projected[...])
    carried[2].wait_recv()
    carried[3].wait_recv()
    panel_out_ref[...] += times(1, projected_others[0])
    panel_out_ref[...] += times(3, projected_others[2])
    carried[4].wait_recv()
    carried[5].wait_recv()
    panel_out_ref[...] += times(2, projected_others[1])
    for h in carried:
        h.wait_send()

    for h in bulks:
        h.wait_send()
    for q in range(ROUNDS):
        await_bytes(from_core.at[q], send.at[0, q])
        await_bytes(from_x.at[q], send.at[1, q])
        await_bytes(from_z.at[q], send.at[2, q])
        await_bytes(gathered.at[q, 0, pl.ds(0, nz - 1)], send.at[3, q])
        await_bytes(gathered.at[q, 0, pl.ds(0, (nx - 1) * nz)], send.at[4, q])
        await_bytes(gathered.at[q, 0], send.at[5, q])
    await_bytes(share.at[pl.ds(0, BANDS - 1)], g_send.at[0])
    await_bytes(pieces_of.at[0, 0, pl.ds(0, nz - 1)], g_send.at[1])
    await_bytes(pieces_of.at[0, pl.ds(0, 2)], g_send.at[2])
    await_bytes(pieces_of.at[0, 0], g_send.at[3])
    await_bytes(pieces_of.at[0], g_send.at[4])


def reduce_and_project(nx, nz, n_grid, basis, panel):
    nq, k = basis.shape
    np_ = panel.shape[0]
    n = np_ * BANDS
    pieces = nx * nz
    rq, rp = nq // pieces, np_ // pieces
    f32 = jnp.float32
    dma = pltpu.SemaphoreType.DMA
    return pl.pallas_call(
        functools.partial(gather_kernel, nx, nz, n_grid),
        out_shape=(
            jax.ShapeDtypeStruct((nq, n), f32),
            jax.ShapeDtypeStruct((np_, k), f32),
        ),
        in_specs=[pl.BlockSpec(memory_space=pltpu.HBM)] * 2,
        out_specs=(pl.BlockSpec(memory_space=pltpu.VMEM),) * 2,
        scratch_shapes=[
            pltpu.VMEM((nq, k), f32),
            pltpu.VMEM((np_, k), f32),
            pltpu.VMEM((BANDS - 1, np_, k), f32),
            pltpu.VMEM((nq + np_, 3 * k), jnp.bfloat16),
            pltpu.VMEM((2 * BLOCK, 3 * k), jnp.bfloat16),
            pltpu.VMEM((ROUNDS, CORES, pieces, rq + rp, BLOCK), f32),
            pltpu.VMEM((ROUNDS, pieces, rq + rp, BLOCK), f32),
            pltpu.VMEM((ROUNDS, nx - 1, nz, rq + rp, BLOCK), f32),
            pltpu.VMEM((ROUNDS, nz - 1, rq + rp, BLOCK), f32),
            pltpu.VMEM((ROUNDS, CORES, pieces, rq, BLOCK), f32),
            pltpu.VMEM((ROUNDS, rp, BLOCK), f32),
            pltpu.VMEM((ROUNDS, CORES, BLOCK, k), f32),
            pltpu.VMEM((BANDS - 1, CORES, BLOCK, k), f32),
            pltpu.VMEM((3 * nq, n), jnp.bfloat16),
            pltpu.VMEM((BANDS, BANDS, KEPT, rp, BLOCK), f32),
            pltpu.VMEM((CORES, nx, nz, BANDS, KEPT, rp, BLOCK), f32),
            pltpu.VMEM((n, n), f32),
            pltpu.VMEM((BLOCK, BLOCK), f32),
            pltpu.VMEM((BLOCK, 3 * BLOCK), jnp.bfloat16),
            pltpu.VMEM((n, 3 * BLOCK), jnp.bfloat16),
            pltpu.VMEM((3 * BLOCK, n), jnp.bfloat16),
            pltpu.VMEM((np_, k), f32),
            pltpu.VMEM((BANDS - 1, np_, k), f32),
            dma((6,)),
            dma((6,)),
            dma((6, ROUNDS)),
            dma((6, ROUNDS)),
            dma((6,)),
            dma((6,)),
            dma((5,)),
            dma((nz - 1,)),
            dma((2, nz)),
            dma((3,)),
            dma((6,)),
            dma((6,)),
            dma((2,)),
        ],
        compiler_params=pltpu.CompilerParams(
            collective_id=0, has_side_effects=True, vmem_limit_bytes=48 * 1024 * 1024
        ),
        cost_estimate=pl.CostEstimate(
            flops=60 * 1024**3, bytes_accessed=8 * 1024 * 1024, transcendentals=0
        ),
    )(basis, panel)


def body(basis, panel):
    grid = lax.axis_size("grid")
    nz = grid // (CORES * ALONG_X)
    coeffs, new_panel = reduce_and_project(
        ALONG_X, nz, panel.shape[1] * grid, basis, panel
    )
    return (new_panel, coeffs)


def solution(mesh):
    placed = (P("band", "grid"), P("band", "grid"))
    return jax.shard_map(
        body,
        mesh=mesh,
        in_specs=placed,
        out_specs=(P("band", "grid"), P("band", None)),
        check_vma=False,
    )
```

```python
import functools

import jax
import jax.numpy as jnp
from jax import lax
from jax.experimental import pallas as pl
from jax.experimental.pallas import tpu as pltpu
from jax.sharding import PartitionSpec as P

BLOCK = 128
ROWS = 8
CORES = 2
BANDS = 4
ROUNDS = 4
KEPT = 3
GROUP = 4
LATE = (1, 3)
MIDWAY = 4
ALONG_X = 4
MESH = pl.DeviceIdType.MESH


def halves(x):
    high = x.astype(jnp.bfloat16)
    low = (x - high.astype(jnp.float32)).astype(jnp.bfloat16)
    return high, low


def left_parts(x):
    high, low = halves(x)
    return jnp.concatenate([high, high, low], 1)


def right_parts(x, axis):
    high, low = halves(x)
    return jnp.concatenate([high, low, high], axis)


def dot_nt(left, right):
    return lax.dot_general(
        left, right, (((1,), (1,)), ((), ())), preferred_element_type=jnp.float32
    )


def tile_of(band, core, turn):
    one, two, three = (lax.rem(band + i, BANDS) for i in (1, 2, 3))
    if turn == 0:
        return 2 * band + core
    if turn == 1:
        return 2 * (three + core * (one - three)) + core
    if turn == 2:
        return 2 * (one + core * (three - one)) + core
    return 2 * two + core


class Place:
    def __init__(self, nx, nz):
        self.nx, self.nz = nx, nz
        self.grid = lax.axis_index("grid")
        self.band = lax.axis_index("band")
        self.core = lax.rem(self.grid, CORES)
        self.x = lax.rem(lax.div(self.grid, CORES), nx)
        self.z = lax.div(self.grid, CORES * nx)
        self.at = self.x * nz + self.z

    def id(self, z, x, core):
        return {"grid": (z * self.nx + x) * CORES + core, "band": self.band}

    def other_core(self):
        return self.id(self.z, self.x, 1 - self.core)

    def over_x(self):
        for d in range(1, self.nx):
            x = lax.rem(self.x + d, self.nx)
            yield d - 1, x, self.id(self.z, x, self.core)

    def over_z(self):
        for d in range(1, self.nz):
            z = lax.rem(self.z + d, self.nz)
            yield d - 1, z, self.id(z, self.x, self.core)

    def over_y(self):
        for d in range(1, BANDS):
            band = lax.rem(self.band + d, BANDS)
            yield d - 1, band, {"grid": self.grid, "band": band}

    def barrier(self):
        sem = pltpu.get_barrier_semaphore()
        ids = [self.other_core()]
        ids += [i for _, _, i in self.over_x()]
        ids += [i for _, _, i in self.over_z()]
        ids += [i for _, _, i in self.over_y()]
        for i in ids:
            pl.semaphore_signal(sem, inc=1, device_id=i, device_id_type=MESH)
        pl.semaphore_wait(sem, len(ids))


def remote(src, dst, send, recv, device):
    return pltpu.make_async_remote_copy(
        src_ref=src,
        dst_ref=dst,
        send_sem=send,
        recv_sem=recv,
        device_id=device,
        device_id_type=MESH,
    )


def await_bytes(ref, sem):
    pltpu.make_async_copy(ref, ref, sem).wait()


def across_lanes(tile, lane):
    return jnp.broadcast_to(tile[:, lane : lane + 1], (ROWS, BLOCK))


def down_rows(tile, row):
    return jnp.broadcast_to(tile[row : row + 1, :], (ROWS, BLOCK))


def block_inverse(tiles):
    lanes = lax.broadcasted_iota(jnp.int32, (ROWS, BLOCK), 1)
    subs = lax.broadcasted_iota(jnp.int32, (ROWS, BLOCK), 0)
    tiles = list(tiles)
    count = len(tiles)
    done = []
    outs = []
    square = [across_lanes(tiles[0], q) for q in range(ROWS)]
    for t in range(count):
        base = ROWS * t
        here = (lanes >= base) & (lanes < base + ROWS)
        more = t + 1 < count
        if more:
            ahead = tiles[t + 1]
            side = [across_lanes(ahead, base + q) for q in range(ROWS)]
            following = [across_lanes(ahead, base + ROWS + q) for q in range(ROWS)]
        far = t + 2 < min(count, (t // GROUP + 1) * GROUP + 1)
        if far:
            beyond = tiles[t + 2]
            wing = [across_lanes(beyond, base + q) for q in range(ROWS)]
        current = jnp.where(here, jnp.where(lanes - base == subs, 1.0, 0.0), tiles[t])
        rows, scaled, unit = [], [], {}
        out = None
        for q in range(ROWS):
            root = lax.rsqrt(down_rows(square[q], q))
            inv = root * root
            scaled.append(inv)
            row = down_rows(current, q)
            rows.append(row)
            out = row * root if q == 0 else jnp.where(subs == q, row * root, out)
            if q + 1 < ROWS:
                current = current - (square[q] * inv) * row
            for s in range(q + 1, ROWS):
                unit[s, q] = down_rows(square[q], s) * inv
                square[s] = square[s] - unit[s, q] * square[q]
            if far:
                for s in range(q + 1, ROWS):
                    wing[s] = wing[s] - unit[s, q] * wing[q]
                beyond = (jnp.where(here, 0.0, beyond) if q == 0 else beyond) - (wing[q] * inv) * row
            if more:
                weight = side[q] * inv
                for s in range(q + 1, ROWS):
                    side[s] = side[s] - unit[s, q] * side[q]
                for s in range(ROWS):
                    following[s] = following[s] - weight * down_rows(side[q], s)
                ahead = (jnp.where(here, 0.0, ahead) if q == 0 else ahead) - weight * row
        if far:
            tiles[t + 2] = beyond
        done.append(jnp.where(lanes <= base + subs, out, 0.0))
        ends = (t // GROUP + 1) * GROUP * ROWS
        outs.append((out, jnp.where((lanes < base + ROWS) | (lanes >= ends), out, 0.0)))
        if more:
            square = following
            tiles[t + 1] = ahead
        if t + 3 < min(count, (t // GROUP + 1) * GROUP + 1):
            back = [rows[p] * scaled[p] for p in range(ROWS)]
            for p in range(ROWS - 1, 0, -1):
                for q in range(p):
                    back[q] = back[q] - unit[p, q] * back[p]
            for u in range(t + 3, min(count, (t // GROUP + 1) * GROUP + 1)):
                old = tiles[u]
                new = jnp.where(here, 0.0, old)
                for p in range(ROWS):
                    new = new - across_lanes(old, base + p) * back[p]
                tiles[u] = new
        first = t + 1 + 1
        if (t + 1) % GROUP == 0 and first < count:
            high, low = halves(jnp.concatenate([o[0] for o in outs[t + 1 - GROUP :]], 0))
            rhigh, rlow = halves(jnp.concatenate([o[1] for o in outs[t + 1 - GROUP :]], 0))
            change = lax.dot_general(
                jnp.concatenate([high, high, low], 0),
                jnp.concatenate([rhigh, rlow, rhigh], 0),
                (((0,), (0,)), ((), ())),
                preferred_element_type=jnp.float32,
            )
            group = (lanes >= base + ROWS - GROUP * ROWS) & (lanes < base + ROWS)
            for u in range(first, count):
                tiles[u] = jnp.where(group, 0.0, tiles[u]) - change[u * ROWS : (u + 1) * ROWS]
    return done


def factor_steps(a_ref, diag_ref, diag_right, lower_ref, right_ref, midway):
    n = a_ref.shape[0]
    blocks = n // BLOCK
    wide = 2 * BLOCK
    diag_right[...] = jnp.zeros_like(diag_right)
    right_ref[...] = jnp.zeros_like(right_ref)

    def step(k, carry):
        pl.when(k == MIDWAY)(midway)
        at = pl.ds(pl.multiple_of(k * BLOCK, BLOCK), BLOCK)
        before = pl.ds(pl.multiple_of(jnp.maximum(k - 1, 0) * BLOCK, BLOCK), BLOCK)
        after = pl.ds(pl.multiple_of(jnp.minimum(k + 1, blocks - 1) * BLOCK, BLOCK), BLOCK)
        base = pl.multiple_of(k * BLOCK, BLOCK)
        tiles = [a_ref[pl.ds(base + ROWS * t, ROWS), at] for t in range(BLOCK // ROWS)]

        for j in range(2, blocks):
            rows = slice(j * BLOCK, (j + 1) * BLOCK)
            on = jnp.where((j > k) & (k > 0), 1.0, 0.0).astype(jnp.float32)
            old = a_ref[rows, before]
            lower_ref[rows, :] = left_parts(dot_nt(left_parts(old), diag_right[...]) * on)
            a_ref[rows, before] = old * (1.0 - on)
        for c in range(n // wide):
            cols = slice(c * wide, (c + 1) * wide)
            for j in range(1, blocks // 2):
                rows = slice(j * wide, (j + 1) * wide)
                a_ref[rows, cols] -= jnp.dot(
                    lower_ref[rows, :], right_ref[:, cols], preferred_element_type=jnp.float32
                )
        for t, tile in enumerate(block_inverse(tiles)):
            diag_ref[ROWS * t : ROWS * (t + 1), :] = tile

        diag = diag_ref[...]
        a_ref[at, :] = jnp.dot(
            left_parts(diag), right_parts(a_ref[at, :], 0), preferred_element_type=jnp.float32
        )
        a_ref[at, at] = diag
        right_ref[...] = right_parts(a_ref[at, :], 0)
        diag_right[...] = right_parts(diag, 1)
        on = jnp.where(k < blocks - 1, 1.0, 0.0).astype(jnp.float32)
        old = a_ref[after, at]
        low = dot_nt(left_parts(old), diag_right[...]) * on
        a_ref[after, at] = old * (1.0 - on)
        a_ref[after, :] -= jnp.dot(left_parts(low), right_ref[...], preferred_element_type=jnp.float32)
        return carry

    lax.fori_loop(0, blocks, step, 0)


def gather_kernel(
    nx, nz, n_grid,
    basis_in, panel_in,
    coeffs_ref, panel_out_ref,
    basis_ref, panel_ref,
    others, lhs, rhs, part, from_core, from_x, from_z, gathered, own,
    removed, from_band, stacked, share, pieces_of,
    gram_ref, diag, diag_right, lower, right_parts_of, projected, projected_others,
    y_send, y_recv, send, recv, b_send, b_recv, g_send, z_recv, x_recv, g_recv, p_send, p_recv, io_sem,
):
    me = Place(nx, nz)
    fetch_panel = pltpu.make_async_copy(panel_in, panel_ref, io_sem.at[0])
    fetch_basis = pltpu.make_async_copy(basis_in, basis_ref, io_sem.at[1])
    fetch_panel.start()
    fetch_basis.start()
    me.barrier()
    nq, k = basis_ref.shape
    np_ = panel_ref.shape[0]
    pieces = nx * nz
    rq, rp = nq // pieces, np_ // pieces
    half = np_ // 2
    lo, hi = pl.ds(0, half), pl.ds(half, half)
    right = {"grid": me.grid, "band": lax.rem(me.band + 1, BANDS)}
    left = {"grid": me.grid, "band": lax.rem(me.band + BANDS - 1, BANDS)}

    def hop(i, src, dst, device):
        return remote(src, dst, y_send.at[i], y_recv.at[i], device)

    hops = [
        hop(0, panel_ref.at[lo], others.at[2, lo], right),
        hop(1, panel_ref.at[hi], others.at[0, hi], left),
        hop(2, panel_ref.at[hi], others.at[2, hi], right),
        hop(3, panel_ref.at[lo], others.at[0, lo], left),
        hop(4, others.at[2, lo], others.at[1, lo], right),
        hop(5, others.at[0, hi], others.at[1, hi], left),
    ]
    fetch_panel.wait()
    for h in hops[:4]:
        h.start()
    fetch_basis.wait()

    high, low = halves(basis_ref[...])
    lhs[:nq, :k] = high
    lhs[:nq, k : 2 * k] = high
    lhs[:nq, 2 * k :] = low
    high, low = halves(panel_ref[...])
    lhs[nq:, :k] = high
    lhs[nq:, k : 2 * k] = high
    lhs[nq:, 2 * k :] = low

    def multiply(q, tiles):
        for t, tile in enumerate(tiles):
            rows = slice(t * BLOCK, (t + 1) * BLOCK)
            high, low = halves(tile)
            rhs[rows, :k] = high
            rhs[rows, k : 2 * k] = low
            rhs[rows, 2 * k :] = high
        out = dot_nt(lhs[:nq, :], rhs[...])
        for t in range(2):
            part[q, t, :, :rq, :] = out[:, t * BLOCK : (t + 1) * BLOCK].reshape(pieces, rq, BLOCK)
        out = dot_nt(lhs[nq:, :], rhs[...])
        for t in range(2):
            part[q, t, :, rq:, :] = out[:, t * BLOCK : (t + 1) * BLOCK].reshape(pieces, rp, BLOCK)

    mine_x = pl.ds(me.x * nz, nz)

    def to_core(q):
        remote(
            part.at[q, 1 - me.core], from_core.at[q], send.at[0, q], recv.at[0, q], me.other_core()
        ).start()

    def to_x(q):
        await_bytes(from_core.at[q], recv.at[0, q])
        part[q, me.core] += from_core[q]
        for d, x, device in me.over_x():
            remote(
                part.at[q, me.core, pl.ds(x * nz, nz)],
                from_x.at[q, d],
                send.at[1, q],
                recv.at[1, q],
                device,
            ).start()

    def to_z(q):
        await_bytes(from_x.at[q], recv.at[1, q])
        total = part[q, me.core, mine_x]
        for d in range(nx - 1):
            total = total + from_x[q, d]
        part[q, me.core, mine_x] = total
        for d, z, device in me.over_z():
            remote(
                part.at[q, me.core, me.x * nz + z],
                from_z.at[q, d],
                send.at[2, q],
                recv.at[2, q],
                device,
            ).start()

    def back_z(q):
        await_bytes(from_z.at[q], recv.at[2, q])
        total = part[q, me.core, me.at]
        for d in range(nz - 1):
            total = total + from_z[q, d]
        total = total * (1.0 / n_grid)
        own[q] = total[rq:]
        gathered[q, me.core, me.at] = total[:rq]
        here = gathered.at[q, me.core, me.at]
        for _, _, device in me.over_z():
            remote(here, here, send.at[3, q], recv.at[3, q], device).start()

    def back_x(q):
        await_bytes(gathered.at[q, 0, pl.ds(0, nz - 1)], recv.at[3, q])
        here = gathered.at[q, me.core, mine_x]
        for _, _, device in me.over_x():
            remote(here, here, send.at[4, q], recv.at[4, q], device).start()

    def back_core(q):
        await_bytes(gathered.at[q, 0, pl.ds(0, (nx - 1) * nz)], recv.at[4, q])
        here = gathered.at[q, me.core]
        remote(here, here, send.at[5, q], recv.at[5, q], me.other_core()).start()

    def finish(q):
        await_bytes(gathered.at[q, 0], recv.at[5, q])
        for t in range(CORES):
            at = pl.multiple_of(tile_of(me.band, t, q) * BLOCK, BLOCK)
            coeffs_ref[:, pl.ds(at, BLOCK)] = gathered[q, t].reshape(nq, BLOCK)

    def remove(q):
        parts = [halves(gathered[q, t].reshape(nq, BLOCK).T) for t in range(CORES)]
        high = jnp.concatenate([p[0] for p in parts], 0)
        both = jnp.concatenate([high] + [p[1] for p in parts], 0)
        out = jnp.dot(both, lhs[:nq, :k], preferred_element_type=jnp.float32)
        out = out[: 2 * BLOCK] + out[2 * BLOCK :]
        out = out + jnp.dot(high, lhs[:nq, 2 * k :], preferred_element_type=jnp.float32)
        removed[q] = out.reshape(CORES, BLOCK, k)

    def bulk(i, src, dst, device):
        return remote(src, dst, b_send.at[i], b_recv.at[i], device)

    bulks = [
        bulk(0, removed.at[1, 0], from_band.at[2, 0], left),
        bulk(1, removed.at[1, 1], from_band.at[0, 1], right),
    ]
    cuts = [slice(0, BLOCK // 2), slice(BLOCK // 2, BLOCK)]
    for i, cut in enumerate(cuts):
        bulks += [
            bulk(4 * i + 2, removed.at[3, 0, cut], from_band.at[1, 0, cut], right),
            bulk(4 * i + 3, removed.at[3, 1, cut], from_band.at[1, 1, cut], left),
            bulk(4 * i + 4, removed.at[2, 0, cut], from_band.at[0, 0, cut], right),
            bulk(4 * i + 5, removed.at[2, 1, cut], from_band.at[2, 1, cut], left),
        ]

    multiply(0, (panel_ref[lo, :], panel_ref[hi, :]))
    to_core(0)
    to_x(0)
    to_z(0)
    hops[0].wait_recv()
    hops[4].start()
    hops[1].wait_recv()
    hops[5].start()
    multiply(1, (others[2, lo, :], others[0, hi, :]))
    to_core(1)
    back_z(0)
    to_x(1)
    back_x(0)
    to_z(1)
    hops[2].wait_recv()
    hops[3].wait_recv()
    multiply(2, (others[0, lo, :], others[2, hi, :]))
    to_core(2)
    back_z(1)
    back_core(0)
    to_x(2)
    hops[4].wait_recv()
    hops[5].wait_recv()
    multiply(3, (others[1, lo, :], others[1, hi, :]))
    to_core(3)
    to_z(2)
    to_x(3)
    back_x(1)
    finish(0)
    back_z(2)
    to_z(3)
    back_core(1)
    back_x(2)
    back_z(3)
    finish(1)
    remove(1)
    bulks[0].start()
    bulks[1].start()
    back_core(2)
    back_x(3)
    remove(0)
    finish(2)
    remove(2)
    back_core(3)
    for h in hops:
        h.wait_send()
    finish(3)

    high, low = halves(coeffs_ref[...])
    stacked[:nq, :] = high
    stacked[nq : 2 * nq, :] = low
    stacked[2 * nq :, :] = high
    n = coeffs_ref.shape[1]
    count = BANDS * rp
    row = lax.broadcasted_iota(jnp.int32, (count, n), 0)
    col = lax.broadcasted_iota(jnp.int32, (count, n), 1)
    want = lax.div(row, rp) * np_ + lax.rem(row, rp) + me.at * rp
    pick = jnp.where(col == want, 1.0, 0.0).astype(jnp.bfloat16)
    high = dot_nt(pick, stacked[:nq, :]).astype(jnp.bfloat16)
    low = dot_nt(pick, stacked[nq : 2 * nq, :]).astype(jnp.bfloat16)
    square = jnp.dot(
        jnp.concatenate([high, high, low], 1), stacked[...], preferred_element_type=jnp.float32
    )
    for band in range(BANDS):
        rows = square[band * rp : (band + 1) * rp]
        for i in range(KEPT):
            first = 2 * ((band + i) % BANDS) * BLOCK
            pair = [rows[:, first + t * BLOCK : first + (t + 1) * BLOCK] for t in range(CORES)]
            share[me.band, band, i] = -jnp.where(me.core == 0, pair[0], pair[1])
    for i, q in enumerate((0, 2 - me.core, ROUNDS - 1)):
        share[me.band, me.band, i] += own[q]
    for _, _, device in me.over_y():
        remote(share.at[me.band], share.at[me.band], g_send.at[0], g_recv.at[0], device).start()
    remove(3)
    for i in (2, 3, 6, 7):
        bulks[i].start()
    await_bytes(share.at[pl.ds(0, BANDS - 1)], g_recv.at[0])
    pieces_of[me.core, me.x, me.z] = (share[0] + share[1]) + (share[2] + share[3])

    up, down = lax.rem(me.x + 1, nx), lax.rem(me.x + nx - 1, nx)
    to_up, to_down = me.id(me.z, up, me.core), me.id(me.z, down, me.core)
    first, second = pl.ds(0, BANDS // 2), pl.ds(BANDS // 2, BANDS // 2)

    def spread(i, z):
        here = pieces_of.at[me.core, me.x, z]
        remote(here, here, g_send.at[2], x_recv.at[0, i], to_up).start()
        remote(here, here, g_send.at[2], x_recv.at[1, i], to_down).start()

    def relay(i, z):
        await_bytes(pieces_of.at[0, 0, 0], x_recv.at[0, i])
        here = pieces_of.at[me.core, down, z, first]
        remote(here, here, g_send.at[3], g_recv.at[1], to_up).start()
        await_bytes(pieces_of.at[0, 0, 0], x_recv.at[1, i])
        here = pieces_of.at[me.core, up, z, second]
        remote(here, here, g_send.at[3], g_recv.at[1], to_down).start()

    def cross(x):
        here = pieces_of.at[me.core, x]
        remote(here, here, g_send.at[4], g_recv.at[2], me.other_core()).start()

    here = pieces_of.at[me.core, me.x, me.z]
    nearest = sorted(range(1, nz), key=lambda d: min(d, nz - d))
    for d in nearest:
        device = me.id(lax.rem(me.z + d, nz), me.x, me.core)
        remote(here, here, g_send.at[1], z_recv.at[d - 1], device).start()
    spread(0, me.z)
    order = [me.z]
    for i, d in enumerate(nearest):
        z = lax.rem(me.z + nz - d, nz)
        await_bytes(pieces_of.at[0, 0, 0], z_recv.at[d - 1])
        spread(i + 1, z)
        relay(i, order[i])
        order.append(z)
        if i in LATE:
            half_of = LATE.index(i)
            for t in range(CORES):
                bulks[4 * half_of + 2 + t].wait_recv()
                removed[2, t, cuts[half_of]] += from_band[1, t, cuts[half_of]]
                bulks[4 * half_of + 4 + t].start()
    cross(me.x)
    relay(nz - 1, order[nz - 1])
    cross(up)
    cross(down)
    await_bytes(pieces_of.at[0, 0], g_recv.at[1])
    cross(lax.rem(me.x + 2, nx))

    def place(core):
        for band in range(BANDS):
            for i in range(KEPT):
                at = (2 * ((band + i) % BANDS) + core) * BLOCK
                tile = pieces_of[core, :, :, band, i].reshape(np_, BLOCK)
                gram_ref[band * np_ : (band + 1) * np_, at : at + BLOCK] = tile
                if i == 1:
                    to = (2 * ((band + i) % BANDS) + core) * BLOCK
                    gram_ref[to : to + BLOCK, band * np_ : (band + 1) * np_] = tile.T

    def carry(i, src, dst, device):
        return remote(src, dst, p_send.at[i], p_recv.at[i], device)

    carried = [
        carry(0, projected.at[lo], projected_others.at[2, lo], right),
        carry(1, projected.at[hi], projected_others.at[0, hi], left),
        carry(2, projected.at[hi], projected_others.at[2, hi], right),
        carry(3, projected.at[lo], projected_others.at[0, lo], left),
        carry(4, projected_others.at[2, lo], projected_others.at[1, lo], right),
        carry(5, projected_others.at[0, hi], projected_others.at[1, hi], left),
    ]
    def early():
        for i in (0, 1, 4, 5, 8, 9):
            bulks[i].wait_recv()
        for t in range(CORES):
            rows = slice(t * BLOCK, (t + 1) * BLOCK)
            total = removed[0, t] + (from_band[0, t] + from_band[2, t])
            projected[rows, :] = panel_ref[rows, :] - total
        for h in carried[:4]:
            h.start()

    def midway():
        carried[0].wait_recv()
        carried[4].start()
        carried[1].wait_recv()
        carried[5].start()

    early()
    await_bytes(pieces_of.at[0], g_recv.at[2])
    place(0)
    place(1)
    factor_steps(gram_ref, diag, diag_right, lower, right_parts_of, midway)
    mine = pl.ds(pl.multiple_of(me.band * np_, np_), np_)
    row = lax.broadcasted_iota(jnp.int32, (np_, np_), 0) + me.band * np_
    col = lax.broadcasted_iota(jnp.int32, (np_, np_), 1)

    def times(r, block):
        first = lax.rem(me.band + r, BANDS) * np_
        tile = gram_ref[mine, pl.ds(pl.multiple_of(first, np_), np_)]
        tile = jnp.where(col + first <= row, tile, 0.0)
        return jnp.dot(
            left_parts(tile), right_parts(block, 0), preferred_element_type=jnp.float32
        )

    panel_out_ref[...] = times(0, projected[...])
    carried[2].wait_recv()
    carried[3].wait_recv()
    panel_out_ref[...] += times(1, projected_others[0])
    panel_out_ref[...] += times(3, projected_others[2])
    carried[4].wait_recv()
    carried[5].wait_recv()
    panel_out_ref[...] += times(2, projected_others[1])
    for h in carried:
        h.wait_send()

    for h in bulks:
        h.wait_send()
    for q in range(ROUNDS):
        await_bytes(from_core.at[q], send.at[0, q])
        await_bytes(from_x.at[q], send.at[1, q])
        await_bytes(from_z.at[q], send.at[2, q])
        await_bytes(gathered.at[q, 0, pl.ds(0, nz - 1)], send.at[3, q])
        await_bytes(gathered.at[q, 0, pl.ds(0, (nx - 1) * nz)], send.at[4, q])
        await_bytes(gathered.at[q, 0], send.at[5, q])
    await_bytes(share.at[pl.ds(0, BANDS - 1)], g_send.at[0])
    await_bytes(pieces_of.at[0, 0, pl.ds(0, nz - 1)], g_send.at[1])
    await_bytes(pieces_of.at[0, pl.ds(0, 2)], g_send.at[2])
    await_bytes(pieces_of.at[0, 0], g_send.at[3])
    await_bytes(pieces_of.at[0], g_send.at[4])


def reduce_and_project(nx, nz, n_grid, basis, panel):
    nq, k = basis.shape
    np_ = panel.shape[0]
    n = np_ * BANDS
    pieces = nx * nz
    rq, rp = nq // pieces, np_ // pieces
    f32 = jnp.float32
    dma = pltpu.SemaphoreType.DMA
    return pl.pallas_call(
        functools.partial(gather_kernel, nx, nz, n_grid),
        out_shape=(
            jax.ShapeDtypeStruct((nq, n), f32),
            jax.ShapeDtypeStruct((np_, k), f32),
        ),
        in_specs=[pl.BlockSpec(memory_space=pltpu.HBM)] * 2,
        out_specs=(pl.BlockSpec(memory_space=pltpu.VMEM),) * 2,
        scratch_shapes=[
            pltpu.VMEM((nq, k), f32),
            pltpu.VMEM((np_, k), f32),
            pltpu.VMEM((BANDS - 1, np_, k), f32),
            pltpu.VMEM((nq + np_, 3 * k), jnp.bfloat16),
            pltpu.VMEM((2 * BLOCK, 3 * k), jnp.bfloat16),
            pltpu.VMEM((ROUNDS, CORES, pieces, rq + rp, BLOCK), f32),
            pltpu.VMEM((ROUNDS, pieces, rq + rp, BLOCK), f32),
            pltpu.VMEM((ROUNDS, nx - 1, nz, rq + rp, BLOCK), f32),
            pltpu.VMEM((ROUNDS, nz - 1, rq + rp, BLOCK), f32),
            pltpu.VMEM((ROUNDS, CORES, pieces, rq, BLOCK), f32),
            pltpu.VMEM((ROUNDS, rp, BLOCK), f32),
            pltpu.VMEM((ROUNDS, CORES, BLOCK, k), f32),
            pltpu.VMEM((BANDS - 1, CORES, BLOCK, k), f32),
            pltpu.VMEM((3 * nq, n), jnp.bfloat16),
            pltpu.VMEM((BANDS, BANDS, KEPT, rp, BLOCK), f32),
            pltpu.VMEM((CORES, nx, nz, BANDS, KEPT, rp, BLOCK), f32),
            pltpu.VMEM((n, n), f32),
            pltpu.VMEM((BLOCK, BLOCK), f32),
            pltpu.VMEM((BLOCK, 3 * BLOCK), jnp.bfloat16),
            pltpu.VMEM((n, 3 * BLOCK), jnp.bfloat16),
            pltpu.VMEM((3 * BLOCK, n), jnp.bfloat16),
            pltpu.VMEM((np_, k), f32),
            pltpu.VMEM((BANDS - 1, np_, k), f32),
            dma((6,)),
            dma((6,)),
            dma((6, ROUNDS)),
            dma((6, ROUNDS)),
            dma((10,)),
            dma((10,)),
            dma((5,)),
            dma((nz - 1,)),
            dma((2, nz)),
            dma((3,)),
            dma((6,)),
            dma((6,)),
            dma((2,)),
        ],
        compiler_params=pltpu.CompilerParams(
            collective_id=0, has_side_effects=True, vmem_limit_bytes=48 * 1024 * 1024
        ),
        cost_estimate=pl.CostEstimate(
            flops=60 * 1024**3, bytes_accessed=8 * 1024 * 1024, transcendentals=0
        ),
    )(basis, panel)


def body(basis, panel):
    grid = lax.axis_size("grid")
    nz = grid // (CORES * ALONG_X)
    coeffs, new_panel = reduce_and_project(
        ALONG_X, nz, panel.shape[1] * grid, basis, panel
    )
    return (new_panel, coeffs)


def solution(mesh):
    placed = (P("band", "grid"), P("band", "grid"))
    return jax.shard_map(
        body,
        mesh=mesh,
        in_specs=placed,
        out_specs=(P("band", "grid"), P("band", None)),
        check_vma=False,
    )
```

```python
import functools

import jax
import jax.numpy as jnp
from jax import lax
from jax.experimental import pallas as pl
from jax.experimental.pallas import tpu as pltpu
from jax.sharding import PartitionSpec as P

BLOCK = 128
ROWS = 8
CORES = 2
BANDS = 4
ROUNDS = 4
KEPT = 3
GROUP = 4
LATE = (1, 3)
MIDWAY = 4
ALONG_X = 4
MESH = pl.DeviceIdType.MESH


def halves(x):
    high = x.astype(jnp.bfloat16)
    low = (x - high.astype(jnp.float32)).astype(jnp.bfloat16)
    return high, low


def left_parts(x):
    high, low = halves(x)
    return jnp.concatenate([high, high, low], 1)


def right_parts(x, axis):
    high, low = halves(x)
    return jnp.concatenate([high, low, high], axis)


def dot_nt(left, right):
    return lax.dot_general(
        left, right, (((1,), (1,)), ((), ())), preferred_element_type=jnp.float32
    )


def tile_of(band, core, turn):
    one, two, three = (lax.rem(band + i, BANDS) for i in (1, 2, 3))
    if turn == 0:
        return 2 * band + core
    if turn == 1:
        return 2 * (three + core * (one - three)) + core
    if turn == 2:
        return 2 * (one + core * (three - one)) + core
    return 2 * two + core


class Place:
    def __init__(self, nx, nz):
        self.nx, self.nz = nx, nz
        self.grid = lax.axis_index("grid")
        self.band = lax.axis_index("band")
        self.core = lax.rem(self.grid, CORES)
        self.x = lax.rem(lax.div(self.grid, CORES), nx)
        self.z = lax.div(self.grid, CORES * nx)
        self.at = self.x * nz + self.z

    def id(self, z, x, core):
        return {"grid": (z * self.nx + x) * CORES + core, "band": self.band}

    def other_core(self):
        return self.id(self.z, self.x, 1 - self.core)

    def over_x(self):
        for d in range(1, self.nx):
            x = lax.rem(self.x + d, self.nx)
            yield d - 1, x, self.id(self.z, x, self.core)

    def over_z(self):
        for d in range(1, self.nz):
            z = lax.rem(self.z + d, self.nz)
            yield d - 1, z, self.id(z, self.x, self.core)

    def over_y(self):
        for d in range(1, BANDS):
            band = lax.rem(self.band + d, BANDS)
            yield d - 1, band, {"grid": self.grid, "band": band}

    def barrier(self):
        sem = pltpu.get_barrier_semaphore()
        ids = [self.other_core()]
        ids += [i for _, _, i in self.over_x()]
        ids += [i for _, _, i in self.over_z()]
        ids += [i for _, _, i in self.over_y()]
        for i in ids:
            pl.semaphore_signal(sem, inc=1, device_id=i, device_id_type=MESH)
        pl.semaphore_wait(sem, len(ids))


def remote(src, dst, send, recv, device):
    return pltpu.make_async_remote_copy(
        src_ref=src,
        dst_ref=dst,
        send_sem=send,
        recv_sem=recv,
        device_id=device,
        device_id_type=MESH,
    )


def await_bytes(ref, sem):
    pltpu.make_async_copy(ref, ref, sem).wait()


def across_lanes(tile, lane):
    return jnp.broadcast_to(tile[:, lane : lane + 1], (ROWS, BLOCK))


def down_rows(tile, row):
    return jnp.broadcast_to(tile[row : row + 1, :], (ROWS, BLOCK))


def block_inverse(tiles):
    lanes = lax.broadcasted_iota(jnp.int32, (ROWS, BLOCK), 1)
    subs = lax.broadcasted_iota(jnp.int32, (ROWS, BLOCK), 0)
    tiles = list(tiles)
    count = len(tiles)
    done = []
    outs = []
    square = [across_lanes(tiles[0], q) for q in range(ROWS)]
    for t in range(count):
        base = ROWS * t
        here = (lanes >= base) & (lanes < base + ROWS)
        more = t + 1 < count
        if more:
            ahead = tiles[t + 1]
            side = [across_lanes(ahead, base + q) for q in range(ROWS)]
            following = [across_lanes(ahead, base + ROWS + q) for q in range(ROWS)]
        far = t + 2 < min(count, (t // GROUP + 1) * GROUP + 1)
        if far:
            beyond = tiles[t + 2]
            wing = [across_lanes(beyond, base + q) for q in range(ROWS)]
        current = jnp.where(here, jnp.where(lanes - base == subs, 1.0, 0.0), tiles[t])
        rows, scaled, unit = [], [], {}
        out = None
        for q in range(ROWS):
            root = lax.rsqrt(down_rows(square[q], q))
            inv = root * root
            scaled.append(inv)
            row = down_rows(current, q)
            rows.append(row)
            out = row * root if q == 0 else jnp.where(subs == q, row * root, out)
            if q + 1 < ROWS:
                current = current - (square[q] * inv) * row
            for s in range(q + 1, ROWS):
                unit[s, q] = down_rows(square[q], s) * inv
                square[s] = square[s] - unit[s, q] * square[q]
            if far:
                for s in range(q + 1, ROWS):
                    wing[s] = wing[s] - unit[s, q] * wing[q]
                beyond = (jnp.where(here, 0.0, beyond) if q == 0 else beyond) - (wing[q] * inv) * row
            if more:
                weight = side[q] * inv
                for s in range(q + 1, ROWS):
                    side[s] = side[s] - unit[s, q] * side[q]
                for s in range(ROWS):
                    following[s] = following[s] - weight * down_rows(side[q], s)
                ahead = (jnp.where(here, 0.0, ahead) if q == 0 else ahead) - weight * row
        if far:
            tiles[t + 2] = beyond
        done.append(jnp.where(lanes <= base + subs, out, 0.0))
        ends = (t // GROUP + 1) * GROUP * ROWS
        outs.append((out, jnp.where((lanes < base + ROWS) | (lanes >= ends), out, 0.0)))
        if more:
            square = following
            tiles[t + 1] = ahead
        if t + 3 < min(count, (t // GROUP + 1) * GROUP + 1):
            back = [rows[p] * scaled[p] for p in range(ROWS)]
            for p in range(ROWS - 1, 0, -1):
                for q in range(p):
                    back[q] = back[q] - unit[p, q] * back[p]
            for u in range(t + 3, min(count, (t // GROUP + 1) * GROUP + 1)):
                old = tiles[u]
                new = jnp.where(here, 0.0, old)
                for p in range(ROWS):
                    new = new - across_lanes(old, base + p) * back[p]
                tiles[u] = new
        first = t + 1 + 1
        if (t + 1) % GROUP == 0 and first < count:
            high, low = halves(jnp.concatenate([o[0] for o in outs[t + 1 - GROUP :]], 0))
            rhigh, rlow = halves(jnp.concatenate([o[1] for o in outs[t + 1 - GROUP :]], 0))
            change = lax.dot_general(
                jnp.concatenate([high, high, low], 0),
                jnp.concatenate([rhigh, rlow, rhigh], 0),
                (((0,), (0,)), ((), ())),
                preferred_element_type=jnp.float32,
            )
            group = (lanes >= base + ROWS - GROUP * ROWS) & (lanes < base + ROWS)
            for u in range(first, count):
                tiles[u] = jnp.where(group, 0.0, tiles[u]) - change[u * ROWS : (u + 1) * ROWS]
    return done


def factor_steps(a_ref, diag_ref, diag_right, lower_ref, right_ref, midway):
    n = a_ref.shape[0]
    blocks = n // BLOCK
    wide = 2 * BLOCK
    diag_right[...] = jnp.zeros_like(diag_right)
    right_ref[...] = jnp.zeros_like(right_ref)

    def step(k, carry):
        pl.when(k == MIDWAY)(midway)
        at = pl.ds(pl.multiple_of(k * BLOCK, BLOCK), BLOCK)
        before = pl.ds(pl.multiple_of(jnp.maximum(k - 1, 0) * BLOCK, BLOCK), BLOCK)
        after = pl.ds(pl.multiple_of(jnp.minimum(k + 1, blocks - 1) * BLOCK, BLOCK), BLOCK)
        base = pl.multiple_of(k * BLOCK, BLOCK)
        tiles = [a_ref[pl.ds(base + ROWS * t, ROWS), at] for t in range(BLOCK // ROWS)]

        for j in range(2, blocks):
            rows = slice(j * BLOCK, (j + 1) * BLOCK)
            on = jnp.where((j > k) & (k > 0), 1.0, 0.0).astype(jnp.float32)
            old = a_ref[rows, before]
            lower_ref[rows, :] = left_parts(dot_nt(left_parts(old), diag_right[...]) * on)
            a_ref[rows, before] = old * (1.0 - on)
        for c in range(n // wide):
            cols = slice(c * wide, (c + 1) * wide)
            for j in range(1, blocks // 2):
                rows = slice(j * wide, (j + 1) * wide)
                a_ref[rows, cols] -= jnp.dot(
                    lower_ref[rows, :], right_ref[:, cols], preferred_element_type=jnp.float32
                )
        for t, tile in enumerate(block_inverse(tiles)):
            diag_ref[ROWS * t : ROWS * (t + 1), :] = tile

        diag = diag_ref[...]
        a_ref[at, :] = jnp.dot(
            left_parts(diag), right_parts(a_ref[at, :], 0), preferred_element_type=jnp.float32
        )
        a_ref[at, at] = diag
        right_ref[...] = right_parts(a_ref[at, :], 0)
        diag_right[...] = right_parts(diag, 1)
        on = jnp.where(k < blocks - 1, 1.0, 0.0).astype(jnp.float32)
        old = a_ref[after, at]
        low = dot_nt(left_parts(old), diag_right[...]) * on
        a_ref[after, at] = old * (1.0 - on)
        a_ref[after, :] -= jnp.dot(left_parts(low), right_ref[...], preferred_element_type=jnp.float32)
        return carry

    lax.fori_loop(0, blocks, step, 0)


def gather_kernel(
    nx, nz, n_grid,
    basis_in, panel_in,
    coeffs_ref, panel_out_ref,
    basis_ref, panel_ref,
    others, lhs, rhs, part, from_core, from_x, from_z, gathered, own,
    removed, from_band, stacked, share, pieces_of,
    gram_ref, diag, diag_right, lower, right_parts_of, projected, projected_others,
    y_send, y_recv, send, recv, b_send, b_recv, g_send, z_recv, x_recv, g_recv, p_send, p_recv, io_sem,
):
    me = Place(nx, nz)
    fetch_panel = pltpu.make_async_copy(panel_in, panel_ref, io_sem.at[0])
    fetch_basis = pltpu.make_async_copy(basis_in, basis_ref, io_sem.at[1])
    fetch_panel.start()
    fetch_basis.start()
    me.barrier()
    nq, k = basis_ref.shape
    np_ = panel_ref.shape[0]
    pieces = nx * nz
    rq, rp = nq // pieces, np_ // pieces
    half = np_ // 2
    lo, hi = pl.ds(0, half), pl.ds(half, half)
    right = {"grid": me.grid, "band": lax.rem(me.band + 1, BANDS)}
    left = {"grid": me.grid, "band": lax.rem(me.band + BANDS - 1, BANDS)}

    def hop(i, src, dst, device):
        return remote(src, dst, y_send.at[i], y_recv.at[i], device)

    hops = [
        hop(0, panel_ref.at[lo], others.at[2, lo], right),
        hop(1, panel_ref.at[hi], others.at[0, hi], left),
        hop(2, panel_ref.at[hi], others.at[2, hi], right),
        hop(3, panel_ref.at[lo], others.at[0, lo], left),
        hop(4, others.at[2, lo], others.at[1, lo], right),
        hop(5, others.at[0, hi], others.at[1, hi], left),
    ]
    fetch_panel.wait()
    for h in hops[:4]:
        h.start()
    fetch_basis.wait()

    high, low = halves(basis_ref[...])
    lhs[:nq, :k] = high
    lhs[:nq, k : 2 * k] = high
    lhs[:nq, 2 * k :] = low
    high, low = halves(panel_ref[...])
    lhs[nq:, :k] = high
    lhs[nq:, k : 2 * k] = high
    lhs[nq:, 2 * k :] = low

    def multiply(q, tiles):
        for t, tile in enumerate(tiles):
            rows = slice(t * BLOCK, (t + 1) * BLOCK)
            high, low = halves(tile)
            rhs[rows, :k] = high
            rhs[rows, k : 2 * k] = low
            rhs[rows, 2 * k :] = high
        out = dot_nt(lhs[:nq, :], rhs[...])
        for t in range(2):
            part[q, t, :, :rq, :] = out[:, t * BLOCK : (t + 1) * BLOCK].reshape(pieces, rq, BLOCK)
        out = dot_nt(lhs[nq:, :], rhs[...])
        for t in range(2):
            part[q, t, :, rq:, :] = out[:, t * BLOCK : (t + 1) * BLOCK].reshape(pieces, rp, BLOCK)

    mine_x = pl.ds(me.x * nz, nz)

    def to_core(q):
        remote(
            part.at[q, 1 - me.core], from_core.at[q], send.at[0, q], recv.at[0, q], me.other_core()
        ).start()

    def to_x(q):
        await_bytes(from_core.at[q], recv.at[0, q])
        part[q, me.core] += from_core[q]
        for d, x, device in me.over_x():
            remote(
                part.at[q, me.core, pl.ds(x * nz, nz)],
                from_x.at[q, d],
                send.at[1, q],
                recv.at[1, q],
                device,
            ).start()

    def to_z(q):
        await_bytes(from_x.at[q], recv.at[1, q])
        total = part[q, me.core, mine_x]
        for d in range(nx - 1):
            total = total + from_x[q, d]
        part[q, me.core, mine_x] = total
        for d, z, device in me.over_z():
            remote(
                part.at[q, me.core, me.x * nz + z],
                from_z.at[q, d],
                send.at[2, q],
                recv.at[2, q],
                device,
            ).start()

    def back_z(q):
        await_bytes(from_z.at[q], recv.at[2, q])
        total = part[q, me.core, me.at]
        for d in range(nz - 1):
            total = total + from_z[q, d]
        total = total * (1.0 / n_grid)
        own[q] = total[rq:]
        gathered[q, me.core, me.at] = total[:rq]
        here = gathered.at[q, me.core, me.at]
        for _, _, device in me.over_z():
            remote(here, here, send.at[3, q], recv.at[3, q], device).start()

    def back_x(q):
        await_bytes(gathered.at[q, 0, pl.ds(0, nz - 1)], recv.at[3, q])
        here = gathered.at[q, me.core, mine_x]
        for _, _, device in me.over_x():
            remote(here, here, send.at[4, q], recv.at[4, q], device).start()

    def back_core(q):
        await_bytes(gathered.at[q, 0, pl.ds(0, (nx - 1) * nz)], recv.at[4, q])
        here = gathered.at[q, me.core]
        remote(here, here, send.at[5, q], recv.at[5, q], me.other_core()).start()

    def finish(q):
        await_bytes(gathered.at[q, 0], recv.at[5, q])
        for t in range(CORES):
            at = pl.multiple_of(tile_of(me.band, t, q) * BLOCK, BLOCK)
            coeffs_ref[:, pl.ds(at, BLOCK)] = gathered[q, t].reshape(nq, BLOCK)

    def remove(q):
        parts = [halves(gathered[q, t].reshape(nq, BLOCK).T) for t in range(CORES)]
        high = jnp.concatenate([p[0] for p in parts], 0)
        both = jnp.concatenate([high] + [p[1] for p in parts], 0)
        out = jnp.dot(both, lhs[:nq, :k], preferred_element_type=jnp.float32)
        out = out[: 2 * BLOCK] + out[2 * BLOCK :]
        out = out + jnp.dot(high, lhs[:nq, 2 * k :], preferred_element_type=jnp.float32)
        removed[q] = out.reshape(CORES, BLOCK, k)

    def bulk(i, src, dst, device):
        return remote(src, dst, b_send.at[i], b_recv.at[i], device)

    bulks = [
        bulk(0, removed.at[1, 0], from_band.at[2, 0], left),
        bulk(1, removed.at[1, 1], from_band.at[0, 1], right),
    ]
    cuts = [slice(0, BLOCK // 2), slice(BLOCK // 2, BLOCK)]
    for i, cut in enumerate(cuts):
        bulks += [
            bulk(4 * i + 2, removed.at[3, 0, cut], from_band.at[1, 0, cut], right),
            bulk(4 * i + 3, removed.at[3, 1, cut], from_band.at[1, 1, cut], left),
            bulk(4 * i + 4, removed.at[2, 0, cut], from_band.at[0, 0, cut], right),
            bulk(4 * i + 5, removed.at[2, 1, cut], from_band.at[2, 1, cut], left),
        ]

    multiply(0, (panel_ref[lo, :], panel_ref[hi, :]))
    to_core(0)
    to_x(0)
    to_z(0)
    hops[0].wait_recv()
    hops[4].start()
    hops[1].wait_recv()
    hops[5].start()
    multiply(1, (others[2, lo, :], others[0, hi, :]))
    to_core(1)
    back_z(0)
    to_x(1)
    back_x(0)
    to_z(1)
    hops[2].wait_recv()
    hops[3].wait_recv()
    multiply(2, (others[0, lo, :], others[2, hi, :]))
    to_core(2)
    back_z(1)
    back_core(0)
    to_x(2)
    hops[4].wait_recv()
    hops[5].wait_recv()
    multiply(3, (others[1, lo, :], others[1, hi, :]))
    to_core(3)
    to_z(2)
    to_x(3)
    back_x(1)
    finish(0)
    back_z(2)
    to_z(3)
    back_core(1)
    back_x(2)
    back_z(3)
    finish(1)
    remove(1)
    bulks[0].start()
    bulks[1].start()
    back_core(2)
    back_x(3)
    remove(0)
    finish(2)
    remove(2)
    back_core(3)
    for h in hops:
        h.wait_send()
    finish(3)

    high, low = halves(coeffs_ref[...])
    stacked[:nq, :] = high
    stacked[nq : 2 * nq, :] = low
    stacked[2 * nq :, :] = high
    n = coeffs_ref.shape[1]
    count = BANDS * rp
    row = lax.broadcasted_iota(jnp.int32, (count, n), 0)
    col = lax.broadcasted_iota(jnp.int32, (count, n), 1)
    want = lax.div(row, rp) * np_ + lax.rem(row, rp) + me.at * rp
    pick = jnp.where(col == want, 1.0, 0.0).astype(jnp.bfloat16)
    high = dot_nt(pick, stacked[:nq, :]).astype(jnp.bfloat16)
    low = dot_nt(pick, stacked[nq : 2 * nq, :]).astype(jnp.bfloat16)
    square = jnp.dot(
        jnp.concatenate([high, high, low], 1), stacked[...], preferred_element_type=jnp.float32
    )
    for band in range(BANDS):
        rows = square[band * rp : (band + 1) * rp]
        for i in range(KEPT):
            first = 2 * ((band + i) % BANDS) * BLOCK
            pair = [rows[:, first + t * BLOCK : first + (t + 1) * BLOCK] for t in range(CORES)]
            share[me.band, band, i] = -jnp.where(me.core == 0, pair[0], pair[1])
    for i, q in enumerate((0, 2 - me.core, ROUNDS - 1)):
        share[me.band, me.band, i] += own[q]
    for _, _, device in me.over_y():
        remote(share.at[me.band], share.at[me.band], g_send.at[0], g_recv.at[0], device).start()
    remove(3)
    for i in (2, 3, 6, 7):
        bulks[i].start()
    await_bytes(share.at[pl.ds(0, BANDS - 1)], g_recv.at[0])
    pieces_of[me.core, me.x, me.z] = (share[0] + share[1]) + (share[2] + share[3])

    up, down = lax.rem(me.x + 1, nx), lax.rem(me.x + nx - 1, nx)
    to_up, to_down = me.id(me.z, up, me.core), me.id(me.z, down, me.core)
    first, second = pl.ds(0, BANDS // 2), pl.ds(BANDS // 2, BANDS // 2)

    def spread(i, z):
        here = pieces_of.at[me.core, me.x, z]
        remote(here, here, g_send.at[2], x_recv.at[0, i], to_up).start()
        remote(here, here, g_send.at[2], x_recv.at[1, i], to_down).start()

    def relay(i, z):
        await_bytes(pieces_of.at[0, 0, 0], x_recv.at[0, i])
        here = pieces_of.at[me.core, down, z, first]
        remote(here, here, g_send.at[3], g_recv.at[1], to_up).start()
        await_bytes(pieces_of.at[0, 0, 0], x_recv.at[1, i])
        here = pieces_of.at[me.core, up, z, second]
        remote(here, here, g_send.at[3], g_recv.at[1], to_down).start()

    def cross(x):
        here = pieces_of.at[me.core, x]
        remote(here, here, g_send.at[4], g_recv.at[2], me.other_core()).start()

    here = pieces_of.at[me.core, me.x, me.z]
    nearest = sorted(range(1, nz), key=lambda d: min(d, nz - d))
    for d in nearest:
        device = me.id(lax.rem(me.z + d, nz), me.x, me.core)
        remote(here, here, g_send.at[1], z_recv.at[d - 1], device).start()
    spread(0, me.z)
    order = [me.z]
    for i, d in enumerate(nearest):
        z = lax.rem(me.z + nz - d, nz)
        await_bytes(pieces_of.at[0, 0, 0], z_recv.at[d - 1])
        spread(i + 1, z)
        relay(i, order[i])
        order.append(z)
        if i in LATE:
            half_of = LATE.index(i)
            for t in range(CORES):
                bulks[4 * half_of + 2 + t].wait_recv()
                removed[2, t, cuts[half_of]] += from_band[1, t, cuts[half_of]]
                bulks[4 * half_of + 4 + t].start()
    cross(me.x)
    relay(nz - 1, order[nz - 1])
    cross(up)
    cross(down)

    def place(core):
        for band in range(BANDS):
            for i in range(KEPT):
                at = (2 * ((band + i) % BANDS) + core) * BLOCK
                tile = pieces_of[core, :, :, band, i].reshape(np_, BLOCK)
                gram_ref[band * np_ : (band + 1) * np_, at : at + BLOCK] = tile
                if i == 1:
                    to = (2 * ((band + i) % BANDS) + core) * BLOCK
                    gram_ref[to : to + BLOCK, band * np_ : (band + 1) * np_] = tile.T

    def carry(i, src, dst, device):
        return remote(src, dst, p_send.at[i], p_recv.at[i], device)

    carried = [
        carry(0, projected.at[lo], projected_others.at[2, lo], right),
        carry(1, projected.at[hi], projected_others.at[0, hi], left),
        carry(2, projected.at[hi], projected_others.at[2, hi], right),
        carry(3, projected.at[lo], projected_others.at[0, lo], left),
        carry(4, projected_others.at[2, lo], projected_others.at[1, lo], right),
        carry(5, projected_others.at[0, hi], projected_others.at[1, hi], left),
    ]
    def early():
        for i in (0, 1, 4, 5, 8, 9):
            bulks[i].wait_recv()
        for t in range(CORES):
            rows = slice(t * BLOCK, (t + 1) * BLOCK)
            total = removed[0, t] + (from_band[0, t] + from_band[2, t])
            projected[rows, :] = panel_ref[rows, :] - total
        for h in carried[:4]:
            h.start()

    def midway():
        carried[0].wait_recv()
        carried[4].start()
        carried[1].wait_recv()
        carried[5].start()

    early()
    await_bytes(pieces_of.at[0, 0], g_recv.at[1])
    cross(lax.rem(me.x + 2, nx))
    await_bytes(pieces_of.at[0], g_recv.at[2])
    place(0)
    place(1)
    factor_steps(gram_ref, diag, diag_right, lower, right_parts_of, midway)
    mine = pl.ds(pl.multiple_of(me.band * np_, np_), np_)
    row = lax.broadcasted_iota(jnp.int32, (np_, np_), 0) + me.band * np_
    col = lax.broadcasted_iota(jnp.int32, (np_, np_), 1)

    def times(r, block):
        first = lax.rem(me.band + r, BANDS) * np_
        tile = gram_ref[mine, pl.ds(pl.multiple_of(first, np_), np_)]
        tile = jnp.where(col + first <= row, tile, 0.0)
        return jnp.dot(
            left_parts(tile), right_parts(block, 0), preferred_element_type=jnp.float32
        )

    panel_out_ref[...] = times(0, projected[...])
    carried[2].wait_recv()
    carried[3].wait_recv()
    panel_out_ref[...] += times(1, projected_others[0])
    panel_out_ref[...] += times(3, projected_others[2])
    carried[4].wait_recv()
    carried[5].wait_recv()
    panel_out_ref[...] += times(2, projected_others[1])
    for h in carried:
        h.wait_send()

    for h in bulks:
        h.wait_send()
    for q in range(ROUNDS):
        await_bytes(from_core.at[q], send.at[0, q])
        await_bytes(from_x.at[q], send.at[1, q])
        await_bytes(from_z.at[q], send.at[2, q])
        await_bytes(gathered.at[q, 0, pl.ds(0, nz - 1)], send.at[3, q])
        await_bytes(gathered.at[q, 0, pl.ds(0, (nx - 1) * nz)], send.at[4, q])
        await_bytes(gathered.at[q, 0], send.at[5, q])
    await_bytes(share.at[pl.ds(0, BANDS - 1)], g_send.at[0])
    await_bytes(pieces_of.at[0, 0, pl.ds(0, nz - 1)], g_send.at[1])
    await_bytes(pieces_of.at[0, pl.ds(0, 2)], g_send.at[2])
    await_bytes(pieces_of.at[0, 0], g_send.at[3])
    await_bytes(pieces_of.at[0], g_send.at[4])


def reduce_and_project(nx, nz, n_grid, basis, panel):
    nq, k = basis.shape
    np_ = panel.shape[0]
    n = np_ * BANDS
    pieces = nx * nz
    rq, rp = nq // pieces, np_ // pieces
    f32 = jnp.float32
    dma = pltpu.SemaphoreType.DMA
    return pl.pallas_call(
        functools.partial(gather_kernel, nx, nz, n_grid),
        out_shape=(
            jax.ShapeDtypeStruct((nq, n), f32),
            jax.ShapeDtypeStruct((np_, k), f32),
        ),
        in_specs=[pl.BlockSpec(memory_space=pltpu.HBM)] * 2,
        out_specs=(pl.BlockSpec(memory_space=pltpu.VMEM),) * 2,
        scratch_shapes=[
            pltpu.VMEM((nq, k), f32),
            pltpu.VMEM((np_, k), f32),
            pltpu.VMEM((BANDS - 1, np_, k), f32),
            pltpu.VMEM((nq + np_, 3 * k), jnp.bfloat16),
            pltpu.VMEM((2 * BLOCK, 3 * k), jnp.bfloat16),
            pltpu.VMEM((ROUNDS, CORES, pieces, rq + rp, BLOCK), f32),
            pltpu.VMEM((ROUNDS, pieces, rq + rp, BLOCK), f32),
            pltpu.VMEM((ROUNDS, nx - 1, nz, rq + rp, BLOCK), f32),
            pltpu.VMEM((ROUNDS, nz - 1, rq + rp, BLOCK), f32),
            pltpu.VMEM((ROUNDS, CORES, pieces, rq, BLOCK), f32),
            pltpu.VMEM((ROUNDS, rp, BLOCK), f32),
            pltpu.VMEM((ROUNDS, CORES, BLOCK, k), f32),
            pltpu.VMEM((BANDS - 1, CORES, BLOCK, k), f32),
            pltpu.VMEM((3 * nq, n), jnp.bfloat16),
            pltpu.VMEM((BANDS, BANDS, KEPT, rp, BLOCK), f32),
            pltpu.VMEM((CORES, nx, nz, BANDS, KEPT, rp, BLOCK), f32),
            pltpu.VMEM((n, n), f32),
            pltpu.VMEM((BLOCK, BLOCK), f32),
            pltpu.VMEM((BLOCK, 3 * BLOCK), jnp.bfloat16),
            pltpu.VMEM((n, 3 * BLOCK), jnp.bfloat16),
            pltpu.VMEM((3 * BLOCK, n), jnp.bfloat16),
            pltpu.VMEM((np_, k), f32),
            pltpu.VMEM((BANDS - 1, np_, k), f32),
            dma((6,)),
            dma((6,)),
            dma((6, ROUNDS)),
            dma((6, ROUNDS)),
            dma((10,)),
            dma((10,)),
            dma((5,)),
            dma((nz - 1,)),
            dma((2, nz)),
            dma((3,)),
            dma((6,)),
            dma((6,)),
            dma((2,)),
        ],
        compiler_params=pltpu.CompilerParams(
            collective_id=0, has_side_effects=True, vmem_limit_bytes=48 * 1024 * 1024
        ),
        cost_estimate=pl.CostEstimate(
            flops=60 * 1024**3, bytes_accessed=8 * 1024 * 1024, transcendentals=0
        ),
    )(basis, panel)


def body(basis, panel):
    grid = lax.axis_size("grid")
    nz = grid // (CORES * ALONG_X)
    coeffs, new_panel = reduce_and_project(
        ALONG_X, nz, panel.shape[1] * grid, basis, panel
    )
    return (new_panel, coeffs)


def solution(mesh):
    placed = (P("band", "grid"), P("band", "grid"))
    return jax.shard_map(
        body,
        mesh=mesh,
        in_specs=placed,
        out_specs=(P("band", "grid"), P("band", None)),
        check_vma=False,
    )
```
